128 devices in a mesh: tp: 2 (over core), fsdp: 64 (over z, y, x).
Axes of the slice: x: 4, y: 4, z: 4, core: 2. Of those that a mesh axis runs over, the one named last changes fastest.
Arguments:
- resid_in: bfloat16 [64, 1536, 1536], P('fsdp', 'tp')
- grad_out: bfloat16 [64, 1536, 1536], P('fsdp', 'tp')
- norm_gain: float32 [1536], replicated
- w_qkv: bfloat16 [1536, 2048], P('fsdp', 'tp')
- b_qkv: bfloat16 [2048], P('tp')
- sinks: float32 [12], P('tp')
- w_out: bfloat16 [1536, 1536], P(('tp', 'fsdp'))
- b_out: bfloat16 [1536], replicated
Outputs:
- output 1: bfloat16 [64, 1536, 1536], P('fsdp', 'tp')
- output 2: bfloat16 [64, 1536, 1536], P('fsdp', 'tp')
- output 3: float32 [1536], replicated
- output 4: float32 [1536, 2048], P('fsdp', 'tp')
- output 5: float32 [2048], P('tp')
- output 6: float32 [12], P('tp')
- output 7: float32 [1536, 1536], P(('tp', 'fsdp'))
- output 8: float32 [1536], replicated
All inputs are finite; a program needn't handle non-finite values.
Results may differ from the reference program's by a relative error of at most 0.0108284.
Values are sent between devices in bfloat16 or wider.
A program may use at most 1 GiB of HBM per device.

```python
import jax
import jax.numpy as jnp
from jax import lax

D = 1536
HEADS = 12
KV_HEADS = 2
HEAD = 128
WINDOW = 128
BATCH = 64
SEQ = 1536

GROUP = HEADS // KV_HEADS
QKV_COLS = (HEADS + 2 * KV_HEADS) * HEAD
N_BLOCKS = SEQ // WINDOW
EPS = 1e-5
ROPE_BASE = 150000.0


def setup_inputs(seed: int = 0) -> dict:
    rng_keys = jax.random.split(jax.random.key(seed), 8)
    resid_in = jax.random.normal(rng_keys[0], (BATCH, SEQ, D), jnp.float32)
    grad_out = jax.random.normal(rng_keys[1], (BATCH, SEQ, D), jnp.float32)
    norm_gain = 1.0 + 0.3 * jax.random.normal(rng_keys[2], (D,), jnp.float32)
    w_qkv = (1.2 / D ** 0.5) * jax.random.normal(rng_keys[3], (D, QKV_COLS), jnp.float32)
    b_qkv = 0.5 * jax.random.normal(rng_keys[4], (QKV_COLS,), jnp.float32)
    sinks = 5.0 + 1.5 * jax.random.normal(rng_keys[5], (HEADS,), jnp.float32)
    w_out = (1.5 / (HEADS * HEAD) ** 0.5) * jax.random.normal(rng_keys[6], (HEADS * HEAD, D), jnp.float32)
    b_out = 0.5 * jax.random.normal(rng_keys[7], (D,), jnp.float32)
    return {
        "resid_in": resid_in.astype(jnp.bfloat16),
        "grad_out": grad_out.astype(jnp.bfloat16),
        "norm_gain": norm_gain,
        "w_qkv": w_qkv.astype(jnp.bfloat16),
        "b_qkv": b_qkv.astype(jnp.bfloat16),
        "sinks": sinks,
        "w_out": w_out.astype(jnp.bfloat16),
        "b_out": b_out.astype(jnp.bfloat16),
    }


def rope_tables(length):
    positions = jnp.arange(length).astype(jnp.float32)
    inv_freq = ROPE_BASE ** (-2.0 * jnp.arange(HEAD // 2).astype(jnp.float32) / HEAD)
    angles = positions[:, None] * inv_freq[None, :]
    return jnp.cos(angles), jnp.sin(angles)


def apply_rope(head_vals, cos_tab, sin_tab):
    half_dim = head_vals.shape[-1] // 2
    first_half = head_vals[..., :half_dim]
    second_half = head_vals[..., half_dim:]
    return jnp.concatenate([first_half * cos_tab - second_half * sin_tab, second_half * cos_tab + first_half * sin_tab], axis=-1)


def block_attend(block_in, sinks):
    q_blk, k_blk, v_blk, block_idx = block_in
    scores = jnp.einsum("iegd,jed->egij", q_blk, k_blk) / HEAD ** 0.5
    q_idx = jnp.arange(WINDOW)[:, None]
    k_idx = jnp.arange(2 * WINDOW)[None, :]
    allowed = (k_idx > q_idx) & (k_idx <= q_idx + WINDOW) & (block_idx * WINDOW - WINDOW + k_idx >= 0)
    scores = jnp.where(allowed, scores, -1e30)
    sink_col = sinks.reshape(KV_HEADS, GROUP)[:, :, None, None]
    row_max = lax.stop_gradient(jnp.maximum(jnp.max(scores, axis=-1, keepdims=True), sink_col))
    exp_scores = jnp.exp(scores - row_max)
    row_denom = jnp.sum(exp_scores, axis=-1, keepdims=True) + jnp.exp(sink_col - row_max)
    attn_probs = (exp_scores / row_denom).astype(jnp.bfloat16).astype(jnp.float32)
    return jnp.einsum("egij,jed->iegd", attn_probs, v_blk)


def row_forward(resid_row, params):
    norm_gain, w_qkv, b_qkv, sinks, w_out, b_out = params
    mean_sq = jnp.mean(resid_row * resid_row, axis=-1, keepdims=True)
    normed = (resid_row * lax.rsqrt(mean_sq + EPS) * norm_gain).astype(jnp.bfloat16).astype(jnp.float32)
    qkv_proj = (jnp.dot(normed, w_qkv, preferred_element_type=jnp.float32) + b_qkv).astype(jnp.bfloat16).astype(jnp.float32)
    qkv_proj = qkv_proj.reshape(SEQ, KV_HEADS, GROUP + 2, HEAD)
    cos_tab, sin_tab = rope_tables(SEQ)
    queries = apply_rope(qkv_proj[:, :, :GROUP], cos_tab[:, None, None], sin_tab[:, None, None]).astype(jnp.bfloat16).astype(jnp.float32)
    keys_rot = apply_rope(qkv_proj[:, :, GROUP], cos_tab[:, None], sin_tab[:, None]).astype(jnp.bfloat16).astype(jnp.float32)
    values = qkv_proj[:, :, GROUP + 1]
    zero_pad = jnp.zeros((WINDOW, KV_HEADS, HEAD), jnp.float32)
    k_prev = jnp.concatenate([zero_pad, keys_rot[:SEQ - WINDOW]], axis=0).reshape(N_BLOCKS, WINDOW, KV_HEADS, HEAD)
    v_prev = jnp.concatenate([zero_pad, values[:SEQ - WINDOW]], axis=0).reshape(N_BLOCKS, WINDOW, KV_HEADS, HEAD)
    k_blocks = jnp.concatenate([k_prev, keys_rot.reshape(N_BLOCKS, WINDOW, KV_HEADS, HEAD)], axis=1)
    v_blocks = jnp.concatenate([v_prev, values.reshape(N_BLOCKS, WINDOW, KV_HEADS, HEAD)], axis=1)
    q_blocks = queries.reshape(N_BLOCKS, WINDOW, KV_HEADS, GROUP, HEAD)
    attend = jax.checkpoint(block_attend)
    attn_out = lax.map(lambda block_in: attend(block_in, sinks), (q_blocks, k_blocks, v_blocks, jnp.arange(N_BLOCKS)))
    attn_out = attn_out.reshape(SEQ, HEADS * HEAD).astype(jnp.bfloat16).astype(jnp.float32)
    resid_out = resid_row + jnp.dot(attn_out, w_out, preferred_element_type=jnp.float32) + b_out
    return resid_out.astype(jnp.bfloat16)


def reference(resid_in, grad_out, norm_gain, w_qkv, b_qkv, sinks, w_out, b_out):
    params = (norm_gain, w_qkv.astype(jnp.float32), b_qkv.astype(jnp.float32), sinks, w_out.astype(jnp.float32), b_out.astype(jnp.float32))

    def row_step(grad_acc, row_in):
        resid_row, grad_row = row_in
        resid_out, pullback = jax.vjp(row_forward, resid_row.astype(jnp.float32), params)
        d_resid, row_grads = pullback(grad_row)
        new_acc = tuple(acc_sum + new_grad for acc_sum, new_grad in zip(grad_acc, row_grads))
        return new_acc, (resid_out, d_resid.astype(jnp.bfloat16))

    zero_acc = tuple(jnp.zeros_like(param_val) for param_val in params)
    grad_sums, (resid_rows, grad_rows) = lax.scan(row_step, zero_acc, (resid_in, grad_out))
    return (resid_rows, grad_rows, grad_sums[0], grad_sums[1], grad_sums[2], grad_sums[3], grad_sums[4], grad_sums[5])
```

```python
import jax
import jax.numpy as jnp
from jax import lax
from jax.experimental import pallas as pl
from jax.experimental.pallas import tpu as pltpu
from jax.sharding import PartitionSpec as P

EPS = 1e-5
ROPE_BASE = 150000.0
WINDOW = 128
MESH = pl.DeviceIdType.MESH
STRIDE = (16, 4, 1)
F32 = jnp.float32
BF16 = jnp.bfloat16
VMEM_LIMIT = 67_000_000
Z, Y, X = range(3)
UP, DOWN, FAR = 1, -1, 2
L = 128
NEG = -1e30


def coord(dim):
    return lax.rem(lax.div(lax.axis_index("fsdp"), STRIDE[dim]), 4)


def shifted(dim, k):
    return lax.rem(coord(dim) + (k + 4), 4)


def peer(dim, k):
    f = lax.axis_index("fsdp")
    return {"fsdp": f + (shifted(dim, k) - coord(dim)) * STRIDE[dim]}


def partner():
    return {"tp": 1 - lax.axis_index("tp")}


def entry_barrier(peers):
    barrier = pltpu.get_barrier_semaphore()
    for p in peers:
        pl.semaphore_signal(barrier, inc=1, device_id=p, device_id_type=MESH)
    pl.semaphore_wait(barrier, len(peers))


def ring_peers():
    return [peer(dim, k) for dim in range(3) for k in (UP, DOWN)]


class Copies:
    def __init__(self, send_sem, recv_sem):
        self.send_sem, self.recv_sem = send_sem, recv_sem
        self.n = 0
        self.sent = []

    def slots(self, count):
        first = self.n
        self.n += count
        return first

    def make(self, src, dst, slot, device):
        return pltpu.make_async_remote_copy(src_ref=src, dst_ref=dst, send_sem=self.send_sem.at[slot], recv_sem=self.recv_sem.at[slot], device_id=device, device_id_type=MESH)

    def send(self, src, dst, slot, device):
        copy = self.make(src, dst, slot, device)
        copy.start()
        self.sent.append(copy)

    def arrive(self, ref, slot, device):
        self.make(ref, ref, slot, device).wait_recv()

    def drain(self):
        for copy in self.sent:
            copy.wait_send()
        self.sent = []


class GatherStage:
    def __init__(self, copies, dim, slot_view, own_view):
        self.c, self.dim, self.view, self.own = copies, dim, slot_view, own_view
        self.base = copies.slots(6)

    def start(self):
        me = coord(self.dim)
        for h in (0, 1):
            self.c.send(self.own(h), self.view(me, h), self.base + h, peer(self.dim, UP))
            self.c.send(self.own(1 - h), self.view(me, 1 - h), self.base + 3 - h, peer(self.dim, DOWN))

    def sides(self):
        return [(shifted(self.dim, k), peer(self.dim, k)) for k in (DOWN, UP)]

    def mid(self):
        (lo, down), (hi, up) = self.sides()
        self.c.arrive(self.view(lo, 0), self.base, down)
        self.c.send(self.view(lo, 0), self.view(lo, 0), self.base + 4, up)
        self.c.arrive(self.view(hi, 1), self.base + 3, up)
        self.c.send(self.view(hi, 1), self.view(hi, 1), self.base + 5, down)

    def finish(self):
        (lo, down), (hi, up) = self.sides()
        far = shifted(self.dim, FAR)
        for n, (at, h, dev) in enumerate(((lo, 1, down), (hi, 0, up))):
            self.c.arrive(self.view(at, h), self.base + 1 + n, dev)
            self.c.arrive(self.view(far, n), self.base + 4 + n, dev)


def gather_stages(copies, in_ref, out_ref, order, cols):
    half_cols = [pl.ds(cols[0], cols[1]), pl.ds(cols[0] + cols[1], cols[2])]
    stages = []
    for n in range(3):
        def view(c, h, n=n):
            idx = []
            for dim in range(3):
                if dim == order[n]:
                    idx.append(c)
                elif dim in order[:n]:
                    idx.append(slice(None))
                else:
                    idx.append(coord(dim))
            return out_ref.at[tuple(idx) + (slice(None), half_cols[h])]
        if n == 0:
            own = lambda h: in_ref.at[:, half_cols[h]]
        else:
            own = lambda h, n=n, view=view: view(coord(order[n]), h)
        stages.append(GatherStage(copies, order[n], view, own))
    return stages


def gather_kernel(wq_in, wo_in, x_ref, dy_ref, g_ref, wq_out, wo_out, h_all, dy_all, wq_oth, wo_oth, h_own, send_sem, recv_sem, loc_sem):
    tp = lax.axis_index("tp")
    for ref, own in ((wq_out, wq_in), (wo_out, wo_in)):
        ref[coord(Z), coord(Y), coord(X)] = own[...]
    entry_barrier(ring_peers() + [partner()])
    copies = Copies(send_sem, recv_sem)
    jobs = [gather_stages(copies, wq_in, wq_out, (X, Y, Z), (0, 256, L)), gather_stages(copies, wq_in, wq_out, (Y, Z, X), (384, L, 256)),
            gather_stages(copies, wq_in, wq_out, (Z, X, Y), (768, L, L))]
    jobs += [gather_stages(copies, wo_in, wo_out, order, (n * 256, L, L)) for n, order in enumerate(((X, Y, Z), (Y, Z, X), (Z, X, Y)))]
    for job in jobs:
        job[0].start()
    local = [pltpu.make_async_copy(dy_ref, dy_all.at[tp], loc_sem.at[0])]
    local[0].start()
    slot_dy = copies.slots(1)
    copies.send(dy_ref, dy_all.at[tp], slot_dy, partner())
    rows = x_ref.shape[0]
    parts = 6
    slot_h = copies.slots(parts)
    step = rows // parts
    gain = g_ref[...]

    def norm_part(k):
        @pl.loop(0, step // 32)
        def _(i):
            at = pl.ds(k * step + i * 32, 32)
            xv = x_ref[at, :].astype(F32)
            inv = lax.rsqrt(jnp.mean(xv * xv, axis=-1, keepdims=True) + EPS)
            h_own[at, :] = (xv * inv * gain).astype(BF16)

    def send_part(k):
        at = pl.ds(k * step, step)
        copy = pltpu.make_async_copy(h_own.at[at, :], h_all.at[tp, at, :], loc_sem.at[1 + k])
        copy.start()
        local.append(copy)
        copies.send(h_own.at[at, :], h_all.at[tp, at, :], slot_h + k, partner())

    part = 0
    for n in range(3):
        for phase in range(2):
            norm_part(part)
            if part > 0:
                send_part(part - 1)
            part += 1
            for job in jobs:
                if phase == 0:
                    job[n].mid()
                else:
                    job[n].finish()
                    if n < 2:
                        job[n + 1].start()
    send_part(parts - 1)
    slot_w = copies.slots(2)
    copies.send(wq_out, wq_oth, slot_w, partner())
    copies.send(wo_out, wo_oth, slot_w + 1, partner())
    oth = 1 - tp
    copies.arrive(dy_all.at[oth], slot_dy, partner())
    for k in range(parts):
        copies.arrive(h_all.at[oth, pl.ds(k * step, step), :], slot_h + k, partner())
    copies.arrive(wq_oth, slot_w, partner())
    copies.arrive(wo_oth, slot_w + 1, partner())
    copies.drain()
    for copy in local:
        copy.wait()


VM = pl.BlockSpec(memory_space=pltpu.VMEM)
ANY = pl.BlockSpec(memory_space=pl.ANY)


def gather_all(wq_in, wo_in, x, dy, gain):
    rows, d = x.shape
    wq_shape = jax.ShapeDtypeStruct((4, 4, 4) + wq_in.shape, BF16)
    wo_shape = jax.ShapeDtypeStruct((4, 4, 4) + wo_in.shape, BF16)
    act = jax.ShapeDtypeStruct((2, rows, d), BF16)
    n = 6 * 18 + 1 + 6 + 2
    return pl.pallas_call(
        gather_kernel, name="gather_all",
        out_shape=(wq_shape, wo_shape, act, act, wq_shape, wo_shape),
        in_specs=[VM] * 5, out_specs=(VM, VM, ANY, ANY, ANY, ANY),
        scratch_shapes=[pltpu.VMEM((rows, d), BF16), pltpu.SemaphoreType.DMA((n,)), pltpu.SemaphoreType.DMA((n,)), pltpu.SemaphoreType.DMA((7,))],
        compiler_params=pltpu.CompilerParams(collective_id=0, has_side_effects=True, vmem_limit_bytes=VMEM_LIMIT),
    )(wq_in, wo_in, x, dy, gain)


def rotate(vals, cos, sin):
    return vals * cos + pltpu.roll(vals, 64, 1) * sin


def stack_heads(ref, heads):
    return jnp.concatenate([ref[:, i * L:(i + 1) * L] for i in range(heads)], axis=0)


def dot_tn(a, b):
    return lax.dot_general(a, b, (((0,), (0,)), ((), ())), preferred_element_type=F32)


def dot_nt(a, b):
    return lax.dot_general(a, b, (((1,), (1,)), ((), ())), preferred_element_type=F32)


def attend_kernel(heads, n_blocks, qkv_ref, do_ref, cos_ref, sin_ref, sink_ref, o_ref, dqkv_ref, dsink_ref, k_buf, v_buf, dk_buf, dv_buf, tab_buf):
    i = pl.program_id(0)
    scale = 128.0 ** -0.5
    width = heads * L

    @pl.when(i == 0)
    def _():
        k_buf[...] = jnp.zeros_like(k_buf)
        v_buf[...] = jnp.zeros_like(v_buf)
        dk_buf[...] = jnp.zeros_like(dk_buf)
        dv_buf[...] = jnp.zeros_like(dv_buf)
        dsink_ref[...] = jnp.zeros_like(dsink_ref)

    @pl.when(i > 0)
    def _():
        k_buf[0:L, :] = k_buf[L:2 * L, :]
        v_buf[0:L, :] = v_buf[L:2 * L, :]
        dk_buf[0:L, :] = dk_buf[L:2 * L, :]
        dv_buf[0:L, :] = dv_buf[L:2 * L, :]
        tab_buf[0:2] = tab_buf[2:4]

    cos, sin = cos_ref[...], sin_ref[...]
    tab_buf[2], tab_buf[3] = cos, sin
    cos_all = jnp.concatenate([cos] * heads, axis=0)
    sin_all = jnp.concatenate([sin] * heads, axis=0)
    k_buf[L:2 * L, :] = rotate(qkv_ref[:, width:width + L].astype(F32), cos, sin).astype(BF16)
    v_buf[L:2 * L, :] = qkv_ref[:, width + L:width + 2 * L]
    q = rotate(stack_heads(qkv_ref, heads).astype(F32), cos_all, sin_all).astype(BF16)
    do = stack_heads(do_ref, heads)
    keys, vals = k_buf[...], v_buf[...]
    sink = sink_ref[...]

    scores = dot_nt(keys, q) * scale
    k_idx = lax.broadcasted_iota(jnp.int32, (256, 128), 0)
    q_idx = lax.broadcasted_iota(jnp.int32, (256, 128), 1)
    allowed = (k_idx > q_idx) & (k_idx <= q_idx + WINDOW) & ((k_idx >= WINDOW) | (i > 0))
    bias = jnp.where(allowed, 0.0, NEG)
    scores = scores + jnp.concatenate([bias] * heads, axis=1)
    top = jnp.maximum(jnp.max(scores, axis=0, keepdims=True), sink)
    probs = jnp.exp(scores - top)
    sink_exp = jnp.exp(sink - top)
    inv = 1.0 / (jnp.sum(probs, axis=0, keepdims=True) + sink_exp)
    probs = probs * inv
    probs_b = probs.astype(BF16)
    out = dot_tn(probs_b, vals).astype(BF16)
    for h in range(heads):
        o_ref[:, h * L:(h + 1) * L] = out[h * L:(h + 1) * L, :]
    d_probs = dot_nt(vals, do).astype(BF16).astype(F32)
    row_dot = jnp.sum(probs * d_probs, axis=0, keepdims=True)
    d_scores = (probs * (d_probs - row_dot)).astype(BF16)
    dsink_ref[...] += -(sink_exp * inv * row_dot)
    dv_new = jnp.dot(probs_b, do, preferred_element_type=F32)
    dk_new = jnp.dot(d_scores, q, preferred_element_type=F32) * scale
    dq = (dot_tn(d_scores, keys) * scale).astype(BF16).astype(F32)
    dq = rotate(dq, cos_all, -sin_all).astype(BF16)
    here = pl.ds(pl.multiple_of(i * L, 128), 128)
    for h in range(heads):
        dqkv_ref[here, h * L:(h + 1) * L] = dq[h * L:(h + 1) * L, :]

    dk_prev = dk_buf[0:L, :] + dk_new[0:L, :]
    dv_prev = dv_buf[0:L, :] + dv_new[0:L, :]

    def put(at, dk, dv, c, s):
        dqkv_ref[at, width:width + L] = rotate(dk.astype(BF16).astype(F32), c, -s).astype(BF16)
        dqkv_ref[at, width + L:width + 2 * L] = dv.astype(BF16)

    @pl.when(i > 0)
    def _():
        put(pl.ds(pl.multiple_of((i - 1) * L, 128), 128), dk_prev, dv_prev, tab_buf[0], tab_buf[1])

    dk_buf[L:2 * L, :] = dk_new[L:2 * L, :]
    dv_buf[L:2 * L, :] = dv_new[L:2 * L, :]

    @pl.when(i == n_blocks - 1)
    def _():
        put(here, dk_new[L:2 * L, :], dv_new[L:2 * L, :], cos, sin)


def attend(qkv, d_o, cos, sin, sink_row):
    seq, cols = qkv.shape
    width = d_o.shape[1]
    heads = width // 128
    n_blocks = seq // WINDOW
    def row(c):
        return pl.BlockSpec((WINDOW, c), lambda i: (i, 0))

    def whole(*s):
        return pl.BlockSpec(s, lambda i: (0, 0))

    def kernel(*refs):
        attend_kernel(heads, n_blocks, *refs)

    return pl.pallas_call(
        kernel, name="attend", grid=(n_blocks,),
        out_shape=(jax.ShapeDtypeStruct((seq, width), BF16), jax.ShapeDtypeStruct((seq, cols), BF16), jax.ShapeDtypeStruct((1, width), F32)),
        in_specs=[row(cols), row(width), row(128), row(128), whole(1, width)],
        out_specs=(row(width), whole(seq, cols), whole(1, width)),
        scratch_shapes=[pltpu.VMEM((2 * L, L), t) for t in (BF16, BF16, F32, F32)] + [pltpu.VMEM((4, L, L), F32)],
        compiler_params=pltpu.CompilerParams(dimension_semantics=("arbitrary",), vmem_limit_bytes=VMEM_LIMIT),
    )(qkv, d_o, cos, sin, sink_row)


class ScatterStage:
    def __init__(self, copies, dim, blk, buf, put):
        self.c, self.dim, self.blk, self.buf, self.put = copies, dim, blk, buf, put
        self.base = copies.slots(6)
        self.a_up, self.a_down, self.lo = 0, 1, (2, 3)
        self.hi = (4, 5)

    def send(self, src, slot, k):
        self.c.send(src, self.buf.at[slot], self.base + slot, peer(self.dim, k))

    def arrive(self, slot, k):
        self.c.arrive(self.buf.at[slot], self.base + slot, peer(self.dim, k))

    def start(self):
        up, down, far = (shifted(self.dim, k) for k in (UP, DOWN, FAR))
        self.send(self.blk(far, 0), self.a_up, UP)
        self.send(self.blk(far, 1), self.a_down, DOWN)
        self.send(self.blk(up, 1), self.lo[1], UP)
        self.send(self.blk(down, 0), self.hi[0], DOWN)

    def add(self, slot, src):
        dst = self.buf.at[slot]
        if len(src.shape) == 2:
            dst[...] = dst[...] + src[...]
        else:
            @pl.loop(0, src.shape[0])
            def _(j):
                dst[j] = dst[j] + src[j]

    def mid(self):
        self.arrive(self.a_up, DOWN)
        self.add(self.a_up, self.blk(shifted(self.dim, UP), 0))
        self.arrive(self.a_down, UP)
        self.add(self.a_down, self.blk(shifted(self.dim, DOWN), 1))
        self.send(self.buf.at[self.a_up], self.lo[0], UP)
        self.send(self.buf.at[self.a_down], self.hi[1], DOWN)

    def finish(self):
        me = coord(self.dim)
        for h in (1, 0):
            self.arrive(self.lo[h], DOWN)
            self.arrive(self.hi[1 - h], UP)
        for h in (0, 1):
            own, a, b = self.blk(me, h), self.buf.at[self.lo[h]], self.buf.at[self.hi[h]]
            if len(own.shape) == 2:
                self.put(h, None, own[...] + a[...] + b[...])
            else:
                @pl.loop(0, own.shape[0])
                def _(j):
                    self.put(h, j, own[j] + a[j] + b[j])


class DirectStage:
    def __init__(self, copies, dim, blk, buf, put):
        self.c, self.dim, self.blk, self.buf, self.put = copies, dim, blk, buf, put
        self.base = copies.slots(3)

    def start(self):
        for slot, k in enumerate((UP, DOWN, FAR)):
            self.c.send(self.blk(shifted(self.dim, k)), self.buf.at[slot], self.base + slot, peer(self.dim, k))

    def finish(self):
        for slot, k in enumerate((UP, DOWN, FAR)):
            self.c.arrive(self.buf.at[slot], self.base + slot, peer(self.dim, k))
        b = self.buf
        self.put((self.blk(coord(self.dim))[...] + b[0]) + (b[1] + b[2]))


def scatter_stages(copies, src, out, order, first, width, bufs, padded):
    hw = width // 2
    r1, r2, r3, s2, s3 = bufs
    rows = out.shape[0]
    rest = [dim for dim in range(3) if dim != order[0]]

    def pick(ref, at, t, cols):
        idx = [slice(None)] * (len(ref.shape) - 1)
        idx[at] = t
        return ref.at[tuple(idx) + (cols,)]

    def part(h, base=0):
        return pl.ds(base + h * hw, hw)

    def put1(h, j, val):
        s2[j, ..., part(h)] = val

    def put2(h, j, val):
        if padded:
            for t in range(4):
                s3[t, 0:rows, part(h)] = val[rows * t:rows * t + rows, :]
        else:
            s3[j, :, part(h)] = val

    def put3(val):
        out[:, pl.ds(first, width)] = val[0:rows, :]

    return (ScatterStage(copies, order[0], lambda t, h: pick(src, order[0], t, part(h, first)), r1, put1),
            ScatterStage(copies, order[1], lambda t, h: pick(s2, rest.index(order[1]), t, part(h)), r2, put2),
            DirectStage(copies, order[2], lambda t: s3.at[t], r3, put3))


WO_JOBS = (((Y, Z, X), 0, 768), ((Z, Y, X), 768, 768))
WQ_JOBS = (((X, Y, Z), 0, 512), ((Y, Z, X), 512, 256), ((Z, X, Y), 768, 256))


def scatter_scratch():
    out = []
    for jobs, lead, rows, pad in ((WO_JOBS, (4,), 48, 16), (WQ_JOBS, (4, 4), 24, 24)):
        for _, _, width in jobs:
            hw = width // 2
            out += [pltpu.VMEM((6,) + lead + (rows, hw), F32), pltpu.VMEM((6,) + lead[1:] + (rows, hw), F32), pltpu.VMEM((3, pad, width), F32),
                    pltpu.VMEM(lead + (rows, width), F32), pltpu.VMEM((4, pad, width), F32)]
    return out


class SmallSums:
    def __init__(self, copies, ar):
        self.c, self.ar = copies, ar
        self.base = copies.slots(10)

    def start(self, n):
        if n < 3:
            for slot, k in enumerate((UP, DOWN, FAR)):
                ref = self.ar.at[n, coord(n)]
                self.c.send(ref, ref, self.base + 3 * n + slot, peer(n, k))
        else:
            ref = self.ar.at[n, lax.axis_index("tp")]
            self.c.send(ref, ref, self.base + 3 * n, partner())

    def finish(self, n):
        ar = self.ar
        if n < 3:
            for slot, k in enumerate((UP, DOWN, FAR)):
                self.c.arrive(ar.at[n, shifted(n, -k)], self.base + 3 * n + slot, peer(n, k))
            total = (ar[n, 0] + ar[n, 1]) + (ar[n, 2] + ar[n, 3])
            ar[n + 1, coord(n + 1) if n < 2 else lax.axis_index("tp")] = total
        else:
            self.c.arrive(ar.at[n, 1 - lax.axis_index("tp")], self.base + 3 * n, partner())


def grads_kernel(o_in, dqkv_in, h_in, dy_in, x_in, wq_in, wo_in, wq2_in, wo2_in, gain_ref, bout_ref, sink_in,
                 y_out, dx_out, gq_out, go_out, gain_out, gbout_out, bqkv_out, sink_out, *scratch):
    bufs = list(scratch)
    o, dqkv, h, dy, x, wq, wo, wq2, wo2, o2, dqkv2, gq, go, ar, loc_sem, send_sem, recv_sem = bufs[:17]
    bufs = bufs[17:]
    tp = lax.axis_index("tp")
    half, d = x.shape
    loads = [pltpu.make_async_copy(a, b, loc_sem.at[n]) for n, (a, b) in enumerate((
        (o_in, o), (dy_in, dy), (h_in, h), (dqkv_in, dqkv), (wo_in, wo), (wo2_in, wo2), (wq_in, wq), (wq2_in, wq2), (x_in, x)))]
    for copy in loads:
        copy.start()
    entry_barrier([peer(dim, k) for dim in range(3) for k in (UP, DOWN, FAR)] + [partner()])
    copies = Copies(send_sem, recv_sem)
    theirs = pl.ds((1 - tp) * half, half)
    slot_x = copies.slots(2)
    copies.send(o_in.at[theirs, :], o2, slot_x, partner())
    copies.send(dqkv_in.at[theirs, :], dqkv2, slot_x + 1, partner())
    small = SmallSums(copies, ar)
    jobs_wo = [scatter_stages(copies, go, go_out, *job, [bufs.pop(0) for _ in range(5)], True) for job in WO_JOBS]
    jobs_wq = [scatter_stages(copies, gq, gq_out, *job, [bufs.pop(0) for _ in range(5)], False) for job in WQ_JOBS]
    own = ar.at[Z, coord(Z)]
    own[...] = jnp.zeros(own.shape, F32)
    for job in jobs_wo:
        s3 = job[2].blk(slice(None))
        s3[...] = jnp.zeros(s3.shape, F32)

    def each(jobs, n, what):
        for job in jobs:
            getattr(job[n], what)()

    loads[0].wait()
    loads[1].wait()

    @pl.loop(0, 2)
    def _(m):
        @pl.loop(0, 3)
        def _(n):
            rows = pl.ds(pl.multiple_of(m * 384, L), 384)
            cols = pl.ds(pl.multiple_of(n * 512, L), 512)
            go[pl.ds(m * 2, 2), :, :, cols] = dot_tn(o[:, rows], dy[:, cols]).reshape(2, 4, 48, 512)

    each(jobs_wo, 0, "start")
    loads[2].wait()
    loads[3].wait()

    @pl.loop(0, 4)
    def _(m):
        gq[m] = dot_tn(h[:, pl.ds(pl.multiple_of(m * 384, L), 384)], dqkv[...]).reshape(4, 4, 24, -1)

    each(jobs_wq, 0, "start")
    ones = jnp.ones((8, 2 * half), BF16)
    own[2:3, 0:dqkv.shape[1]] = jnp.dot(ones, dqkv[...], preferred_element_type=F32)[0:1]
    own[3:4, 0:sink_in.shape[1]] = sink_in[...]
    mine = pl.multiple_of(tp * half, half)
    own[1:2, :] = jnp.dot(ones[:, 0:half], dy[pl.ds(mine, half), :], preferred_element_type=F32)[0:1]
    for copy in loads[4:]:
        copy.wait()
    copies.arrive(o2, slot_x, partner())
    copies.arrive(dqkv2, slot_x + 1, partner())
    each(jobs_wo, 0, "mid")
    tile = half // 3

    @pl.loop(0, 3)
    def _(n):
        at = pl.ds(pl.multiple_of(n * tile, tile), tile)
        at_all = pl.ds(pl.multiple_of(mine + n * tile, tile), tile)
        acc = jnp.dot(o[at_all, :], wo[...], preferred_element_type=F32) + jnp.dot(o2[at, :], wo2[...], preferred_element_type=F32)
        h[at, :] = (x[at, :].astype(F32) + acc + bout_ref[...]).astype(BF16)

    store_y = pltpu.make_async_copy(h.at[pl.ds(0, half), :], y_out, loc_sem.at[0])
    store_y.start()
    each(jobs_wo, 0, "finish")
    each(jobs_wo, 1, "start")
    each(jobs_wq, 0, "mid")
    gain = gain_ref[...]

    @pl.loop(0, 3)
    def _(n):
        at = pl.ds(pl.multiple_of(n * tile, tile), tile)
        at_all = pl.ds(pl.multiple_of(mine + n * tile, tile), tile)
        dh = dot_nt(dqkv[at_all, :], wq[...]) + dot_nt(dqkv2[at, :], wq2[...])
        dh = dh.astype(BF16).astype(F32)
        xv = x[at, :].astype(F32)
        inv = lax.rsqrt(jnp.mean(xv * xv, axis=-1, keepdims=True) + EPS)
        gg = dh * gain
        dx = inv * (gg - xv * (inv * inv * jnp.mean(gg * xv, axis=-1, keepdims=True)))
        dy[at_all, :] = (dy[at_all, :].astype(F32) + dx).astype(BF16)
        own[0:1, :] = own[0:1, :] + jnp.sum(dh * (xv * inv), axis=0, keepdims=True)

    store_dx = pltpu.make_async_copy(dy.at[pl.ds(mine, half), :], dx_out, loc_sem.at[1])
    store_dx.start()
    small.start(0)
    each(jobs_wo, 1, "mid")
    small.finish(0)
    small.start(1)
    each(jobs_wq, 0, "finish")
    each(jobs_wq, 1, "start")
    each(jobs_wo, 1, "finish")
    each(jobs_wo, 2, "start")
    small.finish(1)
    small.start(2)
    each(jobs_wq, 1, "mid")
    small.finish(2)
    small.start(3)
    each(jobs_wo, 2, "finish")
    each(jobs_wq, 1, "finish")
    each(jobs_wq, 2, "start")
    small.finish(3)
    both = ar[3, 0] + ar[3, 1]
    row = ar[3, tp]
    gain_out[...] = both[0:1, :]
    gbout_out[...] = both[1:2, :]
    bqkv_out[...] = row[2:3, 0:bqkv_out.shape[1]]
    lane = lax.broadcasted_iota(jnp.int32, sink_out.shape, 1)
    sinks = jnp.zeros(sink_out.shape, F32)
    for n in range(sink_in.shape[1] // L):
        sinks = jnp.where(lane == n, jnp.sum(row[3:4, n * L:n * L + L], axis=1, keepdims=True), sinks)
    sink_out[...] = sinks
    each(jobs_wq, 2, "finish")
    copies.drain()
    store_y.wait()
    store_dx.wait()


def all_grads(o, dqkv, h, dy, x, wq, wo, wq2, wo2, gain, b_out, sink_part):
    half, d = x.shape
    seq, width = o.shape
    cols = dqkv.shape[1]
    n = 2 + 10 + len(WO_JOBS + WQ_JOBS) * 15
    sds = jax.ShapeDtypeStruct
    row = sds((1, d), F32)
    like = [pltpu.VMEM(a.shape, BF16) for a in (o, dqkv, h, dy, x, wq, wo, wq2, wo2)]
    scratch = like + [pltpu.VMEM((half, width), BF16), pltpu.VMEM((half, cols), BF16), pltpu.VMEM((4, 4, 4, 24, cols), F32), pltpu.VMEM((4, 4, 48, d), F32),
                      pltpu.VMEM((4, 4, 4, d), F32),
                      pltpu.SemaphoreType.DMA((9,)), pltpu.SemaphoreType.DMA((n,)), pltpu.SemaphoreType.DMA((n,))]
    return pl.pallas_call(
        grads_kernel, name="all_grads",
        out_shape=(sds((half, d), BF16), sds((half, d), BF16), sds((24, cols), F32), sds((12, d), F32), row, row, sds((1, cols), F32), sds((1, L), F32)),
        in_specs=[ANY] * 9 + [VM] * 3, out_specs=(ANY, ANY) + (VM,) * 6, scratch_shapes=scratch + scatter_scratch(),
        compiler_params=pltpu.CompilerParams(collective_id=1, has_side_effects=True, vmem_limit_bytes=VMEM_LIMIT),
    )(o, dqkv, h, dy, x, wq, wo, wq2, wo2, gain, b_out, sink_part)


def rope_tables(seq, head_dim):
    inv_freq = ROPE_BASE ** (-2.0 * jnp.arange(head_dim // 2).astype(F32) / head_dim)
    angles = jnp.arange(seq).astype(F32)[:, None] * inv_freq[None, :]
    cos, sin = jnp.cos(angles), jnp.sin(angles)
    return jnp.concatenate([cos, cos], axis=1), jnp.concatenate([-sin, sin], axis=1)


def solution(mesh):
    act_spec = P("fsdp", "tp", None)
    wout_spec = P(("tp", "fsdp"), None)
    in_specs = (act_spec, act_spec, P(), P("fsdp", "tp"), P("tp"), P("tp"), wout_spec, P())
    out_specs = (act_spec, act_spec, P(), P("fsdp", "tp"), P("tp"), P("tp"), wout_spec, P())

    def device_step(resid_loc, grad_loc, norm_gain, wqkv_loc, bqkv_loc, sink_loc, wout_loc, b_out):
        x, dy = resid_loc[0], grad_loc[0]
        half, d = x.shape
        seq = 2 * half
        heads = sink_loc.shape[0]
        width = heads * L
        tp = lax.axis_index("tp")
        wo_slab = jnp.concatenate([wout_loc[:, :d // 2], wout_loc[:, d // 2:]], axis=0)
        wq6, wo6, h_all, dy_all, wq_oth6, wo_oth6 = gather_all(wqkv_loc, wo_slab, x, dy, norm_gain[None, :])

        def wo_rows(w):
            return w.reshape(64, 2, 12, d // 2).transpose(0, 2, 1, 3).reshape(width, d)

        wq, wq_oth = wq6.reshape(d, -1), wq_oth6.reshape(d, -1)
        wo, wo_oth = wo_rows(wo6), wo_rows(wo_oth6)
        h_all, dy_all = h_all.reshape(seq, d), dy_all.reshape(seq, d)
        qkv = (jnp.dot(h_all, wq, preferred_element_type=F32) + bqkv_loc.astype(F32)).astype(BF16)
        d_o = jnp.einsum("tk,hk->th", dy_all, wo, preferred_element_type=F32).astype(BF16)
        cos, sin = rope_tables(seq, 128)
        sink_row = jnp.repeat(sink_loc, 128)[None, :]
        o, dqkv, dsink = attend(qkv, d_o, cos, sin, sink_row)
        outs = all_grads(o, dqkv, h_all, dy_all, x, wq, wo, wq_oth, wo_oth, norm_gain[None, :], b_out.astype(F32)[None, :], dsink)
        resid_out, grad_resid, gq, go, gain_g, bout_g, bqkv_g, sink_g = outs
        return (resid_out[None], grad_resid[None], gain_g[0], gq, bqkv_g[0], sink_g[0, :heads], go, bout_g[0])

    return jax.shard_map(device_step, mesh=mesh, in_specs=in_specs, out_specs=out_specs, check_vma=False)
```

```python
import jax
import jax.numpy as jnp
import numpy as np
from jax import lax
from jax.experimental import pallas as pl
from jax.experimental.pallas import tpu as pltpu
from jax.sharding import PartitionSpec as P

EPS = 1e-5
ROPE_BASE = 150000.0
WINDOW = 128
MESH = pl.DeviceIdType.MESH
STRIDE = (16, 4, 1)
F32 = jnp.float32
BF16 = jnp.bfloat16
VMEM_LIMIT = 67_000_000
Z, Y, X = range(3)
UP, DOWN, FAR = 1, -1, 2
L = 128
NEG = -1e30


def coord(dim):
    return lax.rem(lax.div(lax.axis_index("fsdp"), STRIDE[dim]), 4)


def shifted(dim, k):
    return lax.rem(coord(dim) + (k + 4), 4)


def peer(dim, k):
    f = lax.axis_index("fsdp")
    return {"fsdp": f + (shifted(dim, k) - coord(dim)) * STRIDE[dim]}


def partner():
    return {"tp": 1 - lax.axis_index("tp")}


def entry_barrier(peers):
    barrier = pltpu.get_barrier_semaphore()
    for p in peers:
        pl.semaphore_signal(barrier, inc=1, device_id=p, device_id_type=MESH)
    pl.semaphore_wait(barrier, len(peers))


class Copies:
    def __init__(self, send_sem, recv_sem):
        self.send_sem, self.recv_sem = send_sem, recv_sem
        self.n = 0
        self.sent = []

    def slots(self, count):
        first = self.n
        self.n += count
        return first

    def make(self, src, dst, slot, device):
        return pltpu.make_async_remote_copy(src_ref=src, dst_ref=dst, send_sem=self.send_sem.at[slot], recv_sem=self.recv_sem.at[slot], device_id=device, device_id_type=MESH)

    def send(self, src, dst, slot, device):
        copy = self.make(src, dst, slot, device)
        copy.start()
        self.sent.append(copy)

    def arrive(self, ref, slot, device):
        self.make(ref, ref, slot, device).wait_recv()

    def drain(self):
        for copy in self.sent:
            copy.wait_send()
        self.sent = []


class GatherStage:
    def __init__(self, copies, dim, slot_view, own_view):
        self.c, self.dim, self.view, self.own = copies, dim, slot_view, own_view
        self.base = copies.slots(6)

    def start(self):
        me = coord(self.dim)
        for h in (0, 1):
            self.c.send(self.own(h), self.view(me, h), self.base + h, peer(self.dim, UP))
            self.c.send(self.own(1 - h), self.view(me, 1 - h), self.base + 3 - h, peer(self.dim, DOWN))

    def sides(self):
        return [(shifted(self.dim, k), peer(self.dim, k)) for k in (DOWN, UP)]

    def mid(self):
        (lo, down), (hi, up) = self.sides()
        self.c.arrive(self.view(lo, 0), self.base, down)
        self.c.send(self.view(lo, 0), self.view(lo, 0), self.base + 4, up)
        self.c.arrive(self.view(hi, 1), self.base + 3, up)
        self.c.send(self.view(hi, 1), self.view(hi, 1), self.base + 5, down)

    def finish(self):
        (lo, down), (hi, up) = self.sides()
        far = shifted(self.dim, FAR)
        for n, (at, h, dev) in enumerate(((lo, 1, down), (hi, 0, up))):
            self.c.arrive(self.view(at, h), self.base + 1 + n, dev)
            self.c.arrive(self.view(far, n), self.base + 4 + n, dev)


class GatherDirect:
    def __init__(self, copies, dim, view, own):
        self.c, self.dim, self.view, self.own = copies, dim, view, own
        self.base = copies.slots(3)

    def start(self):
        for slot, k in enumerate((UP, DOWN, FAR)):
            self.c.send(self.own(), self.view(coord(self.dim)), self.base + slot, peer(self.dim, k))

    def finish(self):
        for slot, k in enumerate((UP, DOWN, FAR)):
            self.c.arrive(self.view(shifted(self.dim, -k)), self.base + slot, peer(self.dim, k))


def gather_stages(copies, in_ref, out_ref, order, first, widths):
    whole = pl.ds(first, sum(widths))
    halves = [pl.ds(first, widths[0]), pl.ds(first + widths[0], widths[1])]

    def view(n, c, cols):
        idx = [coord(dim) for dim in range(3)]
        for dim in order[:n]:
            idx[dim] = slice(None)
        idx[order[n]] = c
        return out_ref.at[tuple(idx) + (slice(None), cols)]

    return (GatherDirect(copies, order[0], lambda c: view(0, c, whole), lambda: in_ref.at[:, whole]),
            GatherDirect(copies, order[1], lambda c: view(1, c, whole), lambda: view(1, coord(order[1]), whole)),
            GatherStage(copies, order[2], lambda c, h: view(2, c, halves[h]), lambda h: view(2, coord(order[2]), halves[h])))


ORDERS = ((X, Y, Z), (Y, Z, X), (Z, X, Y))
WQ_GATHER = ((0, (256, L)), (384, (L, 256)), (768, (L, L)))
WO_GATHER = ((0, (L, L)), (256, (L, L)), (512, (L, L)))


def rotate(vals, cos, sin):
    return vals * cos + pltpu.roll(vals, L // 2, 1) * sin


def stack_heads(vals):
    return jnp.concatenate([vals[:, n:n + L] for n in range(0, vals.shape[1], L)], axis=0)


def unstack_heads(vals):
    return jnp.concatenate([vals[n:n + L, :] for n in range(0, vals.shape[0], L)], axis=1)


def dot_nn(a, b):
    return jnp.dot(a, b, preferred_element_type=F32)


def dot_tn(a, b):
    return lax.dot_general(a, b, (((0,), (0,)), ((), ())), preferred_element_type=F32)


def dot_nt(a, b):
    return lax.dot_general(a, b, (((1,), (1,)), ((), ())), preferred_element_type=F32)


def attend(qkv, o, tab_ref, base_ref, sink, dsink, k_buf, v_buf, dk_buf, dv_buf):
    width = o.shape[1]
    heads = width // L
    n_blocks = o.shape[0] // L
    scale = L ** -0.5
    low, high = pl.ds(0, L), pl.ds(L, L)
    k_cols, v_cols = pl.ds(width, L), pl.ds(width + L, L)
    for buf in (k_buf, v_buf, dk_buf, dv_buf, dsink):
        buf[...] = jnp.zeros(buf.shape, buf.dtype)

    def tables(i):
        cos_b, sin_b = base_ref[0, pl.ds(i, 1), :], base_ref[1, pl.ds(i, 1), :]
        cos_r, sin_r = tab_ref[0], tab_ref[1]
        return cos_b * cos_r - sin_b * sin_r, sin_b * cos_r + cos_b * sin_r

    def put_kv(i, dk, dv):
        cos, sin = tables(i)
        at = pl.ds(pl.multiple_of(i * L, L), L)
        qkv[at, k_cols] = rotate(dk.astype(BF16).astype(F32), cos, -sin).astype(BF16)
        qkv[at, v_cols] = dv.astype(BF16)

    @pl.loop(0, n_blocks)
    def _(i):
        for buf in (k_buf, v_buf, dk_buf, dv_buf):
            buf[low, :] = buf[high, :]
        at = pl.ds(pl.multiple_of(i * L, L), L)
        cos, sin = tables(i)
        cos_all = jnp.concatenate([cos] * heads, axis=0)
        sin_all = jnp.concatenate([sin] * heads, axis=0)
        k_buf[high, :] = rotate(qkv[at, k_cols].astype(F32), cos, sin).astype(BF16)
        v_buf[high, :] = qkv[at, v_cols]
        q = rotate(stack_heads(qkv[at, pl.ds(0, width)]).astype(F32), cos_all, sin_all).astype(BF16)
        do = stack_heads(o[at, :])
        keys, vals = k_buf[...], v_buf[...]
        k_idx = lax.broadcasted_iota(jnp.int32, (2 * L, L), 0)
        q_idx = lax.broadcasted_iota(jnp.int32, (2 * L, L), 1)
        allowed = (k_idx > q_idx) & (k_idx <= q_idx + WINDOW) & ((k_idx >= WINDOW) | (i > 0))
        bias = jnp.where(allowed, 0.0, NEG)
        scores = dot_nt(keys, q) * scale + jnp.concatenate([bias] * heads, axis=1)
        top = jnp.maximum(jnp.max(scores, axis=0, keepdims=True), sink)
        probs = jnp.exp(scores - top)
        sink_exp = jnp.exp(sink - top)
        inv = 1.0 / (jnp.sum(probs, axis=0, keepdims=True) + sink_exp)
        probs = probs * inv
        probs_b = probs.astype(BF16)
        o[at, :] = unstack_heads(dot_tn(probs_b, vals).astype(BF16))
        d_probs = dot_nt(vals, do).astype(BF16).astype(F32)
        row_dot = jnp.sum(probs * d_probs, axis=0, keepdims=True)
        d_scores = (probs * (d_probs - row_dot)).astype(BF16)
        dsink[...] = dsink[...] - sink_exp * inv * row_dot
        for buf, new in ((dv_buf, dot_nn(probs_b, do)), (dk_buf, dot_nn(d_scores, q) * scale)):
            buf[low, :] = buf[low, :] + new[0:L, :]
            buf[high, :] = new[L:, :]
        dq = (dot_tn(d_scores, keys) * scale).astype(BF16).astype(F32)
        qkv[at, pl.ds(0, width)] = unstack_heads(rotate(dq, cos_all, -sin_all).astype(BF16))

        @pl.when(i > 0)
        def _():
            put_kv(i - 1, dk_buf[low, :], dv_buf[low, :])

    put_kv(n_blocks - 1, dk_buf[high, :], dv_buf[high, :])


class ScatterStage:
    def __init__(self, copies, dim, blk, buf, put):
        self.c, self.dim, self.blk, self.buf, self.put = copies, dim, blk, buf, put
        self.base = copies.slots(6)
        self.a_up, self.a_down, self.lo = 0, 1, (2, 3)
        self.hi = (4, 5)

    def send(self, src, slot, k):
        self.c.send(src, self.buf.at[slot], self.base + slot, peer(self.dim, k))

    def arrive(self, slot, k):
        self.c.arrive(self.buf.at[slot], self.base + slot, peer(self.dim, k))

    def start(self):
        up, down, far = (shifted(self.dim, k) for k in (UP, DOWN, FAR))
        self.send(self.blk(far, 0), self.a_up, UP)
        self.send(self.blk(far, 1), self.a_down, DOWN)
        self.send(self.blk(up, 1), self.lo[1], UP)
        self.send(self.blk(down, 0), self.hi[0], DOWN)

    def add(self, slot, src):
        dst = self.buf.at[slot]
        if len(src.shape) == 2:
            dst[...] = dst[...] + src[...]
        else:
            @pl.loop(0, src.shape[0])
            def _(j):
                dst[j] = dst[j] + src[j]

    def mid(self):
        self.arrive(self.a_up, DOWN)
        self.add(self.a_up, self.blk(shifted(self.dim, UP), 0))
        self.arrive(self.a_down, UP)
        self.add(self.a_down, self.blk(shifted(self.dim, DOWN), 1))
        self.send(self.buf.at[self.a_up], self.lo[0], UP)
        self.send(self.buf.at[self.a_down], self.hi[1], DOWN)

    def finish(self):
        me = coord(self.dim)
        for h in (1, 0):
            self.arrive(self.lo[h], DOWN)
            self.arrive(self.hi[1 - h], UP)
        for h in (0, 1):
            own, a, b = self.blk(me, h), self.buf.at[self.lo[h]], self.buf.at[self.hi[h]]
            if len(own.shape) == 2:
                self.put(h, None, own[...] + a[...] + b[...])
            else:
                @pl.loop(0, own.shape[0])
                def _(j):
                    self.put(h, j, own[j] + a[j] + b[j])


class DirectStage:
    def __init__(self, copies, dim, blk, buf, put):
        self.c, self.dim, self.blk, self.buf, self.put = copies, dim, blk, buf, put
        self.base = copies.slots(3)

    def start(self):
        for slot, k in enumerate((UP, DOWN, FAR)):
            self.c.send(self.blk(shifted(self.dim, k)), self.buf.at[slot], self.base + slot, peer(self.dim, k))

    def finish(self):
        for slot, k in enumerate((UP, DOWN, FAR)):
            self.c.arrive(self.buf.at[slot], self.base + slot, peer(self.dim, k))
        b = self.buf
        self.put((self.blk(coord(self.dim))[...] + b[0]) + (b[1] + b[2]))


def scatter_stages(copies, src, out, order, first, width, bufs, padded):
    hw = width // 2
    r1, r2, r3, s2, s3 = bufs
    rows = out.shape[0]
    rest = [dim for dim in range(3) if dim != order[0]]

    def pick(ref, at, t, cols):
        idx = [slice(None)] * (len(ref.shape) - 1)
        idx[at] = t
        return ref.at[tuple(idx) + (cols,)]

    def part(h, base=0):
        return pl.ds(base + h * hw, hw)

    def put1(h, j, val):
        s2[j, ..., part(h)] = val

    def put2(h, j, val):
        if padded:
            for t in range(4):
                s3[t, 0:rows, part(h)] = val[rows * t:rows * t + rows, :]
        else:
            s3[j, :, part(h)] = val

    def put3(val):
        out[:, pl.ds(first, width)] = val[0:rows, :]

    return (ScatterStage(copies, order[0], lambda t, h: pick(src, order[0], t, part(h, first)), r1, put1),
            ScatterStage(copies, order[1], lambda t, h: pick(s2, rest.index(order[1]), t, part(h)), r2, put2),
            DirectStage(copies, order[2], lambda t: s3.at[t], r3, put3))


WO_JOBS = (((Y, Z, X), 0, 768), ((Z, Y, X), 768, 768))
WQ_JOBS = (((X, Y, Z), 0, 512), ((Y, Z, X), 512, 256), ((Z, X, Y), 768, 256))


def scatter_scratch():
    out = []
    for jobs, lead, rows, pad in ((WO_JOBS, (4,), 48, 16), (WQ_JOBS, (4, 4), 24, 24)):
        for _, _, width in jobs:
            hw = width // 2
            out += [pltpu.VMEM((6,) + lead + (rows, hw), F32), pltpu.VMEM((6,) + lead[1:] + (rows, hw), F32), pltpu.VMEM((3, pad, width), F32),
                    pltpu.VMEM(lead + (rows, width), F32), pltpu.VMEM((4, pad, width), F32)]
    return out


class SmallSums:
    def __init__(self, copies, ar):
        self.c, self.ar = copies, ar
        self.base = copies.slots(10)

    def start(self, n):
        if n < 3:
            for slot, k in enumerate((UP, DOWN, FAR)):
                ref = self.ar.at[n, coord(n)]
                self.c.send(ref, ref, self.base + 3 * n + slot, peer(n, k))
        else:
            ref = self.ar.at[n, lax.axis_index("tp")]
            self.c.send(ref, ref, self.base + 3 * n, partner())

    def finish(self, n):
        ar = self.ar
        if n < 3:
            for slot, k in enumerate((UP, DOWN, FAR)):
                self.c.arrive(ar.at[n, shifted(n, -k)], self.base + 3 * n + slot, peer(n, k))
            total = (ar[n, 0] + ar[n, 1]) + (ar[n, 2] + ar[n, 3])
            ar[n + 1, coord(n + 1) if n < 2 else lax.axis_index("tp")] = total
        else:
            self.c.arrive(ar.at[n, 1 - lax.axis_index("tp")], self.base + 3 * n, partner())


def layer_kernel(wq_in, wo_in, x_in, x5_in, dy_in, small_in, perm_ref, tab_ref, base_ref,
                 y_out, dx_out, gq_out, go_out, gain_out, gbout_out, bqkv_out, sink_out, *scratch):
    bufs = list(scratch)
    (wq5, wo5, h, dy, qkv, o, wq, wo, wq2, wo2, o2, dqkv2, gq, go, ar, k_buf, v_buf, dk_buf, dv_buf, dsink,
     loc_sem, send_sem, recv_sem) = bufs[:23]
    bufs = bufs[23:]
    tp = lax.axis_index("tp")
    half, d = x_in.shape
    width, cols = o.shape[1], qkv.shape[1]
    start = pl.multiple_of(tp * half, half)
    mine, theirs = pl.ds(start, half), pl.ds((1 - tp) * half, half)
    wide, rest = pl.ds(0, cols), pl.ds(0, d - cols)
    x_low, x_high = qkv.at[pl.ds(0, half), :], qkv.at[pl.ds(half, half), rest]
    local = [pltpu.make_async_copy(a, b, loc_sem.at[n]) for n, (a, b) in enumerate((
        (x_in.at[:, wide], x_low), (x_in.at[:, pl.ds(cols, d - cols)], x_high), (dy_in, dy.at[mine, :])))]
    for copy in local:
        copy.start()
    for ref, own in ((wq5, wq_in), (wo5, wo_in)):
        ref[coord(Z), coord(Y), coord(X)] = own[...]
    entry_barrier([peer(dim, k) for dim in range(3) for k in (UP, DOWN, FAR)] + [partner()])
    copies = Copies(send_sem, recv_sem)
    jobs_q = [gather_stages(copies, wq_in, wq5, order, *job) for order, job in zip(ORDERS, WQ_GATHER)]
    jobs_o = [gather_stages(copies, wo_in, wo5, order, *job) for order, job in zip(ORDERS, WO_GATHER)]

    def each(jobs, n, *names):
        for name in names:
            for job in jobs:
                getattr(job[n], name)()

    each(jobs_q, 0, "start")
    each(jobs_o, 0, "start")
    gain, b_out = small_in[0:1, :], small_in[1:2, :]
    parts = 6
    step = half // parts
    slot_h, slot_dy = copies.slots(parts), copies.slots(5)
    for copy in local:
        copy.wait()
    copies.send(dy.at[mine, :], dy.at[mine, :], slot_dy, partner())

    def norm_part(k):
        @pl.loop(0, step // 32)
        def _(i):
            n = k * step + i * 32
            at = pl.ds(pl.multiple_of(n, 32), 32)
            xv = jnp.concatenate([x_low[at, :], x_high[at, :]], axis=1).astype(F32)
            inv = lax.rsqrt(jnp.mean(xv * xv, axis=-1, keepdims=True) + EPS)
            h[pl.ds(pl.multiple_of(start + n, 32), 32), :] = (xv * inv * gain).astype(BF16)

    def send_part(k):
        at = pl.ds(pl.multiple_of(start + k * step, step), step)
        copies.send(h.at[at, :], h.at[at, :], slot_h + k, partner())

    norm_part(0)
    norm_part(1)
    each(jobs_q, 0, "finish")
    each(jobs_q, 1, "start")
    each(jobs_o, 0, "finish")
    send_part(0)
    send_part(1)
    norm_part(2)
    norm_part(3)
    each(jobs_q, 1, "finish")
    each(jobs_q, 2, "start")
    each(jobs_o, 1, "start")
    send_part(2)
    send_part(3)
    norm_part(4)
    norm_part(5)
    each(jobs_o, 1, "finish")
    send_part(4)
    send_part(5)
    each(jobs_q, 2, "mid")
    each(jobs_o, 2, "start")
    for k in range(parts):
        copies.arrive(h.at[pl.ds((1 - tp) * half + k * step, step), :], slot_h + k, partner())
    copies.arrive(dy.at[theirs, :], slot_dy, partner())
    each(jobs_q, 2, "finish")

    @pl.loop(0, 16)
    def _(n):
        wq[pl.ds(pl.multiple_of(n * 96, 32), 96), :] = wq5[lax.div(n, 4), lax.rem(n, 4)].reshape(96, cols)

    copies.send(wq, wq2, slot_dy + 1, partner())
    bias = small_in[2:3, 0:cols]
    tile = 512

    def qkv_tile(n):
        qkv[pl.ds(n * tile, tile), :] = (dot_nn(h[pl.ds(n * tile, tile), :], wq[...]) + bias).astype(BF16)

    qkv_tile(0)
    qkv_tile(1)
    each(jobs_o, 2, "mid")
    qkv_tile(2)
    each(jobs_o, 2, "finish")

    def slabs(z, pair):
        return wo5[z, pl.ds(pair * 2, 2)].reshape(192, d // 2)

    @pl.loop(0, 8)
    def _(n):
        group = slabs(lax.div(n, 2), lax.rem(n, 2))
        for c in (0, 1):
            wo[pl.ds(pl.multiple_of(n * 96, 32), 96), pl.ds(c * (d // 2), d // 2)] = dot_nn(perm_ref[c], group).astype(BF16)

    @pl.loop(0, 3)
    def _(n):
        at = pl.ds(pl.multiple_of(n * tile, tile), tile)
        o[at, :] = dot_nt(dy[at, :], wo[...]).astype(BF16)

    copies.send(wo, wo2, slot_dy + 2, partner())
    attend(qkv, o, tab_ref, base_ref, small_in[3:4, 0:width], dsink, k_buf, v_buf, dk_buf, dv_buf)
    copies.arrive(wq2, slot_dy + 1, partner())
    copies.arrive(wo2, slot_dy + 2, partner())
    copies.drain()
    copies.send(o.at[theirs, :], o2, slot_dy + 3, partner())
    copies.send(qkv.at[theirs, :], dqkv2, slot_dy + 4, partner())
    loads = [pltpu.make_async_copy(x5_in.at[:, :, :, :, pl.ds(c * (d // 2), d // 2)], wo5.at[pl.ds(c * 2, 2)], loc_sem.at[c]) for c in (0, 1)]
    for copy in loads:
        copy.start()

    small = SmallSums(copies, ar)
    jobs_wo = [scatter_stages(copies, go, go_out, *job, [bufs.pop(0) for _ in range(5)], True) for job in WO_JOBS]
    jobs_wq = [scatter_stages(copies, gq, gq_out, *job, [bufs.pop(0) for _ in range(5)], False) for job in WQ_JOBS]
    own = ar.at[Z, coord(Z)]
    own[...] = jnp.zeros(own.shape, F32)
    for job in jobs_wo:
        s3 = job[2].blk(slice(None))
        s3[...] = jnp.zeros(s3.shape, F32)

    @pl.loop(0, 2)
    def _(m):
        @pl.loop(0, 3)
        def _(n):
            at, to = pl.ds(pl.multiple_of(m * 384, L), 384), pl.ds(pl.multiple_of(n * tile, L), tile)
            go[pl.ds(m * 2, 2), :, :, to] = dot_tn(o[:, at], dy[:, to]).reshape(2, 4, 48, tile)

    each(jobs_wo, 0, "start")

    @pl.loop(0, 4)
    def _(m):
        gq[m] = dot_tn(h[:, pl.ds(pl.multiple_of(m * 384, L), 384)], qkv[...]).reshape(4, 4, 24, cols)

    each(jobs_wq, 0, "start")
    ones = jnp.ones((8, 2 * half), BF16)
    own[2:3, 0:cols] = dot_nn(ones, qkv[...])[0:1]
    own[3:4, 0:width] = dsink[...]
    own[1:2, :] = dot_nn(ones[:, 0:half], dy[mine, :])[0:1]
    for copy in loads:
        copy.wait()
    copies.arrive(o2, slot_dy + 3, partner())
    copies.arrive(dqkv2, slot_dy + 4, partner())
    each(jobs_wo, 0, "mid")
    third = 192

    def x_tile(n):
        return jnp.concatenate([slabs(lax.div(n, 2) + c, lax.rem(n, 2)) for c in (0, 2)], axis=1).astype(F32)

    @pl.loop(0, 4)
    def _(n):
        at = pl.ds(pl.multiple_of(n * third, third), third)
        at_all = pl.ds(pl.multiple_of(start + n * third, third), third)
        acc = dot_nn(o[at_all, :], wo[...]) + dot_nn(o2[at, :], wo2[...])
        h[at, :] = (x_tile(n) + acc + b_out).astype(BF16)

    store_y = pltpu.make_async_copy(h.at[pl.ds(0, half), :], y_out, loc_sem.at[0])
    store_y.start()
    each(jobs_wo, 0, "finish")
    each(jobs_wo, 1, "start")
    each(jobs_wq, 0, "mid")

    @pl.loop(0, 4)
    def _(n):
        at = pl.ds(pl.multiple_of(n * third, third), third)
        at_all = pl.ds(pl.multiple_of(start + n * third, third), third)
        dh = dot_nt(qkv[at_all, :], wq[...]) + dot_nt(dqkv2[at, :], wq2[...])
        dh = dh.astype(BF16).astype(F32)
        xv = x_tile(n)
        inv = lax.rsqrt(jnp.mean(xv * xv, axis=-1, keepdims=True) + EPS)
        gg = dh * gain
        dx = inv * (gg - xv * (inv * inv * jnp.mean(gg * xv, axis=-1, keepdims=True)))
        dy[at_all, :] = (dy[at_all, :].astype(F32) + dx).astype(BF16)
        own[0:1, :] = own[0:1, :] + jnp.sum(dh * (xv * inv), axis=0, keepdims=True)

    store_dx = pltpu.make_async_copy(dy.at[mine, :], dx_out, loc_sem.at[1])
    store_dx.start()
    small.start(0)
    each(jobs_wo, 1, "mid")
    small.finish(0)
    small.start(1)
    each(jobs_wq, 0, "finish")
    each(jobs_wq, 1, "start")
    each(jobs_wo, 1, "finish")
    each(jobs_wo, 2, "start")
    small.finish(1)
    small.start(2)
    each(jobs_wq, 1, "mid")
    small.finish(2)
    small.start(3)
    each(jobs_wo, 2, "finish")
    each(jobs_wq, 1, "finish")
    each(jobs_wq, 2, "start")
    small.finish(3)
    both = ar[3, 0] + ar[3, 1]
    row = ar[3, tp]
    gain_out[...] = both[0]
    gbout_out[...] = both[1]
    bqkv_out[...] = row[2, 0:cols]
    lane = lax.broadcasted_iota(jnp.int32, (1, L), 1)
    sinks = jnp.zeros(lane.shape, F32)
    for n in range(width // L):
        sinks = jnp.where(lane == n, jnp.sum(row[3:4, n * L:n * L + L], axis=1, keepdims=True), sinks)
    sink_out[...] = sinks[0]
    each(jobs_wq, 2, "finish")
    copies.drain()
    store_y.wait()
    store_dx.wait()


VM = pl.BlockSpec(memory_space=pltpu.VMEM)
ANY = pl.BlockSpec(memory_space=pl.ANY)


def layer(wq, wo, x, x5, dy, small, perm, tab, base):
    half, d = x.shape
    cols, width = wq.shape[1], wo.shape[1]
    seq = 2 * half
    n = 11 + 10 + len(ORDERS) * 2 * 12 + len(WO_JOBS + WQ_JOBS) * 15
    sds = jax.ShapeDtypeStruct
    shapes = ((4, 4, 4) + wq.shape, (4, 4, 4) + wo.shape, (seq, d), (seq, d), (seq, cols), (seq, width), (d, cols), (width, d), (d, cols), (width, d), (half, width), (half, cols))
    scratch = [pltpu.VMEM(shape, BF16) for shape in shapes]
    scratch += [pltpu.VMEM((4, 4, 4, 24, cols), F32), pltpu.VMEM((4, 4, 48, d), F32), pltpu.VMEM((4, 4, 4, d), F32)]
    scratch += [pltpu.VMEM((2 * L, L), t) for t in (BF16, BF16, F32, F32)] + [pltpu.VMEM((1, width), F32)]
    scratch += [pltpu.SemaphoreType.DMA((k,)) for k in (3, n, n)]
    return pl.pallas_call(
        layer_kernel, name="layer",
        out_shape=(sds((half, d), BF16), sds((half, d), BF16), sds((24, cols), F32), sds((12, d), F32), sds((d,), F32), sds((d,), F32), sds((cols,), F32), sds((L,), F32)),
        in_specs=[VM, VM, ANY, ANY, ANY] + [VM] * 4, out_specs=(ANY, ANY) + (VM,) * 6, scratch_shapes=scratch + scatter_scratch(),
        compiler_params=pltpu.CompilerParams(collective_id=0, has_side_effects=True, vmem_limit_bytes=VMEM_LIMIT),
    )(wq, wo, x, x5, dy, small, perm, tab, base)


def rope_constants(n_blocks):
    freq = np.tile(ROPE_BASE ** (-2.0 * np.arange(L // 2) / L), 2)
    sign = np.where(np.arange(L) < L // 2, -1.0, 1.0)

    def pair(positions):
        angle = positions[:, None] * freq[None, :]
        return jnp.asarray(np.stack([np.cos(angle), np.sin(angle) * sign]), F32)

    return pair(np.arange(L)), pair(np.arange(n_blocks) * L)


def row_permutation():
    row = np.arange(96)[:, None]
    col = np.arange(192)[None, :]
    return jnp.asarray(np.stack([col == row // 12 * 24 + c * 12 + row % 12 for c in (0, 1)]), BF16)


def solution(mesh):
    act_spec = P("fsdp", "tp", None)
    wout_spec = P(("tp", "fsdp"), None)
    in_specs = (act_spec, act_spec, P(), P("fsdp", "tp"), P("tp"), P("tp"), wout_spec, P())
    out_specs = (act_spec, act_spec, P(), P("fsdp", "tp"), P("tp"), P("tp"), wout_spec, P())

    def device_step(resid_loc, grad_loc, norm_gain, wqkv_loc, bqkv_loc, sink_loc, wout_loc, b_out):
        x, dy = resid_loc[0], grad_loc[0]
        half, d = x.shape
        heads = sink_loc.shape[0]
        wo_slab = jnp.concatenate([wout_loc[:, :d // 2], wout_loc[:, d // 2:]], axis=0)
        rows = (norm_gain, b_out.astype(F32), bqkv_loc.astype(F32), jnp.repeat(sink_loc, L))
        small = jnp.stack([jnp.pad(r, (0, d - r.shape[0])) for r in rows])
        tab, base = rope_constants(2 * half // L)
        y, dx, gq, go, gain_g, bout_g, bqkv_g, sink_g = layer(wqkv_loc, wo_slab, x, x.reshape(2, 4, 4, 24, d), dy, small, row_permutation(), tab, base)
        return (y[None], dx[None], gain_g, gq, bqkv_g, sink_g[:heads], go, bout_g)

    return jax.shard_map(device_step, mesh=mesh, in_specs=in_specs, out_specs=out_specs, check_vma=False)
```

```python
import math

import jax
import jax.numpy as jnp
import numpy as np
from jax import lax
from jax.experimental import pallas as pl
from jax.experimental.pallas import tpu as pltpu
from jax.sharding import PartitionSpec as P

EPS = 1e-5
ROPE_BASE = 150000.0
WINDOW = 128
MESH = pl.DeviceIdType.MESH
STRIDE = (16, 4, 1)
F32 = jnp.float32
BF16 = jnp.bfloat16
VMEM_LIMIT = 67_000_000
Z, Y, X = range(3)
UP, DOWN, FAR = 1, -1, 2
L = 128
PAIR = (0, 1)
RING = (4, 4)
NEG = -1e30


def coord(dim):
    return lax.rem(lax.div(lax.axis_index("fsdp"), STRIDE[dim]), 4)


def shifted(dim, k):
    return lax.rem(coord(dim) + (k + 4), 4)


def peer(dim, k):
    f = lax.axis_index("fsdp")
    return {"fsdp": f + (shifted(dim, k) - coord(dim)) * STRIDE[dim]}


def partner():
    return {"tp": 1 - lax.axis_index("tp")}


def span(n, size, base=0):
    return pl.ds(pl.multiple_of(base + n * size, math.gcd(size, L)), size)


def entry_barrier(peers):
    barrier = pltpu.get_barrier_semaphore()
    for p in peers:
        pl.semaphore_signal(barrier, inc=1, device_id=p, device_id_type=MESH)
    pl.semaphore_wait(barrier, len(peers))


class Copies:
    def __init__(self, send_sem, recv_sem):
        self.send_sem, self.recv_sem = send_sem, recv_sem
        self.n = 0
        self.sent = []

    def slots(self, count):
        first = self.n
        self.n += count
        return first

    def make(self, src, dst, slot, device):
        return pltpu.make_async_remote_copy(src_ref=src, dst_ref=dst, send_sem=self.send_sem.at[slot], recv_sem=self.recv_sem.at[slot], device_id=device, device_id_type=MESH)

    def send(self, src, dst, slot, device):
        copy = self.make(src, dst, slot, device)
        copy.start()
        self.sent.append(copy)

    def arrive(self, ref, slot, device):
        self.make(ref, ref, slot, device).wait_recv()

    def drain(self):
        for copy in self.sent:
            copy.wait_send()
        self.sent = []


class GatherStage:
    def __init__(self, copies, dim, slot_view, own_view):
        self.c, self.dim, self.view, self.own = copies, dim, slot_view, own_view
        self.base = copies.slots(6)

    def start(self):
        me = coord(self.dim)
        for h in PAIR:
            self.c.send(self.own(h), self.view(me, h), self.base + h, peer(self.dim, UP))
            self.c.send(self.own(1 - h), self.view(me, 1 - h), self.base + 3 - h, peer(self.dim, DOWN))

    def sides(self):
        return [(shifted(self.dim, k), peer(self.dim, k)) for k in (DOWN, UP)]

    def mid(self):
        (lo, down), (hi, up) = self.sides()
        self.c.arrive(self.view(lo, 0), self.base, down)
        self.c.send(self.view(lo, 0), self.view(lo, 0), self.base + 4, up)
        self.c.arrive(self.view(hi, 1), self.base + 3, up)
        self.c.send(self.view(hi, 1), self.view(hi, 1), self.base + 5, down)

    def finish(self):
        (lo, down), (hi, up) = self.sides()
        far = shifted(self.dim, FAR)
        for n, (at, h, dev) in enumerate(((lo, 1, down), (hi, 0, up))):
            self.c.arrive(self.view(at, h), self.base + 1 + n, dev)
            self.c.arrive(self.view(far, n), self.base + 4 + n, dev)


class GatherDirect:
    def __init__(self, copies, dim, view, own):
        self.c, self.dim, self.view, self.own = copies, dim, view, own
        self.base = copies.slots(3)

    def start(self):
        for slot, k in enumerate((UP, DOWN, FAR)):
            self.c.send(self.own(), self.view(coord(self.dim)), self.base + slot, peer(self.dim, k))

    def finish(self):
        for slot, k in enumerate((UP, DOWN, FAR)):
            self.c.arrive(self.view(shifted(self.dim, -k)), self.base + slot, peer(self.dim, k))


def gather_stages(copies, in_ref, out_ref, order, first, widths):
    whole = pl.ds(first, sum(widths))
    halves = [pl.ds(first, widths[0]), pl.ds(first + widths[0], widths[1])]

    def view(n, c, cols):
        idx = [coord(dim) for dim in (Z, Y, X)]
        for dim in order[:n]:
            idx[dim] = slice(None)
        idx[order[n]] = c
        return out_ref.at[tuple(idx) + (slice(None), cols)]

    return (GatherDirect(copies, order[0], lambda c: view(0, c, whole), lambda: in_ref.at[:, whole]),
            GatherDirect(copies, order[1], lambda c: view(1, c, whole), lambda: view(1, coord(order[1]), whole)),
            GatherStage(copies, order[2], lambda c, h: view(2, c, halves[h]), lambda h: view(2, coord(order[2]), halves[h])))


ORDERS = ((X, Y, Z), (Y, Z, X), (Z, X, Y))
WQ_GATHER = ((0, (256, L)), (384, (L, 256)), (768, (L, L)))
WO_GATHER = ((0, (L, L)), (256, (L, L)), (512, (L, L)))


def rotate(vals, cos, sin):
    return vals * cos + pltpu.roll(vals, L // 2, 1) * sin


def stack_heads(vals):
    return jnp.concatenate([vals[:, n:n + L] for n in range(0, vals.shape[1], L)], axis=0)


def unstack_heads(vals):
    return jnp.concatenate([vals[n:n + L, :] for n in range(0, vals.shape[0], L)], axis=1)


def dot_nn(a, b):
    return jnp.dot(a, b, preferred_element_type=F32)


def dot_tn(a, b):
    return lax.dot_general(a, b, (((0,), (0,)), ((), ())), preferred_element_type=F32)


def dot_nt(a, b):
    return lax.dot_general(a, b, (((1,), (1,)), ((), ())), preferred_element_type=F32)


class Attention:
    def __init__(self, qkv, o, d_o, tab, base, sink_ref, dsink, keys, vals, dk, dv, top, inv, bias):
        self.qkv, self.o, self.d_o, self.tab, self.base, self.dsink = qkv, o, d_o, tab, base, dsink
        self.keys, self.vals, self.dk, self.dv, self.top, self.inv, self.bias = keys, vals, dk, dv, top, inv, bias
        self.width = o.shape[1]
        self.blocks = o.shape[0] // L
        self.scale = L ** -0.5
        self.sink = jnp.concatenate([jnp.full((1, L), sink_ref[n], F32) for n in range(self.width // L)], axis=1)

    def prepare(self):
        for ref in (self.keys, self.vals, self.dk, self.dv):
            ref[pl.ds(0, L), :] = jnp.zeros((L, L), ref.dtype)
        self.dsink[...] = jnp.zeros(self.dsink.shape, F32)
        k_idx = lax.broadcasted_iota(jnp.int32, (2 * L, L), 0)
        q_idx = lax.broadcasted_iota(jnp.int32, (2 * L, L), 1)
        allowed = (k_idx > q_idx) & (k_idx <= q_idx + WINDOW)
        self.bias[1] = jnp.where(allowed, 0.0, NEG).astype(BF16)
        self.bias[0] = jnp.where(allowed & (k_idx >= WINDOW), 0.0, NEG).astype(BF16)

    def tables(self, i):
        cos_b, sin_b = self.base[0, pl.ds(i, 1), :], self.base[1, pl.ds(i, 1), :]
        cos_r, sin_r = self.tab[0], self.tab[1]
        return cos_b * cos_r - sin_b * sin_r, sin_b * cos_r + cos_b * sin_r

    def scores(self, i, keys, q, heads):
        bias = self.bias[jnp.minimum(i, 1)].astype(F32)
        return dot_nt(keys, q) * self.scale + jnp.concatenate([bias] * heads, axis=1)

    def forward(self, first, last):
        heads = self.width // L

        @pl.loop(first, last)
        def _(i):
            at, nxt = (span(i + n, L) for n in PAIR)
            cos, sin = self.tables(i)
            cos_all, sin_all = jnp.concatenate([cos] * heads, axis=0), jnp.concatenate([sin] * heads, axis=0)
            self.keys[nxt, :] = rotate(self.qkv[at, pl.ds(self.width, L)].astype(F32), cos, sin).astype(BF16)
            self.vals[nxt, :] = self.qkv[at, pl.ds(self.width + L, L)]
            for ref in (self.dk, self.dv):
                ref[nxt, :] = jnp.zeros((L, L), F32)
            q = rotate(stack_heads(self.qkv[at, pl.ds(0, self.width)]).astype(F32), cos_all, sin_all).astype(BF16)
            self.qkv[at, pl.ds(0, self.width)] = unstack_heads(q)
            pair = pl.ds(pl.multiple_of(i * L, L), 2 * L)
            scores = self.scores(i, self.keys[pair, :], q, heads)
            top = jnp.maximum(jnp.max(scores, axis=0, keepdims=True), self.sink)
            probs = jnp.exp(scores - top)
            inv = 1.0 / (jnp.sum(probs, axis=0, keepdims=True) + jnp.exp(self.sink - top))
            self.top[pl.ds(i, 1), :] = top
            self.inv[pl.ds(i, 1), :] = inv
            self.o[at, :] = unstack_heads(dot_tn((probs * inv).astype(BF16), self.vals[pair, :]).astype(BF16))

    def backward(self, g, first, last):
        heads = GROUP // L
        here = span(g, GROUP)
        sink = self.sink[:, g * GROUP:(g + 1) * GROUP]

        @pl.loop(first // TRIPLE, last // TRIPLE)
        def _(m):
            d_o = self.d_o[m, :, :, :, here].reshape(TRIPLE * L, GROUP)
            loads = []
            for n in range(TRIPLE):
                i = m * TRIPLE + n
                pair = pl.ds(pl.multiple_of(i * L, L), 2 * L)
                loads.append((i, stack_heads(self.qkv[span(i, L), here]), stack_heads(d_o[n * L:(n + 1) * L]), self.keys[pair, :], self.vals[pair, :],
                              self.top[pl.ds(i, 1), here], self.inv[pl.ds(i, 1), here], self.tables(i)))
            wide = [[jnp.concatenate([t] * heads, axis=0) for t in load[-1]] for load in loads]
            scores = [self.scores(i, keys, q, heads) for i, q, _, keys, *_ in loads]
            d_probs = [dot_nt(load[4], load[2]) for load in loads]
            probs = [jnp.exp(sc - load[5]) * load[6] for sc, load in zip(scores, loads)]
            d_probs = [dp.astype(BF16).astype(F32) for dp in d_probs]
            dvs = [dot_nn(p.astype(BF16), load[2]) for p, load in zip(probs, loads)]
            row_dots = [jnp.sum(p * dp, axis=0, keepdims=True) for p, dp in zip(probs, d_probs)]
            d_scores = [(p * (dp - rd)).astype(BF16) for p, dp, rd in zip(probs, d_probs, row_dots)]
            d_sink = self.dsink[:, here]
            for rd, load in zip(row_dots, loads):
                d_sink = d_sink - jnp.exp(sink - load[5]) * load[6] * rd
            dqs = [(dot_tn(ds, load[3]) * self.scale).astype(BF16).astype(F32) for ds, load in zip(d_scores, loads)]
            dks = [dot_nn(ds, load[1]) * self.scale for ds, load in zip(d_scores, loads)]
            stores = [unstack_heads(rotate(dq, cos, -sin).astype(BF16)) for dq, (cos, sin) in zip(dqs, wide)]
            self.dsink[:, here] = d_sink
            self.qkv[span(m, TRIPLE * L), here] = jnp.concatenate(stores, axis=0)
            rows = pl.ds(pl.multiple_of(m * TRIPLE * L, L), (TRIPLE + 1) * L)
            for ref, new in ((self.dv, dvs), (self.dk, dks)):
                parts = [new[0][:L]] + [p[L:] + q[:L] for p, q in zip(new, new[1:])] + [new[-1][L:]]
                ref[rows, :] = ref[rows, :] + jnp.concatenate(parts, axis=0)

    def backward_kv(self):
        @pl.loop(0, self.blocks)
        def _(i):
            at, nxt = (span(i + n, L) for n in PAIR)
            cos, sin = self.tables(i)
            self.qkv[at, pl.ds(self.width, L)] = rotate(self.dk[nxt, :].astype(BF16).astype(F32), cos, -sin).astype(BF16)
            self.qkv[at, pl.ds(self.width + L, L)] = self.dv[nxt, :].astype(BF16)


class ScatterStage:
    def __init__(self, copies, dim, blk, buf, put):
        self.c, self.dim, self.blk, self.buf, self.put = copies, dim, blk, buf, put
        self.base = copies.slots(6)
        self.a_up, self.a_down, self.lo = 0, 1, (2, 3)
        self.hi = (4, 5)

    def send(self, src, slot, k):
        self.c.send(src, self.buf.at[slot], self.base + slot, peer(self.dim, k))

    def arrive(self, slot, k):
        self.c.arrive(self.buf.at[slot], self.base + slot, peer(self.dim, k))

    def start(self):
        up, down, far = (shifted(self.dim, k) for k in (UP, DOWN, FAR))
        self.send(self.blk(far, 0), self.a_up, UP)
        self.send(self.blk(far, 1), self.a_down, DOWN)
        self.send(self.blk(up, 1), self.lo[1], UP)
        self.send(self.blk(down, 0), self.hi[0], DOWN)

    def add(self, slot, src):
        dst = self.buf.at[slot]
        if len(src.shape) == 2:
            dst[...] = dst[...] + src[...]
        else:
            @pl.loop(0, src.shape[0])
            def _(j):
                dst[j] = dst[j] + src[j]

    def mid(self):
        self.arrive(self.a_up, DOWN)
        self.add(self.a_up, self.blk(shifted(self.dim, UP), 0))
        self.arrive(self.a_down, UP)
        self.add(self.a_down, self.blk(shifted(self.dim, DOWN), 1))
        self.send(self.buf.at[self.a_up], self.lo[0], UP)
        self.send(self.buf.at[self.a_down], self.hi[1], DOWN)

    def finish(self):
        me = coord(self.dim)
        for h in (1, 0):
            self.arrive(self.lo[h], DOWN)
            self.arrive(self.hi[1 - h], UP)
        for h in PAIR:
            own, a, b = self.blk(me, h), self.buf.at[self.lo[h]], self.buf.at[self.hi[h]]
            if len(own.shape) == 2:
                self.put(h, None, own[...] + a[...] + b[...])
            else:
                @pl.loop(0, own.shape[0])
                def _(j):
                    self.put(h, j, own[j] + a[j] + b[j])


class DirectStage:
    def __init__(self, copies, dim, blk, buf, put):
        self.c, self.dim, self.blk, self.buf, self.put = copies, dim, blk, buf, put
        self.base = copies.slots(3)

    def start(self):
        for slot, k in enumerate((UP, DOWN, FAR)):
            self.c.send(self.blk(shifted(self.dim, k)), self.buf.at[slot], self.base + slot, peer(self.dim, k))

    def finish(self):
        for slot, k in enumerate((UP, DOWN, FAR)):
            self.c.arrive(self.buf.at[slot], self.base + slot, peer(self.dim, k))
        b = self.buf
        self.put((self.blk(coord(self.dim))[...] + b[0]) + (b[1] + b[2]))


def scatter_steps(copies, src, out, order, first, width, bufs, padded):
    r1, r2, r3, s2, s3 = bufs
    rows = out.shape[0]
    rest = [dim for dim in (Z, Y, X) if dim != order[0]]

    def pick(ref, at, t, h, cols):
        idx = [slice(None)] * (len(ref.shape) - 1)
        cut = 1 if at == 0 else 0
        half = ref.shape[cut] // 2
        idx[at], idx[cut] = t, pl.ds(h * half, half)
        return ref.at[tuple(idx) + (cols,)]

    def put1(h, j, val):
        s2[h * 2 + j] = val

    def put2(h, j, val):
        if padded:
            for t in PAIR:
                s3[h * 2 + t, 0:rows, :] = val[rows * t:rows * t + rows, :]
        else:
            s3[h * 2 + j] = val

    def put3(val):
        out[:, pl.ds(first, width)] = val[0:rows, :]

    one = ScatterStage(copies, order[0], lambda t, h: pick(src, order[0], t, h, pl.ds(first, width)), r1, put1)
    two = ScatterStage(copies, order[1], lambda t, h: pick(s2, rest.index(order[1]), t, h, slice(None)), r2, put2)
    three = DirectStage(copies, order[2], lambda t: s3.at[t], r3, put3)
    return iter(((one.start,), (one.mid,), (one.finish, two.start), (two.mid,), (two.finish, three.start), (three.finish,)))


def advance(*groups):
    for jobs in groups:
        for job in jobs:
            for step in next(job):
                step()


WO_JOBS = (((Y, Z, X), 0, 768), ((Z, Y, X), 768, 768))
GROUP = 2 * L
TRIPLE = 3
WQ_JOBS = tuple((order, first * L, size) for order, first, size in zip(ORDERS * 2, (0, 2, 3, 4, 6, 7), (GROUP, L, L) * 2))


def scatter_scratch():
    out = []
    for jobs, lead, rows, pad in ((WO_JOBS, (), 48, 16), (WQ_JOBS, (4,), 24, 24)):
        for _, _, width in jobs:
            half = (2, rows, width) if lead else (rows // 2, width)
            out += [pltpu.VMEM((6, 2) + lead + (rows, width), F32), pltpu.VMEM((6,) + half, F32), pltpu.VMEM((3, pad, width), F32),
                    pltpu.VMEM((4,) + lead + (rows, width), F32), pltpu.VMEM((4, pad, width), F32)]
    return out


class SmallSums:
    def __init__(self, copies, ar):
        self.c, self.ar = copies, ar
        self.base = copies.slots(10)

    def start(self, n):
        if n < 3:
            for slot, k in enumerate((UP, DOWN, FAR)):
                ref = self.ar.at[n, coord(n)]
                self.c.send(ref, ref, self.base + 3 * n + slot, peer(n, k))
        else:
            ref = self.ar.at[n, lax.axis_index("tp")]
            self.c.send(ref, ref, self.base + 3 * n, partner())

    def finish(self, n):
        ar = self.ar
        if n < 3:
            for slot, k in enumerate((UP, DOWN, FAR)):
                self.c.arrive(ar.at[n, shifted(n, -k)], self.base + 3 * n + slot, peer(n, k))
            total = (ar[n, 0] + ar[n, 1]) + (ar[n, 2] + ar[n, 3])
            ar[n + 1, coord(n + 1) if n < 2 else lax.axis_index("tp")] = total
        else:
            self.c.arrive(ar.at[n, 1 - lax.axis_index("tp")], self.base + 3 * n, partner())


def layer_kernel(wq_in, wo_in, x_in, x5_in, dy_in, gain_ref, bout_ref, bqkv_ref, sink_ref, perm_ref, tab_ref, base_ref,
                 y_out, dx_out, gq_out, go_out, gain_out, gbout_out, bqkv_out, sink_out, wo2_hbm, *scratch):
    bufs = list(scratch)
    (wq5, wo5, h, dy, qkv, o, wq, wo, wq2, o2, dqkv2, gq, go, ar, keys, vals, dk, dv, dsink, top, inv, bias, gain_sum,
     loc_sem, send_sem, recv_sem) = bufs[:26]
    bufs = bufs[26:]
    tp = lax.axis_index("tp")
    half, d = x_in.shape
    width, cols = o.shape[1], qkv.shape[1]
    start = tp * half
    mine, theirs = span(tp, half), span(1 - tp, half)
    wide, rest = pl.ds(0, cols), pl.ds(0, d - cols)
    x_low, x_high = qkv.at[pl.ds(0, half), :], qkv.at[pl.ds(half, half), rest]
    local = [pltpu.make_async_copy(a, b, loc_sem.at[n]) for n, (a, b) in enumerate((
        (x_in.at[:, wide], x_low), (x_in.at[:, pl.ds(cols, d - cols)], x_high), (dy_in, dy.at[mine, :])))]
    for copy in local:
        copy.start()
    for ref, own in ((wq5, wq_in), (wo5, wo_in)):
        ref[coord(Z), coord(Y), coord(X)] = own[...]
    entry_barrier([peer(dim, k) for dim in (Z, Y, X) for k in (UP, DOWN, FAR)] + [partner()])
    copies = Copies(send_sem, recv_sem)
    jobs_q = [gather_stages(copies, wq_in, wq5, order, *job) for order, job in zip(ORDERS, WQ_GATHER)]
    jobs_o = [gather_stages(copies, wo_in, wo5, order, *job) for order, job in zip(ORDERS, WO_GATHER)]

    def each(jobs, n, *names):
        for name in names:
            for job in jobs:
                getattr(job[n], name)()

    each(jobs_q, 0, "start")
    each(jobs_o, 0, "start")
    gain, b_out = gain_ref[...][None, :], bout_ref[...].astype(F32)[None, :]
    parts = 3
    step = half // parts
    slot_h = copies.slots(parts)
    slot_dy, slot_wq, slot_wo, slot_o, slot_dqkv = (copies.slots(n) for n in (1, 1, 1, 1, 3))
    att = Attention(qkv, o, wq5, tab_ref, base_ref, sink_ref, dsink, keys, vals, dk, dv, top, inv, bias)
    att.prepare()
    for copy in local:
        copy.wait()
    copies.send(dy.at[mine, :], dy.at[mine, :], slot_dy, partner())

    pieces = iter(range(parts))

    def norm_piece():
        k = next(pieces)
        first = k * step

        @pl.loop(0, step // 32)
        def _(i):
            at = span(i, 32, first)
            xv = jnp.concatenate([x_low[at, :], x_high[at, :]], axis=1).astype(F32)
            inv = lax.rsqrt(jnp.mean(xv * xv, axis=-1, keepdims=True) + EPS)
            h[span(i, 32, start + first), :] = (xv * inv * gain).astype(BF16)

        return k

    def send_piece(k):
        at = span(k, step, start)
        copies.send(h.at[at, :], h.at[at, :], slot_h + k, partner())

    ready = norm_piece()
    each(jobs_q, 0, "finish")
    each(jobs_q, 1, "start")
    each(jobs_o, 0, "finish")
    send_piece(ready)
    ready = norm_piece()
    each(jobs_q, 1, "finish")
    each(jobs_q, 2, "start")
    send_piece(ready)
    send_piece(norm_piece())
    each(jobs_q, 2, "mid")
    each(jobs_o, 1, "start")
    for k in range(parts):
        copies.arrive(h.at[span(k, step, (1 - tp) * half), :], slot_h + k, partner())
    copies.arrive(dy.at[theirs, :], slot_dy, partner())
    each(jobs_q, 2, "finish")

    @pl.loop(0, 16)
    def _(n):
        wq[span(n, 96), :] = wq5[lax.div(n, 4), lax.rem(n, 4)].reshape(96, cols)

    b_qkv = bqkv_ref[...].astype(F32)[None, :]
    tile = 384

    def qkv_tile(n):
        qkv[span(n, tile), :] = (dot_nn(h[span(n, tile), :], wq[...]) + b_qkv).astype(BF16)

    qkv_tile(0)
    copies.send(wq, wq2, slot_wq, partner())
    each(jobs_o, 1, "finish")
    each(jobs_o, 2, "start")
    for n in range(1, 4):
        qkv_tile(n)
    att.forward(0, att.blocks // 2)
    each(jobs_o, 2, "mid")
    att.forward(att.blocks // 2, att.blocks)
    copies.send(o.at[theirs, :], o2, slot_o, partner())
    each(jobs_o, 2, "finish")

    def slabs(z, pair):
        return wo5[z, pl.ds(pair * 2, 2)].reshape(192, d // 2)

    @pl.loop(0, 8)
    def _(n):
        group = slabs(lax.div(n, 2), lax.rem(n, 2))
        for c in PAIR:
            wo[span(n, 96), span(c, d // 2)] = dot_nn(perm_ref[c], group).astype(BF16)

    copies.send(wo, wo2_hbm, slot_wo, partner())
    scatters = []
    for jobs, src, out, padded in ((WO_JOBS, go, go_out, True), (WQ_JOBS, gq, gq_out, False)):
        for job in jobs:
            five, bufs = bufs[:5], bufs[5:]
            if padded:
                five[4][...] = jnp.zeros(five[4].shape, F32)
            scatters.append(scatter_steps(copies, src, out, *job, five, padded))
    s_wo, s_0, s_1, s_2 = scatters[:2], scatters[2:3], scatters[3:5], scatters[5:]

    @pl.loop(0, 2)
    def _(m):
        @pl.loop(0, 3)
        def _(n):
            at, to = span(m, tile), span(n, 2 * GROUP)
            go[pl.ds(m * 2, 2), :, :, to] = dot_tn(o[:, at], dy[:, to]).reshape(2, 4, 48, 2 * GROUP)

    copies.drain()
    advance(s_wo)
    @pl.loop(0, 4)
    def _(n):
        at = span(n, tile)
        wq5[n, :, :, :, pl.ds(0, width)] = dot_nt(dy[at, :], wo[...]).astype(BF16).reshape(*RING, 24, width)


    def done(g):
        return pl.ds(g * GROUP, GROUP if g < 2 else 2 * GROUP)

    def wq_grad(to):

        @pl.loop(0, 4)
        def _(m):
            gq[m, :, :, :, to] = dot_tn(h[:, span(m, tile)], qkv[:, to]).reshape(*RING, 24, to.size)

    early = 9
    plan = ((s_0, (s_wo,), ()), (s_1, (), (s_0,)), (s_2, (s_wo,), (s_0,)))
    for g, (jobs, during, after) in enumerate(plan):
        att.backward(g, 0, early)
        advance(*during)
        att.backward(g, early, att.blocks)
        if g == 2:
            att.backward_kv()
        copies.send(qkv.at[theirs, done(g)], dqkv2.at[:, done(g)], slot_dqkv + g, partner())
        if jobs is s_2:
            advance(s_1)
        wq_grad(done(g))
        advance(jobs)
        advance(*after)
    own = ar.at[Z, coord(Z)]
    own[...] = jnp.zeros(own.shape, F32)
    small = SmallSums(copies, ar)
    ones = jnp.ones((8, 2 * half), BF16)
    own[2:3, 0:cols] = dot_nn(ones, qkv[...])[0:1]
    own[3:4, 0:width] = dsink[...]
    own[1:2, :] = dot_nn(ones[:, 0:half], dy[mine, :])[0:1]
    loads = [pltpu.make_async_copy(x5_in.at[:, :, :, :, span(c, d // 2)], wo5.at[pl.ds(c * 2, 2)], loc_sem.at[c]) for c in PAIR]
    wo2 = h.at[pl.ds(0, half), :]
    loads.append(pltpu.make_async_copy(wo2_hbm, wo2, loc_sem.at[2]))
    for ref, slot in ((wo2_hbm, slot_wo), (wq2, slot_wq), (o2, slot_o)):
        copies.arrive(ref, slot, partner())
    for copy in loads:
        copy.start()
    for g in range(3):
        copies.arrive(dqkv2.at[:, done(g)], slot_dqkv + g, partner())
    wide_half = d // 2

    def dh_tiles(c):
        to = span(c, wide_half)

        @pl.loop(0, 2)
        def _(n):
            h[span(n, tile, half), to] = (dot_nt(qkv[span(n, tile, start), :], wq[to, :]) + dot_nt(dqkv2[span(n, tile), :], wq2[to, :])).astype(BF16)

    dh_tiles(0)
    advance(s_wo, s_0)
    dh_tiles(1)
    for copy in loads:
        copy.wait()
    advance(s_1, s_2)
    rows = 48
    gain_sum[...] = jnp.zeros(gain_sum.shape, F32)

    def norm_back(c):
        count = half // rows // 2

        @pl.loop(c * count, c * count + count)
        def _(n):
            at = span(n, rows, start)
            z, yy, pair = lax.div(n, 8), lax.rem(lax.div(n, 2), 4), pl.ds(lax.rem(n, 2) * 2, 2)
            xv = jnp.concatenate([wo5[z + c, yy, pair].reshape(rows, d // 2) for c in (0, 2)], axis=1).astype(F32)
            dh = h[span(n, rows, half), :].astype(F32)
            inv = lax.rsqrt(jnp.mean(xv * xv, axis=-1, keepdims=True) + EPS)
            xn, gg = xv * inv, dh * gain
            dx = inv * (gg - xn * jnp.mean(gg * xn, axis=-1, keepdims=True))
            dy[at, :] = (dy[at, :].astype(F32) + dx).astype(BF16)
            gain_sum[...] = gain_sum[...] + jnp.sum((dh * xn).reshape(rows // 8, 8, d), axis=0)

    norm_back(0)
    advance(s_wo, s_0, s_1)
    norm_back(1)
    own[0:1, :] = jnp.sum(gain_sum[...], axis=0, keepdims=True)
    store_dx = pltpu.make_async_copy(dy.at[mine, :], dx_out, loc_sem.at[1])
    store_dx.start()
    small.start(0)
    advance(s_0, s_2)
    def y_tiles(c):
        to = span(c, wide_half)

        @pl.loop(0, 2)
        def _(n):
            at = span(n, tile)
            xv = wo5[n + 2 * c].reshape(tile, wide_half).astype(F32)
            acc = dot_nn(o[span(n, tile, start), :], wo[:, to]) + dot_nn(o2[at, :], wo2[:, to])
            dy[span(n, tile, (1 - tp) * half), to] = (xv + acc + b_out[:, c * wide_half:(c + 1) * wide_half]).astype(BF16)

    y_tiles(0)
    small.finish(0)
    small.start(1)
    advance(s_1)
    y_tiles(1)
    store_y = pltpu.make_async_copy(dy.at[theirs, :], y_out, loc_sem.at[0])
    store_y.start()
    small.finish(1)
    small.start(2)
    advance(s_2)
    small.finish(2)
    small.start(3)
    advance(s_wo, s_1)
    advance(s_2)
    small.finish(3)
    advance(s_2)
    both = ar[3, 0] + ar[3, 1]
    row = ar[3, tp]
    gain_out[...] = both[0]
    gbout_out[...] = both[1]
    bqkv_out[...] = row[2, 0:cols]
    lane = lax.broadcasted_iota(jnp.int32, (1, L), 1)
    sinks = jnp.zeros(lane.shape, F32)
    for n in range(width // L):
        sinks = jnp.where(lane == n, jnp.sum(row[3:4, n * L:n * L + L], axis=1, keepdims=True), sinks)
    sink_out[...] = sinks[0]
    for jobs in (s_wo, s_0, s_1, s_2):
        for job in jobs:
            assert next(job, None) is None
    copies.drain()
    store_y.wait()
    store_dx.wait()


VM = pl.BlockSpec(memory_space=pltpu.VMEM)
ANY = pl.BlockSpec(memory_space=pl.ANY)


def layer(wq, wo, x, x5, dy, gain, b_out, b_qkv, sinks, perm, tab, base):
    half, d = x.shape
    cols, width = wq.shape[1], wo.shape[1]
    seq = 2 * half
    n = 10 + 10 + len(ORDERS) * 2 * 12 + len(WO_JOBS + WQ_JOBS) * 15
    sds = jax.ShapeDtypeStruct
    shapes = ((4,) + RING + wq.shape, (4,) + RING + wo.shape, (seq, d), (seq, d), (seq, cols), (seq, width), (d, cols), (width, d), (d, cols), (half, width), (half, cols))
    scratch = [pltpu.VMEM(shape, BF16) for shape in shapes]
    scratch += [pltpu.VMEM((4, *RING, 24, cols), F32), pltpu.VMEM((*RING, 48, d), F32), pltpu.VMEM((4, *RING, d), F32)]
    scratch += [pltpu.VMEM((seq + L, L), t) for t in (BF16, BF16, F32, F32)] + [pltpu.VMEM((1, width), F32)]
    scratch += [pltpu.VMEM((seq // L, width), F32)] * 2 + [pltpu.VMEM((2, 2 * L, L), BF16), pltpu.VMEM((8, d), F32)]
    scratch += [pltpu.SemaphoreType.DMA((k,)) for k in (3, n, n)]
    outs = (sds((half, d), BF16), sds((half, d), BF16), sds((24, cols), F32), sds((12, d), F32), sds((d,), F32), sds((d,), F32), sds((cols,), F32), sds((L,), F32))
    results = pl.pallas_call(
        layer_kernel, name="layer", out_shape=outs + (sds((width, d), BF16),),
        in_specs=[VM, VM, ANY, ANY, ANY, VM, VM, VM, pl.BlockSpec(memory_space=pltpu.SMEM)] + [VM] * 3, out_specs=(ANY, ANY) + (VM,) * 6 + (ANY,), scratch_shapes=scratch + scatter_scratch(),
        compiler_params=pltpu.CompilerParams(collective_id=0, has_side_effects=True, vmem_limit_bytes=VMEM_LIMIT),
    )(wq, wo, x, x5, dy, gain, b_out, b_qkv, sinks, perm, tab, base)
    return pl.pallas_call(
        hand_over, name="hand_over", out_shape=outs, in_specs=[ANY, ANY] + [VM] * 6, out_specs=(ANY, ANY) + (VM,) * 6,
        scratch_shapes=[pltpu.VMEM((2, half, d), BF16), pltpu.SemaphoreType.DMA((2, 3)), pltpu.SemaphoreType.DMA((2, 3))],
    )(*results[:-1])


def hand_over(*refs):
    ins, outs = refs[:8], refs[8:16]
    buf, in_sem, out_sem = refs[16:]
    parts = in_sem.shape[1]
    step = buf.shape[1] // parts
    copies = []
    for n in range(parts):
        at = pl.ds(n * step, step)
        for c in PAIR:
            copies.append((pltpu.make_async_copy(ins[c].at[at, :], buf.at[c, at, :], in_sem.at[c, n]), pltpu.make_async_copy(buf.at[c, at, :], outs[c].at[at, :], out_sem.at[c, n])))
    for load, _ in copies:
        load.start()
    for a, b in zip(ins[2:], outs[2:]):
        b[...] = a[...]
    for load, store in copies:
        load.wait()
        store.start()
    for _, store in copies:
        store.wait()


def rope_constants(n_blocks):
    freq = np.tile(ROPE_BASE ** (-2.0 * np.arange(L // 2) / L), 2)
    sign = np.where(np.arange(L) < L // 2, -1.0, 1.0)

    def pair(positions):
        angle = positions[:, None] * freq[None, :]
        return jnp.asarray(np.stack([np.cos(angle), np.sin(angle) * sign]), F32)

    return pair(np.arange(L)), pair(np.arange(n_blocks) * L)


def row_permutation():
    row = np.arange(96)[:, None]
    col = np.arange(192)[None, :]
    return jnp.asarray(np.stack([col == row // 12 * 24 + c * 12 + row % 12 for c in PAIR]), BF16)


def solution(mesh):
    act_spec = P("fsdp", "tp", None)
    wout_spec = P(("tp", "fsdp"), None)
    in_specs = (act_spec, act_spec, P(), P("fsdp", "tp"), P("tp"), P("tp"), wout_spec, P())
    out_specs = (act_spec, act_spec, P(), P("fsdp", "tp"), P("tp"), P("tp"), wout_spec, P())

    def device_step(resid_loc, grad_loc, norm_gain, wqkv_loc, bqkv_loc, sink_loc, wout_loc, b_out):
        x, dy = resid_loc[0], grad_loc[0]
        half, d = x.shape
        heads = sink_loc.shape[0]
        wo_slab = jnp.concatenate([wout_loc[:, :d // 2], wout_loc[:, d // 2:]], axis=0)
        tab, base = rope_constants(2 * half // L)
        y, dx, gq, go, gain_g, bout_g, bqkv_g, sink_g = layer(wqkv_loc, wo_slab, x, x.reshape(2, *RING, 24, d), dy, norm_gain, b_out, bqkv_loc, sink_loc, row_permutation(), tab, base)
        return (y[None], dx[None], gain_g, gq, bqkv_g, sink_g[:heads], go, bout_g)

    return jax.shard_map(device_step, mesh=mesh, in_specs=in_specs, out_specs=out_specs, check_vma=False)
```

```python
import math

import jax
import jax.numpy as jnp
import numpy as np
from jax import lax
from jax.experimental import pallas as pl
from jax.experimental.pallas import tpu as pltpu
from jax.sharding import PartitionSpec as P

EPS = 1e-5
ROPE_BASE = 150000.0
WINDOW = 128
MESH = pl.DeviceIdType.MESH
STRIDE = (16, 4, 1)
F32 = jnp.float32
BF16 = jnp.bfloat16
VMEM_LIMIT = 67_000_000
Z, Y, X = range(3)
UP, DOWN, FAR = 1, -1, 2
L = 128
PAIR = (0, 1)
RING = (4, 4)
GROUP = 2 * L
TRIPLE = 3
NEG = -1e30


def coord(dim):
    return lax.rem(lax.div(lax.axis_index("fsdp"), STRIDE[dim]), 4)


def shifted(dim, k):
    return lax.rem(coord(dim) + (k + 4), 4)


def peer(dim, k):
    f = lax.axis_index("fsdp")
    return {"fsdp": f + (shifted(dim, k) - coord(dim)) * STRIDE[dim]}


def partner():
    return {"tp": 1 - lax.axis_index("tp")}


def span(n, size, base=0):
    return pl.ds(pl.multiple_of(base + n * size, math.gcd(size, L)), size)


def entry_barrier(peers):
    barrier = pltpu.get_barrier_semaphore()
    for p in peers:
        pl.semaphore_signal(barrier, inc=1, device_id=p, device_id_type=MESH)
    pl.semaphore_wait(barrier, len(peers))


class Copies:
    def __init__(self, send_sem, recv_sem):
        self.send_sem, self.recv_sem = send_sem, recv_sem
        self.n = 0
        self.sent = []

    def slots(self, count):
        first = self.n
        self.n += count
        return first

    def make(self, src, dst, slot, device):
        send = len(self.sent) % self.send_sem.shape[0]
        return pltpu.make_async_remote_copy(src_ref=src, dst_ref=dst, send_sem=self.send_sem.at[send], recv_sem=self.recv_sem.at[slot], device_id=device, device_id_type=MESH)

    def send(self, src, dst, slot, device):
        copy = self.make(src, dst, slot, device)
        copy.start()
        assert len(self.sent) < self.send_sem.shape[0]
        self.sent.append(copy)

    def arrive(self, ref, slot, device):
        self.make(ref, ref, slot, device).wait_recv()

    def drain(self):
        for copy in self.sent:
            copy.wait_send()
        self.sent = []


class GatherStage:
    def __init__(self, copies, dim, slot_view, own_view):
        self.c, self.dim, self.view, self.own = copies, dim, slot_view, own_view
        self.base = copies.slots(6)

    def start(self):
        me = coord(self.dim)
        for h in PAIR:
            self.c.send(self.own(h), self.view(me, h), self.base + h, peer(self.dim, UP))
            self.c.send(self.own(1 - h), self.view(me, 1 - h), self.base + 3 - h, peer(self.dim, DOWN))

    def sides(self):
        return [(shifted(self.dim, k), peer(self.dim, k)) for k in (DOWN, UP)]

    def mid(self):
        (lo, down), (hi, up) = self.sides()
        self.c.arrive(self.view(lo, 0), self.base, down)
        self.c.send(self.view(lo, 0), self.view(lo, 0), self.base + 4, up)
        self.c.arrive(self.view(hi, 1), self.base + 3, up)
        self.c.send(self.view(hi, 1), self.view(hi, 1), self.base + 5, down)

    def finish(self):
        (lo, down), (hi, up) = self.sides()
        far = shifted(self.dim, FAR)
        for n, (at, h, dev) in enumerate(((lo, 1, down), (hi, 0, up))):
            self.c.arrive(self.view(at, h), self.base + 1 + n, dev)
            self.c.arrive(self.view(far, n), self.base + 4 + n, dev)


class GatherDirect:
    def __init__(self, copies, dim, view, own):
        self.c, self.dim, self.view, self.own = copies, dim, view, own
        self.base = copies.slots(3)

    def start(self):
        for slot, k in enumerate((UP, DOWN, FAR)):
            self.c.send(self.own(), self.view(coord(self.dim)), self.base + slot, peer(self.dim, k))

    def finish(self):
        for slot, k in enumerate((UP, DOWN, FAR)):
            self.c.arrive(self.view(shifted(self.dim, -k)), self.base + slot, peer(self.dim, k))


def gather_stages(copies, in_ref, out_ref, order, first, size):
    rows = pl.ds(first, size)

    def view(n, c, h=None):
        idx = [coord(dim) for dim in (Z, Y, X)]
        for dim in order[:n]:
            idx[dim] = slice(None)
        idx[order[n]] = c
        if h is not None:
            cut = min(order[:n])
            idx[cut] = pl.ds(h * 2, 2)
        return out_ref.at[tuple(idx) + (rows,)]

    return (GatherDirect(copies, order[0], lambda c: view(0, c), lambda: in_ref.at[rows]),
            GatherDirect(copies, order[1], lambda c: view(1, c), lambda: view(1, coord(order[1]))),
            GatherStage(copies, order[2], lambda c, h: view(2, c, h), lambda h: view(2, coord(order[2]), h)))


ORDERS = ((X, Y, Z), (Y, Z, X), (Z, X, Y))


def rotate(vals, cos, sin):
    return vals * cos + pltpu.roll(vals, L // 2, 1) * sin


def stack_heads(vals):
    return jnp.concatenate([vals[:, n:n + L] for n in range(0, vals.shape[1], L)], axis=0)


def unstack_heads(vals):
    return jnp.concatenate([vals[n:n + L, :] for n in range(0, vals.shape[0], L)], axis=1)


def dot_nn(a, b):
    return jnp.dot(a, b, preferred_element_type=F32)


def dot_tn(a, b):
    return lax.dot_general(a, b, (((0,), (0,)), ((), ())), preferred_element_type=F32)


def dot_nt(a, b):
    return lax.dot_general(a, b, (((1,), (1,)), ((), ())), preferred_element_type=F32)


class Attention:
    def __init__(self, qkv, o, d_o, tab, base, sink_ref, dsink, keys, vals, dk, dv, top, inv, bias):
        self.qkv, self.o, self.d_o, self.tab, self.base, self.dsink = qkv, o, d_o, tab, base, dsink
        self.keys, self.vals, self.dk, self.dv, self.top, self.inv, self.bias = keys, vals, dk, dv, top, inv, bias
        self.width = o.shape[1]
        self.blocks = o.shape[0] // L
        self.scale = L ** -0.5
        self.sink = jnp.concatenate([jnp.full((1, L), sink_ref[n], F32) for n in range(self.width // L)], axis=1)

    def prepare(self):
        for ref in (self.keys, self.vals, self.dk, self.dv):
            ref[pl.ds(0, L), :] = jnp.zeros((L, L), ref.dtype)
        self.dsink[...] = jnp.zeros(self.dsink.shape, F32)
        k_idx = lax.broadcasted_iota(jnp.int32, (GROUP, L), 0)
        q_idx = lax.broadcasted_iota(jnp.int32, (GROUP, L), 1)
        allowed = (k_idx > q_idx) & (k_idx <= q_idx + WINDOW)
        self.bias[1] = jnp.where(allowed, 0.0, NEG).astype(BF16)
        self.bias[0] = jnp.where(allowed & (k_idx >= WINDOW), 0.0, NEG).astype(BF16)

    def tables(self, i):
        cos_b, sin_b = self.base[0, pl.ds(i, 1), :], self.base[1, pl.ds(i, 1), :]
        cos_r, sin_r = self.tab[0], self.tab[1]
        return cos_b * cos_r - sin_b * sin_r, sin_b * cos_r + cos_b * sin_r

    def scores(self, i, keys, q, heads):
        bias = self.bias[jnp.minimum(i, 1)].astype(F32)
        return dot_nt(keys, q) * self.scale + jnp.concatenate([bias] * heads, axis=1)

    def forward(self, first, last):
        heads = self.width // L

        @pl.loop(first // len(PAIR), last // len(PAIR))
        def _(m):
            at = span(m, GROUP)
            blocks = [m * len(PAIR) + n for n in PAIR]
            tables = [self.tables(i) for i in blocks]
            cos, sin = (jnp.concatenate(t, axis=0) for t in zip(*tables))
            new = pl.ds(pl.multiple_of(m * GROUP + L, L), GROUP)
            self.keys[new, :] = rotate(self.qkv[at, pl.ds(self.width, L)].astype(F32), cos, sin).astype(BF16)
            self.vals[new, :] = self.qkv[at, pl.ds(self.width + L, L)]
            for ref in (self.dk, self.dv):
                ref[new, :] = jnp.zeros((GROUP, L), F32)
            seen = pl.ds(pl.multiple_of(m * GROUP, L), TRIPLE * L)
            all_keys, all_vals = self.keys[seen, :], self.vals[seen, :]
            keys, vals = ([t[n * L:n * L + GROUP] for n in PAIR] for t in (all_keys, all_vals))
            raw = [stack_heads(self.qkv[span(i, L), pl.ds(0, self.width)]) for i in blocks]
            wide = [[jnp.concatenate([t] * heads, axis=0) for t in pair] for pair in tables]
            queries = [rotate(q.astype(F32), *w).astype(BF16) for q, w in zip(raw, wide)]
            scores = [self.scores(i, k, q, heads) for i, k, q in zip(blocks, keys, queries)]
            tops = [jnp.maximum(jnp.max(sc, axis=0, keepdims=True), self.sink) for sc in scores]
            probs = [jnp.exp(sc - top) for sc, top in zip(scores, tops)]
            invs = [1.0 / (jnp.sum(p, axis=0, keepdims=True) + jnp.exp(self.sink - top)) for p, top in zip(probs, tops)]
            outs = [dot_tn((p * inv).astype(BF16), v) for p, inv, v in zip(probs, invs, vals)]
            for ref, parts in ((self.o, outs), (self.qkv, queries)):
                ref[at, pl.ds(0, self.width)] = jnp.concatenate([unstack_heads(p.astype(BF16)) for p in parts], axis=0)
            for i, top, inv in zip(blocks, tops, invs):
                self.top[pl.ds(i, 1), :] = top
                self.inv[pl.ds(i, 1), :] = inv

    def backward(self, g, first, last):
        heads = GROUP // L
        here = span(g, GROUP)
        sink = self.sink[:, g * GROUP:(g + 1) * GROUP]

        @pl.loop(first // TRIPLE, last // TRIPLE)
        def _(m):
            d_o = self.d_o[m, :, :, :, here].reshape(TRIPLE * L, GROUP)
            loads = []
            for n in range(TRIPLE):
                i = m * TRIPLE + n
                pair = pl.ds(pl.multiple_of(i * L, L), GROUP)
                loads.append((i, stack_heads(self.qkv[span(i, L), here]), stack_heads(d_o[n * L:(n + 1) * L]), self.keys[pair, :], self.vals[pair, :],
                              self.top[pl.ds(i, 1), here], self.inv[pl.ds(i, 1), here], self.tables(i)))
            wide = [[jnp.concatenate([t] * heads, axis=0) for t in load[-1]] for load in loads]
            scores = [self.scores(i, keys, q, heads) for i, q, _, keys, *_ in loads]
            d_probs = [dot_nt(load[4], load[2]) for load in loads]
            probs = [jnp.exp(sc - load[5]) * load[6] for sc, load in zip(scores, loads)]
            d_probs = [dp.astype(BF16).astype(F32) for dp in d_probs]
            dvs = [dot_nn(p.astype(BF16), load[2]) for p, load in zip(probs, loads)]
            row_dots = [jnp.sum(p * dp, axis=0, keepdims=True) for p, dp in zip(probs, d_probs)]
            d_scores = [(p * (dp - rd)).astype(BF16) for p, dp, rd in zip(probs, d_probs, row_dots)]
            d_sink = self.dsink[:, here]
            for rd, load in zip(row_dots, loads):
                d_sink = d_sink - jnp.exp(sink - load[5]) * load[6] * rd
            dqs = [(dot_tn(ds, load[3]) * self.scale).astype(BF16).astype(F32) for ds, load in zip(d_scores, loads)]
            dks = [dot_nn(ds, load[1]) * self.scale for ds, load in zip(d_scores, loads)]
            stores = [unstack_heads(rotate(dq, cos, -sin).astype(BF16)) for dq, (cos, sin) in zip(dqs, wide)]
            self.dsink[:, here] = d_sink
            self.qkv[span(m, TRIPLE * L), here] = jnp.concatenate(stores, axis=0)
            rows = pl.ds(pl.multiple_of(m * TRIPLE * L, L), (TRIPLE + 1) * L)
            for ref, new in ((self.dv, dvs), (self.dk, dks)):
                parts = [new[0][:L]] + [p[L:] + q[:L] for p, q in zip(new, new[1:])] + [new[-1][L:]]
                ref[rows, :] = ref[rows, :] + jnp.concatenate(parts, axis=0)

    def backward_kv(self):
        @pl.loop(0, self.blocks)
        def _(i):
            at, nxt = (span(i + n, L) for n in PAIR)
            cos, sin = self.tables(i)
            self.qkv[at, pl.ds(self.width, L)] = rotate(self.dk[nxt, :].astype(BF16).astype(F32), cos, -sin).astype(BF16)
            self.qkv[at, pl.ds(self.width + L, L)] = self.dv[nxt, :].astype(BF16)


class ScatterStage:
    def __init__(self, copies, dim, blk, buf, put):
        self.c, self.dim, self.blk, self.buf, self.put = copies, dim, blk, buf, put
        self.base = copies.slots(6)
        self.a_up, self.a_down, self.lo = 0, 1, (2, 3)
        self.hi = (4, 5)

    def send(self, src, slot, k):
        self.c.send(src, self.buf.at[slot], self.base + slot, peer(self.dim, k))

    def arrive(self, slot, k):
        self.c.arrive(self.buf.at[slot], self.base + slot, peer(self.dim, k))

    def start(self):
        up, down, far = (shifted(self.dim, k) for k in (UP, DOWN, FAR))
        self.send(self.blk(far, 0), self.a_up, UP)
        self.send(self.blk(far, 1), self.a_down, DOWN)
        self.send(self.blk(up, 1), self.lo[1], UP)
        self.send(self.blk(down, 0), self.hi[0], DOWN)

    def add(self, slot, src):
        dst = self.buf.at[slot]
        if len(src.shape) == 2:
            dst[...] = dst[...] + src[...]
        else:
            @pl.loop(0, src.shape[0])
            def _(j):
                dst[j] = dst[j] + src[j]

    def mid(self):
        self.arrive(self.a_up, DOWN)
        self.add(self.a_up, self.blk(shifted(self.dim, UP), 0))
        self.arrive(self.a_down, UP)
        self.add(self.a_down, self.blk(shifted(self.dim, DOWN), 1))
        self.send(self.buf.at[self.a_up], self.lo[0], UP)
        self.send(self.buf.at[self.a_down], self.hi[1], DOWN)

    def finish(self):
        me = coord(self.dim)
        for h in (1, 0):
            self.arrive(self.lo[h], DOWN)
            self.arrive(self.hi[1 - h], UP)
        for h in PAIR:
            own, a, b = self.blk(me, h), self.buf.at[self.lo[h]], self.buf.at[self.hi[h]]
            if len(own.shape) == 2:
                self.put(h, None, own[...] + a[...] + b[...])
            else:
                @pl.loop(0, own.shape[0])
                def _(j):
                    self.put(h, j, own[j] + a[j] + b[j])


class DirectStage:
    def __init__(self, copies, dim, blk, buf, put):
        self.c, self.dim, self.blk, self.buf, self.put = copies, dim, blk, buf, put
        self.base = copies.slots(3)

    def start(self):
        for slot, k in enumerate((UP, DOWN, FAR)):
            self.c.send(self.blk(shifted(self.dim, k)), self.buf.at[slot], self.base + slot, peer(self.dim, k))

    def finish(self):
        for slot, k in enumerate((UP, DOWN, FAR)):
            self.c.arrive(self.buf.at[slot], self.base + slot, peer(self.dim, k))
        b = self.buf
        self.put((self.blk(coord(self.dim))[...] + b[0]) + (b[1] + b[2]))


def scatter_steps(copies, src, out, order, first, width, bufs, padded):
    r1, r2, r3, s2, s3 = bufs
    rows = out.shape[0]
    rest = [dim for dim in (Z, Y, X) if dim != order[0]]

    def pick(ref, at, t, h, cols):
        idx = [slice(None)] * (len(ref.shape) - 1)
        cut = 1 if at == 0 else 0
        half = ref.shape[cut] // 2
        idx[at], idx[cut] = t, pl.ds(h * half, half)
        return ref.at[tuple(idx) + (cols,)]

    def put1(h, j, val):
        s2[h * 2 + j] = val

    def put2(h, j, val):
        for t in PAIR:
            s3[h * 2 + t, 0:rows, :] = val[rows * t:rows * t + rows, :]

    def put_slabs(val):
        s3[...] = val

    def put3(val):
        out[:, pl.ds(first, width)] = val[0:rows, :]

    one = ScatterStage(copies, order[0], lambda t, h: pick(src, order[0], t, h, pl.ds(first, width)), r1, put1)
    three = DirectStage(copies, order[2], lambda t: s3.at[t], r3, put3)
    if padded:
        two = ScatterStage(copies, order[1], lambda t, h: pick(s2, rest.index(order[1]), t, h, slice(None)), r2, put2)
        return iter(((one.start,), (one.mid,), (one.finish, two.start), (two.mid,), (two.finish, three.start), (three.finish,)))
    side = rest.index(order[1])
    two = DirectStage(copies, order[1], lambda t: s2.at[(slice(None),) * side + (t,)], r2, put_slabs)
    return iter(((one.start,), (one.mid,), (one.finish, two.start), (two.finish, three.start), (three.finish,)))


def advance(*groups):
    for jobs in groups:
        for job in jobs:
            for step in next(job):
                step()


WO_JOBS = (((Y, Z, X), 0, 768), ((Z, Y, X), 768, 768))
WQ_JOBS = tuple((order, first * L, size) for order, first, size in zip(ORDERS * 2, (0, 2, 3, 4, 6, 7), (GROUP, L, L) * 2))


def scatter_scratch():
    out = []
    for jobs, lead, rows, pad in ((WO_JOBS, (), 48, 16), (WQ_JOBS, (4,), 24, 24)):
        for _, _, width in jobs:
            second = (3, 4, rows, width) if lead else (6, rows // 2, width)
            out += [pltpu.VMEM((6, 2) + lead + (rows, width), F32), pltpu.VMEM(second, F32), pltpu.VMEM((3, pad, width), F32),
                    pltpu.VMEM((4,) + lead + (rows, width), F32), pltpu.VMEM((4, pad, width), F32)]
    return out


class SmallSums:
    def __init__(self, copies, ar):
        self.c, self.ar = copies, ar
        self.base = copies.slots(10)

    def start(self, n):
        if n < 3:
            for slot, k in enumerate((UP, DOWN, FAR)):
                ref = self.ar.at[n, coord(n)]
                self.c.send(ref, ref, self.base + 3 * n + slot, peer(n, k))
        else:
            ref = self.ar.at[n, lax.axis_index("tp")]
            self.c.send(ref, ref, self.base + 3 * n, partner())

    def finish(self, n):
        ar = self.ar
        if n < 3:
            for slot, k in enumerate((UP, DOWN, FAR)):
                self.c.arrive(ar.at[n, shifted(n, -k)], self.base + 3 * n + slot, peer(n, k))
            total = (ar[n, 0] + ar[n, 1]) + (ar[n, 2] + ar[n, 3])
            ar[n + 1, coord(n + 1) if n < 2 else lax.axis_index("tp")] = total
        else:
            self.c.arrive(ar.at[n, 1 - lax.axis_index("tp")], self.base + 3 * n, partner())


def layer_kernel(wq_in, wo_in, x_in, x5_in, dy_in, gain_ref, bout_ref, bqkv_ref, sink_ref, perm_ref, tab_ref, base_ref,
                 y_out, dx_out, *outs_and_scratch):
    hbm_outs, wo2_hbm, bufs = outs_and_scratch[:6], outs_and_scratch[6], list(outs_and_scratch[7:])
    (wq5, wo5, h, dy, qkv, o, wq, wo, wq2, o2, dqkv2, gq, go, ar, keys, vals, dk, dv, dsink, top, inv, bias, gain_sum,
     gq_out, go_out, gain_out, gbout_out, bqkv_out, sink_out, loc_sem, send_sem, recv_sem) = bufs[:32]
    bufs = bufs[32:]
    tp = lax.axis_index("tp")
    half, d = x_in.shape
    width, cols = o.shape[1], qkv.shape[1]
    start = tp * half
    mine, theirs = span(tp, half), span(1 - tp, half)
    wide, rest = pl.ds(0, cols), pl.ds(0, d - cols)
    x_low, x_high = qkv.at[pl.ds(0, half), :], qkv.at[pl.ds(half, half), rest]
    local = [pltpu.make_async_copy(a, b, loc_sem.at[n]) for n, (a, b) in enumerate((
        (x_in.at[:, wide], x_low), (x_in.at[:, pl.ds(cols, d - cols)], x_high), (dy_in, dy.at[mine, :])))]
    for copy in local:
        copy.start()
    for ref, own in ((wq5, wq_in), (wo5, wo_in)):
        ref[coord(Z), coord(Y), coord(X)] = own[...]
    entry_barrier([peer(dim, k) for dim in (Z, Y, X) for k in (UP, DOWN, FAR)] + [partner()])
    copies = Copies(send_sem, recv_sem)
    jobs_q, jobs_o = ([gather_stages(copies, a, b, order, 8 * n, 8) for n, order in enumerate(ORDERS)] for a, b in ((wq_in, wq5), (wo_in, wo5)))

    def each(jobs, n, *names):
        for name in names:
            for job in jobs:
                getattr(job[n], name)()

    each(jobs_q, 0, "start")
    each(jobs_o, 0, "start")
    gain, b_out = gain_ref[...][None, :], bout_ref[...].astype(F32)[None, :]
    parts = 3
    step = half // parts
    slot_h = copies.slots(parts)
    slot_dy, slot_wq, slot_wo, slot_o, slot_dqkv = (copies.slots(n) for n in (1, 1, 1, 1, 3))
    att = Attention(qkv, o, wq5, tab_ref, base_ref, sink_ref, dsink, keys, vals, dk, dv, top, inv, bias)
    att.prepare()
    for copy in local:
        copy.wait()
    copies.send(dy.at[mine, :], dy.at[mine, :], slot_dy, partner())

    pieces = iter(range(parts))

    def norm_piece():
        k = next(pieces)
        first = k * step

        @pl.loop(0, step // 32)
        def _(i):
            at = span(i, 32, first)
            xv = jnp.concatenate([x_low[at, :], x_high[at, :]], axis=1).astype(F32)
            inv = lax.rsqrt(jnp.mean(xv * xv, axis=-1, keepdims=True) + EPS)
            h[span(i, 32, start + first), :] = (xv * inv * gain).astype(BF16)

        return k

    def send_piece(k):
        at = span(k, step, start)
        copies.send(h.at[at, :], h.at[at, :], slot_h + k, partner())

    ready = norm_piece()
    each(jobs_q, 0, "finish")
    each(jobs_q, 1, "start")
    each(jobs_o, 0, "finish")
    send_piece(ready)
    ready = norm_piece()
    each(jobs_q, 1, "finish")
    each(jobs_q, 2, "start")
    send_piece(ready)
    send_piece(norm_piece())
    each(jobs_q, 2, "mid")
    each(jobs_o, 1, "start")
    for k in range(parts):
        copies.arrive(h.at[span(k, step, (1 - tp) * half), :], slot_h + k, partner())
    copies.arrive(dy.at[theirs, :], slot_dy, partner())
    each(jobs_q, 2, "finish")

    @pl.loop(0, 16)
    def _(n):
        wq[span(n, 96), :] = wq5[lax.div(n, 4), lax.rem(n, 4)].reshape(96, cols)

    b_qkv = bqkv_ref[...].astype(F32)[None, :]
    tile = 384

    def qkv_tile(n):
        qkv[span(n, tile), :] = (dot_nn(h[span(n, tile), :], wq[...]) + b_qkv).astype(BF16)

    qkv_tile(0)
    copies.send(wq, wq2, slot_wq, partner())
    each(jobs_o, 1, "finish")
    each(jobs_o, 2, "start")
    for n in range(1, 4):
        qkv_tile(n)
    att.forward(0, att.blocks // 2)
    each(jobs_o, 2, "mid")
    att.forward(att.blocks // 2, att.blocks)
    copies.send(o.at[theirs, :], o2, slot_o, partner())
    each(jobs_o, 2, "finish")

    def slabs(z, pair):
        return wo5[z, pl.ds(pair * 2, 2)].reshape(192, d // 2)

    @pl.loop(0, 8)
    def _(n):
        group = slabs(lax.div(n, 2), lax.rem(n, 2))
        for c in PAIR:
            wo[span(n, 96), span(c, d // 2)] = dot_nn(perm_ref[c], group).astype(BF16)

    copies.send(wo, wo2_hbm, slot_wo, partner())
    scatters = []
    for jobs, src, out, padded in ((WO_JOBS, go, go_out, True), (WQ_JOBS, gq, gq_out, False)):
        for job in jobs:
            five, bufs = bufs[:5], bufs[5:]
            if padded:
                five[4][...] = jnp.zeros(five[4].shape, F32)
            scatters.append(scatter_steps(copies, src, out, *job, five, padded))
    s_wo, s_0, s_1, s_2 = scatters[:2], scatters[2:3], scatters[3:5], scatters[5:]

    @pl.loop(0, 2)
    def _(m):
        @pl.loop(0, 3)
        def _(n):
            at, to = span(m, tile), span(n, 2 * GROUP)
            go[pl.ds(m * 2, 2), :, :, to] = dot_tn(o[:, at], dy[:, to]).reshape(2, 4, 48, 2 * GROUP)

    copies.drain()
    advance(s_wo)
    @pl.loop(0, 4)
    def _(n):
        at = span(n, tile)
        wq5[n, :, :, :, pl.ds(0, width)] = dot_nt(dy[at, :], wo[...]).astype(BF16).reshape(*RING, 24, width)


    def done(g):
        return pl.ds(g * GROUP, GROUP if g < 2 else 2 * GROUP)

    def wq_grad(to):

        @pl.loop(0, 4)
        def _(m):
            gq[m, :, :, :, to] = dot_tn(h[:, span(m, tile)], qkv[:, to]).reshape(*RING, 24, to.size)

    early = 9
    plan = ((s_0, (s_wo,), ()), (s_1, (), (s_0,)), (s_2, (s_wo,), (s_0,)))
    for g, (jobs, during, after) in enumerate(plan):
        att.backward(g, 0, early)
        advance(*during)
        att.backward(g, early, att.blocks)
        if g == 2:
            att.backward_kv()
        copies.send(qkv.at[theirs, done(g)], dqkv2.at[:, done(g)], slot_dqkv + g, partner())
        if jobs is s_2:
            advance(s_1)
        wq_grad(done(g))
        advance(*after, jobs)
    own = ar.at[Z, coord(Z)]
    own[...] = jnp.zeros(own.shape, F32)
    small = SmallSums(copies, ar)
    ones = jnp.ones((8, 2 * half), BF16)
    own[2:3, 0:cols] = dot_nn(ones, qkv[...])[0:1]
    own[3:4, 0:width] = dsink[...]
    own[1:2, :] = dot_nn(ones[:, 0:half], dy[mine, :])[0:1]
    loads = [pltpu.make_async_copy(x5_in.at[:, :, :, :, span(c, d // 2)], wo5.at[pl.ds(c * 2, 2)], loc_sem.at[c]) for c in PAIR]
    wo2 = h.at[pl.ds(0, half), :]
    loads.append(pltpu.make_async_copy(wo2_hbm, wo2, loc_sem.at[2]))
    for ref, slot in ((wo2_hbm, slot_wo), (wq2, slot_wq), (o2, slot_o)):
        copies.arrive(ref, slot, partner())
    for copy in loads:
        copy.start()
    for g in range(3):
        copies.arrive(dqkv2.at[:, done(g)], slot_dqkv + g, partner())
    wide_half = d // 2

    def dh_tiles(c):
        to = span(c, wide_half)

        @pl.loop(0, 2)
        def _(n):
            h[span(n, tile, half), to] = (dot_nt(qkv[span(n, tile, start), :], wq[to, :]) + dot_nt(dqkv2[span(n, tile), :], wq2[to, :])).astype(BF16)

    dh_tiles(0)
    advance(s_wo)
    dh_tiles(1)
    for copy in loads:
        copy.wait()
    advance(s_1, s_0, s_2)
    rows = 48
    gain_sum[...] = jnp.zeros(gain_sum.shape, F32)

    def norm_back(c):
        count = half // rows // 2

        @pl.loop(c * count, c * count + count)
        def _(n):
            at = span(n, rows, start)
            z, yy, pair = lax.div(n, 8), lax.rem(lax.div(n, 2), 4), pl.ds(lax.rem(n, 2) * 2, 2)
            xv = jnp.concatenate([wo5[z + c, yy, pair].reshape(rows, d // 2) for c in (0, 2)], axis=1).astype(F32)
            dh = h[span(n, rows, half), :].astype(F32)
            inv = lax.rsqrt(jnp.mean(xv * xv, axis=-1, keepdims=True) + EPS)
            xn, gg = xv * inv, dh * gain
            dx = inv * (gg - xn * jnp.mean(gg * xn, axis=-1, keepdims=True))
            dy[at, :] = (dy[at, :].astype(F32) + dx).astype(BF16)
            gain_sum[...] = gain_sum[...] + jnp.sum((dh * xn).reshape(rows // 8, 8, d), axis=0)

    norm_back(0)
    advance(s_wo)
    norm_back(1)
    own[0:1, :] = jnp.sum(gain_sum[...], axis=0, keepdims=True)
    store_dx = pltpu.make_async_copy(dy.at[mine, :], dx_out, loc_sem.at[7])
    store_dx.start()
    small.start(0)
    advance(s_0, s_1)
    def y_tiles(c):
        to = span(c, wide_half)

        @pl.loop(0, 2)
        def _(n):
            at = span(n, tile)
            xv = wo5[n + 2 * c].reshape(tile, wide_half).astype(F32)
            acc = dot_nn(o[span(n, tile, start), :], wo[:, to]) + dot_nn(o2[at, :], wo2[:, to])
            dy[span(n, tile, (1 - tp) * half), to] = (xv + acc + b_out[:, c * wide_half:(c + 1) * wide_half]).astype(BF16)

    y_tiles(0)
    small.finish(0)
    small.start(1)
    advance(s_2)
    y_tiles(1)
    store_y = pltpu.make_async_copy(dy.at[theirs, :], y_out, loc_sem.at[6])
    store_y.start()
    small.finish(1)
    small.start(2)
    advance(s_2, s_1)
    small.finish(2)
    small.start(3)
    advance(s_wo)
    small.finish(3)
    advance(s_2)
    both = ar[3, 0] + ar[3, 1]
    row = ar[3, tp]
    gain_out[...] = both[0]
    gbout_out[...] = both[1]
    bqkv_out[...] = row[2, 0:cols]
    lane = lax.broadcasted_iota(jnp.int32, (1, L), 1)
    sinks = jnp.zeros(lane.shape, F32)
    for n in range(width // L):
        sinks = jnp.where(lane == n, jnp.sum(row[3:4, n * L:n * L + L], axis=1, keepdims=True), sinks)
    sink_out[...] = sinks[0]
    stores = [pltpu.make_async_copy(a, b, loc_sem.at[n]) for n, (a, b) in enumerate(zip((gq_out, go_out, gain_out, gbout_out, bqkv_out, sink_out), hbm_outs))]
    for copy in stores[1:]:
        copy.start()
    for jobs in (s_wo, s_0, s_1, s_2):
        for job in jobs:
            assert next(job, None) is None
    copies.drain()
    stores[0].start()
    for copy in stores + [store_y, store_dx]:
        copy.wait()


VM = pl.BlockSpec(memory_space=pltpu.VMEM)
ANY = pl.BlockSpec(memory_space=pl.ANY)


def layer(wq, wo, x, x5, dy, gain, b_out, b_qkv, sinks, perm, tab, base):
    half, d = x.shape
    cols, width = wq.shape[1], wo.shape[1]
    seq = 2 * half
    n = 10 + 10 + len(ORDERS + ORDERS + WQ_JOBS) * 12 + len(WO_JOBS) * 15
    sds = jax.ShapeDtypeStruct
    shapes = ((4,) + RING + wq.shape, (4,) + RING + wo.shape, (seq, d), (seq, d), (seq, cols), (seq, width), (d, cols), (width, d), (d, cols), (half, width), (half, cols))
    scratch = [pltpu.VMEM(shape, BF16) for shape in shapes]
    scratch += [pltpu.VMEM((4, *RING, 24, cols), F32), pltpu.VMEM((*RING, 48, d), F32), pltpu.VMEM((4, *RING, d), F32)]
    scratch += [pltpu.VMEM((seq + L, L), t) for t in (BF16, BF16, F32, F32)] + [pltpu.VMEM((1, width), F32)]
    scratch += [pltpu.VMEM((seq // L, width), F32)] * 2 + [pltpu.VMEM((2, GROUP, L), BF16), pltpu.VMEM((8, d), F32)]
    outs = (sds((half, d), BF16), sds((half, d), BF16), sds((24, cols), F32), sds((12, d), F32), sds((d,), F32), sds((d,), F32), sds((cols,), F32), sds((L,), F32))
    scratch += [pltpu.VMEM(o.shape, F32) for o in outs[2:]] + [pltpu.SemaphoreType.DMA((k,)) for k in (8, n * 3 // 5, n)]
    results = pl.pallas_call(
        layer_kernel, name="layer", out_shape=outs + (sds((width, d), BF16),),
        in_specs=[VM, VM, ANY, ANY, ANY, VM, VM, VM, pl.BlockSpec(memory_space=pltpu.SMEM)] + [VM] * 3, out_specs=(ANY,) * 9, scratch_shapes=scratch + scatter_scratch(),
        compiler_params=pltpu.CompilerParams(collective_id=0, has_side_effects=True, vmem_limit_bytes=VMEM_LIMIT),
    )(wq, wo, x, x5, dy, gain, b_out, b_qkv, sinks, perm, tab, base)
    return pl.pallas_call(
        hand_over, name="hand_over", out_shape=outs, in_specs=[ANY] * 8, out_specs=(ANY,) * 8,
        scratch_shapes=[pltpu.VMEM(o.shape, o.dtype) for o in outs] + [pltpu.SemaphoreType.DMA((8, 4))] * 2,
    )(*results[:-1])


def hand_over(*refs):
    ins, outs, bufs = refs[:8], refs[8:16], refs[16:24]
    in_sem, out_sem = refs[24:]
    copies = []
    for k, (a, buf, b) in enumerate(zip(ins, bufs, outs)):
        parts = in_sem.shape[1] if k < 2 else 1
        step = a.shape[0] // parts
        for n in range(parts):
            at = pl.ds(n * step, step)
            copies.append((pltpu.make_async_copy(a.at[at], buf.at[at], in_sem.at[k, n]), pltpu.make_async_copy(buf.at[at], b.at[at], out_sem.at[k, n])))
    for load, _ in copies:
        load.start()
    for load, store in copies:
        load.wait()
        store.start()
    for _, store in copies:
        store.wait()


def rope_constants(n_blocks):
    freq = np.tile(ROPE_BASE ** (-2.0 * np.arange(L // 2) / L), 2)
    sign = np.where(np.arange(L) < L // 2, -1.0, 1.0)

    def pair(positions):
        angle = positions[:, None] * freq[None, :]
        return jnp.asarray(np.stack([np.cos(angle), np.sin(angle) * sign]), F32)

    return pair(np.arange(L)), pair(np.arange(n_blocks) * L)


def row_permutation():
    row = np.arange(96)[:, None]
    col = np.arange(192)[None, :]
    return jnp.asarray(np.stack([col == row // 12 * 24 + c * 12 + row % 12 for c in PAIR]), BF16)


def solution(mesh):
    act_spec = P("fsdp", "tp", None)
    wout_spec = P(("tp", "fsdp"), None)
    in_specs = (act_spec, act_spec, P(), P("fsdp", "tp"), P("tp"), P("tp"), wout_spec, P())
    out_specs = (act_spec, act_spec, P(), P("fsdp", "tp"), P("tp"), P("tp"), wout_spec, P())

    def device_step(resid_loc, grad_loc, norm_gain, wqkv_loc, bqkv_loc, sink_loc, wout_loc, b_out):
        x, dy = resid_loc[0], grad_loc[0]
        half, d = x.shape
        heads = sink_loc.shape[0]
        wo_slab = jnp.concatenate([wout_loc[:, :d // 2], wout_loc[:, d // 2:]], axis=0)
        tab, base = rope_constants(2 * half // L)
        y, dx, gq, go, gain_g, bout_g, bqkv_g, sink_g = layer(wqkv_loc, wo_slab, x, x.reshape(2, *RING, 24, d), dy, norm_gain, b_out, bqkv_loc, sink_loc, row_permutation(), tab, base)
        return (y[None], dx[None], gain_g, gq, bqkv_g, sink_g[:heads], go, bout_g)

    return jax.shard_map(device_step, mesh=mesh, in_specs=in_specs, out_specs=out_specs, check_vma=False)
```

```python
import math

import jax
import jax.numpy as jnp
import numpy as np
from jax import lax
from jax.experimental import pallas as pl
from jax.experimental.pallas import tpu as pltpu
from jax.sharding import PartitionSpec as P

EPS = 1e-5
ROPE_BASE = 150000.0
WINDOW = 128
MESH = pl.DeviceIdType.MESH
STRIDE = (16, 4, 1)
F32 = jnp.float32
BF16 = jnp.bfloat16
VMEM_LIMIT = 67_000_000
Z, Y, X = range(3)
UP, DOWN, FAR = 1, -1, 2
L = 128
PAIR = (0, 1)
RING = (4, 4)
GROUP = 2 * L
TRIPLE = 3
NEG = -1e30


def coord(dim):
    return lax.rem(lax.div(lax.axis_index("fsdp"), STRIDE[dim]), 4)


def shifted(dim, k):
    return lax.rem(coord(dim) + (k + 4), 4)


def peer(dim, k):
    f = lax.axis_index("fsdp")
    return {"fsdp": f + (shifted(dim, k) - coord(dim)) * STRIDE[dim]}


def partner():
    return {"tp": 1 - lax.axis_index("tp")}


def span(n, size, base=0):
    return pl.ds(pl.multiple_of(base + n * size, math.gcd(size, L)), size)


def entry_barrier(peers):
    barrier = pltpu.get_barrier_semaphore()
    for p in peers:
        pl.semaphore_signal(barrier, inc=1, device_id=p, device_id_type=MESH)
    pl.semaphore_wait(barrier, len(peers))


class Copies:
    def __init__(self, send_sem, recv_sem):
        self.send_sem, self.recv_sem = send_sem, recv_sem
        self.n = 0
        self.sent = []

    def slots(self, count):
        first = self.n
        self.n += count
        return first

    def make(self, src, dst, slot, device):
        send = len(self.sent) % self.send_sem.shape[0]
        return pltpu.make_async_remote_copy(src_ref=src, dst_ref=dst, send_sem=self.send_sem.at[send], recv_sem=self.recv_sem.at[slot], device_id=device, device_id_type=MESH)

    def send(self, src, dst, slot, device):
        copy = self.make(src, dst, slot, device)
        copy.start()
        assert len(self.sent) < self.send_sem.shape[0]
        self.sent.append(copy)

    def arrive(self, ref, slot, device):
        self.make(ref, ref, slot, device).wait_recv()

    def drain(self):
        for copy in self.sent:
            copy.wait_send()
        self.sent = []


class GatherStage:
    def __init__(self, copies, dim, slot_view, own_view):
        self.c, self.dim, self.view, self.own = copies, dim, slot_view, own_view
        self.base = copies.slots(6)

    def start(self):
        me = coord(self.dim)
        for h in PAIR:
            self.c.send(self.own(h), self.view(me, h), self.base + h, peer(self.dim, UP))
            self.c.send(self.own(1 - h), self.view(me, 1 - h), self.base + 3 - h, peer(self.dim, DOWN))

    def sides(self):
        return [(shifted(self.dim, k), peer(self.dim, k)) for k in (DOWN, UP)]

    def mid(self):
        (lo, down), (hi, up) = self.sides()
        self.c.arrive(self.view(lo, 0), self.base, down)
        self.c.send(self.view(lo, 0), self.view(lo, 0), self.base + 4, up)
        self.c.arrive(self.view(hi, 1), self.base + 3, up)
        self.c.send(self.view(hi, 1), self.view(hi, 1), self.base + 5, down)

    def finish(self):
        (lo, down), (hi, up) = self.sides()
        far = shifted(self.dim, FAR)
        for n, (at, h, dev) in enumerate(((lo, 1, down), (hi, 0, up))):
            self.c.arrive(self.view(at, h), self.base + 1 + n, dev)
            self.c.arrive(self.view(far, n), self.base + 4 + n, dev)


class GatherDirect:
    def __init__(self, copies, dim, view, own):
        self.c, self.dim, self.view, self.own = copies, dim, view, own
        self.base = copies.slots(3)

    def start(self):
        for slot, k in enumerate((UP, DOWN, FAR)):
            self.c.send(self.own(), self.view(coord(self.dim)), self.base + slot, peer(self.dim, k))

    def finish(self):
        for slot, k in enumerate((UP, DOWN, FAR)):
            self.c.arrive(self.view(shifted(self.dim, -k)), self.base + slot, peer(self.dim, k))


def gather_stages(copies, in_ref, out_ref, order, first, size):
    rows = pl.ds(first, size)

    def view(n, c, h=None):
        idx = [coord(dim) for dim in (Z, Y, X)]
        for dim in order[:n]:
            idx[dim] = slice(None)
        idx[order[n]] = c
        if h is not None:
            cut = min(order[:n])
            idx[cut] = pl.ds(h * 2, 2)
        return out_ref.at[tuple(idx) + (rows,)]

    return (GatherDirect(copies, order[0], lambda c: view(0, c), lambda: in_ref.at[rows]),
            GatherDirect(copies, order[1], lambda c: view(1, c), lambda: view(1, coord(order[1]))),
            GatherStage(copies, order[2], lambda c, h: view(2, c, h), lambda h: view(2, coord(order[2]), h)))


ORDERS = ((X, Y, Z), (Y, Z, X), (Z, X, Y))


def rotate(vals, cos, sin):
    return vals * cos + pltpu.roll(vals, L // 2, 1) * sin


def stack_heads(vals):
    return jnp.concatenate([vals[:, n:n + L] for n in range(0, vals.shape[1], L)], axis=0)


def unstack_heads(vals):
    return jnp.concatenate([vals[n:n + L, :] for n in range(0, vals.shape[0], L)], axis=1)


def dot_nn(a, b):
    return jnp.dot(a, b, preferred_element_type=F32)


def dot_tn(a, b):
    return lax.dot_general(a, b, (((0,), (0,)), ((), ())), preferred_element_type=F32)


def dot_nt(a, b):
    return lax.dot_general(a, b, (((1,), (1,)), ((), ())), preferred_element_type=F32)


class Attention:
    def __init__(self, qkv, o, d_o, tab, base, sink_ref, dsink, keys, vals, dk, dv, top, inv, bias):
        self.qkv, self.o, self.d_o, self.tab, self.base, self.dsink = qkv, o, d_o, tab, base, dsink
        self.keys, self.vals, self.dk, self.dv, self.top, self.inv, self.bias = keys, vals, dk, dv, top, inv, bias
        self.width = o.shape[1]
        self.blocks = o.shape[0] // L
        self.scale = L ** -0.5
        self.sink = jnp.concatenate([jnp.full((1, L), sink_ref[n], F32) for n in range(self.width // L)], axis=1)

    def prepare(self):
        for ref in (self.keys, self.vals, self.dk, self.dv):
            ref[pl.ds(0, L), :] = jnp.zeros((L, L), ref.dtype)
        self.dsink[...] = jnp.zeros(self.dsink.shape, F32)
        k_idx = lax.broadcasted_iota(jnp.int32, (GROUP, L), 0)
        q_idx = lax.broadcasted_iota(jnp.int32, (GROUP, L), 1)
        allowed = (k_idx > q_idx) & (k_idx <= q_idx + WINDOW)
        self.bias[1] = jnp.where(allowed, 0.0, NEG).astype(BF16)
        self.bias[0] = jnp.where(allowed & (k_idx >= WINDOW), 0.0, NEG).astype(BF16)

    def tables(self, i):
        cos_b, sin_b = self.base[0, pl.ds(i, 1), :], self.base[1, pl.ds(i, 1), :]
        cos_r, sin_r = self.tab[0], self.tab[1]
        return cos_b * cos_r - sin_b * sin_r, sin_b * cos_r + cos_b * sin_r

    def scores(self, i, keys, q, heads):
        bias = self.bias[jnp.minimum(i, 1)].astype(F32)
        return dot_nt(keys, q) * self.scale + jnp.concatenate([bias] * heads, axis=1)

    def forward(self, first, last):
        heads = self.width // L

        @pl.loop(first // len(PAIR), last // len(PAIR))
        def _(m):
            at = span(m, GROUP)
            blocks = [m * len(PAIR) + n for n in PAIR]
            tables = [self.tables(i) for i in blocks]
            cos, sin = (jnp.concatenate(t, axis=0) for t in zip(*tables))
            new = pl.ds(pl.multiple_of(m * GROUP + L, L), GROUP)
            self.keys[new, :] = rotate(self.qkv[at, pl.ds(self.width, L)].astype(F32), cos, sin).astype(BF16)
            self.vals[new, :] = self.qkv[at, pl.ds(self.width + L, L)]
            for ref in (self.dk, self.dv):
                ref[new, :] = jnp.zeros((GROUP, L), F32)
            seen = pl.ds(pl.multiple_of(m * GROUP, L), TRIPLE * L)
            all_keys, all_vals = self.keys[seen, :], self.vals[seen, :]
            keys, vals = ([t[n * L:n * L + GROUP] for n in PAIR] for t in (all_keys, all_vals))
            raw = [stack_heads(self.qkv[span(i, L), pl.ds(0, self.width)]) for i in blocks]
            wide = [[jnp.concatenate([t] * heads, axis=0) for t in pair] for pair in tables]
            queries = [rotate(q.astype(F32), *w).astype(BF16) for q, w in zip(raw, wide)]
            scores = [self.scores(i, k, q, heads) for i, k, q in zip(blocks, keys, queries)]
            tops = [jnp.maximum(jnp.max(sc, axis=0, keepdims=True), self.sink) for sc in scores]
            probs = [jnp.exp(sc - top) for sc, top in zip(scores, tops)]
            invs = [1.0 / (jnp.sum(p, axis=0, keepdims=True) + jnp.exp(self.sink - top)) for p, top in zip(probs, tops)]
            outs = [dot_tn((p * inv).astype(BF16), v) for p, inv, v in zip(probs, invs, vals)]
            for ref, parts in ((self.o, outs), (self.qkv, queries)):
                ref[at, pl.ds(0, self.width)] = jnp.concatenate([unstack_heads(p.astype(BF16)) for p in parts], axis=0)
            for i, top, inv in zip(blocks, tops, invs):
                self.top[pl.ds(i, 1), :] = top
                self.inv[pl.ds(i, 1), :] = inv

    def backward(self, g):
        heads = GROUP // L
        here = span(g, GROUP)
        sink = self.sink[:, g * GROUP:(g + 1) * GROUP]

        @pl.loop(0, self.blocks // TRIPLE)
        def _(m):
            d_o = self.d_o[m, :, :, :, here].reshape(TRIPLE * L, GROUP)
            loads = []
            for n in range(TRIPLE):
                i = m * TRIPLE + n
                pair = pl.ds(pl.multiple_of(i * L, L), GROUP)
                loads.append((i, stack_heads(self.qkv[span(i, L), here]), stack_heads(d_o[n * L:(n + 1) * L]), self.keys[pair, :], self.vals[pair, :],
                              self.top[pl.ds(i, 1), here], self.inv[pl.ds(i, 1), here], self.tables(i)))
            wide = [[jnp.concatenate([t] * heads, axis=0) for t in load[-1]] for load in loads]
            scores = [self.scores(i, keys, q, heads) for i, q, _, keys, *_ in loads]
            d_probs = [dot_nt(load[4], load[2]) for load in loads]
            probs = [jnp.exp(sc - load[5]) * load[6] for sc, load in zip(scores, loads)]
            d_probs = [dp.astype(BF16).astype(F32) for dp in d_probs]
            dvs = [dot_nn(p.astype(BF16), load[2]) for p, load in zip(probs, loads)]
            row_dots = [jnp.sum(p * dp, axis=0, keepdims=True) for p, dp in zip(probs, d_probs)]
            d_scores = [(p * (dp - rd)).astype(BF16) for p, dp, rd in zip(probs, d_probs, row_dots)]
            d_sink = self.dsink[:, here]
            for rd, load in zip(row_dots, loads):
                d_sink = d_sink - jnp.exp(sink - load[5]) * load[6] * rd
            dqs = [(dot_tn(ds, load[3]) * self.scale).astype(BF16).astype(F32) for ds, load in zip(d_scores, loads)]
            dks = [dot_nn(ds, load[1]) * self.scale for ds, load in zip(d_scores, loads)]
            stores = [unstack_heads(rotate(dq, cos, -sin).astype(BF16)) for dq, (cos, sin) in zip(dqs, wide)]
            self.dsink[:, here] = d_sink
            self.qkv[span(m, TRIPLE * L), here] = jnp.concatenate(stores, axis=0)
            rows = pl.ds(pl.multiple_of(m * TRIPLE * L, L), (TRIPLE + 1) * L)
            for ref, new in ((self.dv, dvs), (self.dk, dks)):
                parts = [new[0][:L]] + [p[L:] + q[:L] for p, q in zip(new, new[1:])] + [new[-1][L:]]
                ref[rows, :] = ref[rows, :] + jnp.concatenate(parts, axis=0)

    def backward_kv(self):
        @pl.loop(0, self.blocks)
        def _(i):
            at, nxt = (span(i + n, L) for n in PAIR)
            cos, sin = self.tables(i)
            self.qkv[at, pl.ds(self.width, L)] = rotate(self.dk[nxt, :].astype(BF16).astype(F32), cos, -sin).astype(BF16)
            self.qkv[at, pl.ds(self.width + L, L)] = self.dv[nxt, :].astype(BF16)


class ScatterStage:
    def __init__(self, copies, dim, blk, buf, put):
        self.c, self.dim, self.blk, self.buf, self.put = copies, dim, blk, buf, put
        self.base = copies.slots(6)
        self.a_up, self.a_down, self.lo = 0, 1, (2, 3)
        self.hi = (4, 5)

    def send(self, src, slot, k):
        self.c.send(src, self.buf.at[slot], self.base + slot, peer(self.dim, k))

    def arrive(self, slot, k):
        self.c.arrive(self.buf.at[slot], self.base + slot, peer(self.dim, k))

    def start(self):
        up, down, far = (shifted(self.dim, k) for k in (UP, DOWN, FAR))
        self.send(self.blk(far, 0), self.a_up, UP)
        self.send(self.blk(far, 1), self.a_down, DOWN)
        self.send(self.blk(up, 1), self.lo[1], UP)
        self.send(self.blk(down, 0), self.hi[0], DOWN)

    def add(self, slot, src):
        dst = self.buf.at[slot]
        if len(src.shape) == 2:
            dst[...] = dst[...] + src[...]
        else:
            @pl.loop(0, src.shape[0])
            def _(j):
                dst[j] = dst[j] + src[j]

    def mid(self):
        self.arrive(self.a_up, DOWN)
        self.add(self.a_up, self.blk(shifted(self.dim, UP), 0))
        self.arrive(self.a_down, UP)
        self.add(self.a_down, self.blk(shifted(self.dim, DOWN), 1))
        self.send(self.buf.at[self.a_up], self.lo[0], UP)
        self.send(self.buf.at[self.a_down], self.hi[1], DOWN)

    def finish(self):
        me = coord(self.dim)
        for h in (1, 0):
            self.arrive(self.lo[h], DOWN)
            self.arrive(self.hi[1 - h], UP)
        for h in PAIR:
            own, a, b = self.blk(me, h), self.buf.at[self.lo[h]], self.buf.at[self.hi[h]]
            if len(own.shape) == 2:
                self.put(h, None, own[...] + a[...] + b[...])
            else:
                @pl.loop(0, own.shape[0])
                def _(j):
                    self.put(h, j, own[j] + a[j] + b[j])


class DirectStage:
    def __init__(self, copies, dim, blk, buf, put):
        self.c, self.dim, self.blk, self.buf, self.put = copies, dim, blk, buf, put
        self.base = copies.slots(3)

    def start(self):
        for slot, k in enumerate((UP, DOWN, FAR)):
            self.c.send(self.blk(shifted(self.dim, k)), self.buf.at[slot], self.base + slot, peer(self.dim, k))

    def finish(self):
        for slot, k in enumerate((UP, DOWN, FAR)):
            self.c.arrive(self.buf.at[slot], self.base + slot, peer(self.dim, k))
        b = self.buf
        self.put((self.blk(coord(self.dim))[...] + b[0]) + (b[1] + b[2]))


def scatter_steps(copies, src, out, order, first, width, band, bufs, padded):
    r1, r2, r3, s2, s3 = bufs
    rows = out.shape[0] if padded else band.size
    rest = [dim for dim in (Z, Y, X) if dim != order[0]]

    def pick(ref, at, t, h, in_band, cols):
        idx = [slice(None)] * (len(ref.shape) - 2) + [in_band]
        cut = 1 if at == 0 else 0
        half = ref.shape[cut] // 2
        idx[at], idx[cut] = t, pl.ds(h * half, half)
        return ref.at[tuple(idx) + (cols,)]

    def put1(h, j, val):
        s2[h * 2 + j] = val

    def put2(h, j, val):
        for t in PAIR:
            s3[h * 2 + t, 0:rows, :] = val[rows * t:rows * t + rows, :]

    def put_slabs(val):
        s3[...] = val

    def put3(val):
        out[pl.ds(0, rows) if padded else band, pl.ds(first, width)] = val[0:rows, :]

    one = ScatterStage(copies, order[0], lambda t, h: pick(src, order[0], t, h, band, pl.ds(first, width)), r1, put1)
    three = DirectStage(copies, order[2], lambda t: s3.at[t], r3, put3)
    if padded:
        two = ScatterStage(copies, order[1], lambda t, h: pick(s2, rest.index(order[1]), t, h, slice(None), slice(None)), r2, put2)
        return iter(((one.start,), (one.mid,), (one.finish, two.start), (two.mid,), (two.finish, three.start), (three.finish,)))
    side = rest.index(order[1])
    two = DirectStage(copies, order[1], lambda t: s2.at[(slice(None),) * side + (t,)], r2, put_slabs)
    return iter(((one.start,), (one.mid,), (one.finish, two.start), (two.finish, three.start), (three.finish,)))


def advance(*groups):
    for jobs in groups:
        for job in jobs:
            for step in next(job):
                step()


WO_JOBS = tuple((order, n * 768, 768, pl.ds(0, 48)) for n, order in enumerate(((Y, Z, X), (Z, Y, X))))
SLAB = pl.ds(0, 24)
WQ_JOBS = tuple((order, first * L, size, SLAB) for order, first, size in zip(ORDERS * 2, (0, 2, 3, 4, 6, 7), (GROUP, L, L) * 2))


def scatter_scratch():
    out = []
    for jobs, lead, pad in ((WO_JOBS, (), 16), (WQ_JOBS, (4,), None)):
        for _, _, width, band in jobs:
            rows = band.size
            second = (3, 4, rows, width) if lead else (6, rows // 2, width)
            shapes = ((6, 2) + lead + (rows, width), second, (3, pad or rows, width), (4,) + lead + (rows, width), (4, pad or rows, width))
            out += [pltpu.VMEM(shape, F32) for shape in shapes]
    return out


class SmallSums:
    def __init__(self, copies, ar):
        self.c, self.ar = copies, ar
        self.base = copies.slots(10)

    def start(self, n):
        if n < 3:
            for slot, k in enumerate((UP, DOWN, FAR)):
                ref = self.ar.at[n, coord(n)]
                self.c.send(ref, ref, self.base + 3 * n + slot, peer(n, k))
        else:
            ref = self.ar.at[n, lax.axis_index("tp")]
            self.c.send(ref, ref, self.base + 3 * n, partner())

    def finish(self, n):
        ar = self.ar
        if n < 3:
            for slot, k in enumerate((UP, DOWN, FAR)):
                self.c.arrive(ar.at[n, shifted(n, -k)], self.base + 3 * n + slot, peer(n, k))
            total = (ar[n, 0] + ar[n, 1]) + (ar[n, 2] + ar[n, 3])
            ar[n + 1, coord(n + 1) if n < 2 else lax.axis_index("tp")] = total
        else:
            self.c.arrive(ar.at[n, 1 - lax.axis_index("tp")], self.base + 3 * n, partner())


def layer_kernel(wq_in, wo_in, x_in, x5_in, dy_in, gain_ref, bout_ref, bqkv_ref, sink_ref, perm_ref, tab_ref, base_ref,
                 y_out, dx_out, *outs_and_scratch):
    hbm_outs, wo2_hbm, bufs = outs_and_scratch[:6], outs_and_scratch[6], list(outs_and_scratch[7:])
    (wq5, wo5, h, dy, qkv, o, wq, wo, wq2, o2, dqkv2, gq, go, ar, keys, vals, dk, dv, dsink, top, inv, bias, gain_sum,
     gq_out, go_out, gain_out, gbout_out, bqkv_out, sink_out, loc_sem, send_sem, recv_sem) = bufs[:32]
    bufs = bufs[32:]
    tp = lax.axis_index("tp")
    half, d = x_in.shape
    width, cols = o.shape[1], qkv.shape[1]
    start = tp * half
    mine, theirs = span(tp, half), span(1 - tp, half)
    wide, rest = pl.ds(0, cols), pl.ds(0, d - cols)
    x_low, x_high = qkv.at[pl.ds(0, half), :], qkv.at[pl.ds(half, half), rest]
    local = [pltpu.make_async_copy(a, b, loc_sem.at[n]) for n, (a, b) in enumerate((
        (x_in.at[:, wide], x_low), (x_in.at[:, pl.ds(cols, d - cols)], x_high), (dy_in, dy.at[mine, :])))]
    for copy in local:
        copy.start()
    for ref, own in ((wq5, wq_in), (wo5, wo_in)):
        ref[coord(Z), coord(Y), coord(X)] = own[...]
    entry_barrier([peer(dim, k) for dim in (Z, Y, X) for k in (UP, DOWN, FAR)] + [partner()])
    copies = Copies(send_sem, recv_sem)
    jobs_q, jobs_o = ([gather_stages(copies, a, b, order, 8 * n, 8) for n, order in enumerate(ORDERS)] for a, b in ((wq_in, wq5), (wo_in, wo5)))

    def each(jobs, n, *names):
        for name in names:
            for job in jobs:
                getattr(job[n], name)()

    each(jobs_q, 0, "start")
    each(jobs_o, 0, "start")
    gain, b_out = gain_ref[...][None, :], bout_ref[...].astype(F32)[None, :]
    parts = 3
    step = half // parts
    slot_h = copies.slots(parts)
    slot_dy, slot_wq, slot_wo, slot_o, slot_dqkv = (copies.slots(n) for n in (1, 1, 1, 1, 3))
    att = Attention(qkv, o, wq5, tab_ref, base_ref, sink_ref, dsink, keys, vals, dk, dv, top, inv, bias)
    att.prepare()
    for copy in local:
        copy.wait()
    copies.send(dy.at[mine, :], dy.at[mine, :], slot_dy, partner())

    pieces = iter(range(parts))

    def norm_piece():
        k = next(pieces)
        first = k * step

        @pl.loop(0, step // 32)
        def _(i):
            at = span(i, 32, first)
            xv = jnp.concatenate([x_low[at, :], x_high[at, :]], axis=1).astype(F32)
            inv = lax.rsqrt(jnp.mean(xv * xv, axis=-1, keepdims=True) + EPS)
            h[span(i, 32, start + first), :] = (xv * inv * gain).astype(BF16)

        return k

    def send_piece(k):
        at = span(k, step, start)
        copies.send(h.at[at, :], h.at[at, :], slot_h + k, partner())

    ready = norm_piece()
    each(jobs_q, 0, "finish")
    each(jobs_q, 1, "start")
    each(jobs_o, 0, "finish")
    send_piece(ready)
    ready = norm_piece()
    each(jobs_q, 1, "finish")
    each(jobs_q, 2, "start")
    send_piece(ready)
    send_piece(norm_piece())
    each(jobs_q, 2, "mid")
    each(jobs_o, 1, "start")
    for k in range(parts):
        copies.arrive(h.at[span(k, step, (1 - tp) * half), :], slot_h + k, partner())
    copies.arrive(dy.at[theirs, :], slot_dy, partner())
    each(jobs_q, 2, "finish")

    @pl.loop(0, 16)
    def _(n):
        wq[span(n, 96), :] = wq5[lax.div(n, 4), lax.rem(n, 4)].reshape(96, cols)

    b_qkv = bqkv_ref[...].astype(F32)[None, :]
    tile = 384

    def qkv_tile(n):
        qkv[span(n, tile), :] = (dot_nn(h[span(n, tile), :], wq[...]) + b_qkv).astype(BF16)

    qkv_tile(0)
    copies.send(wq, wq2, slot_wq, partner())
    each(jobs_o, 1, "finish")
    each(jobs_o, 2, "start")
    for n in range(1, 4):
        qkv_tile(n)
    att.forward(0, att.blocks // 2)
    each(jobs_o, 2, "mid")
    att.forward(att.blocks // 2, att.blocks)
    copies.send(o.at[theirs, :], o2, slot_o, partner())
    each(jobs_o, 2, "finish")

    def slabs(z, pair):
        return wo5[z, pl.ds(pair * 2, 2)].reshape(192, d // 2)

    @pl.loop(0, 8)
    def _(n):
        group = slabs(lax.div(n, 2), lax.rem(n, 2))
        for c in PAIR:
            wo[span(n, 96), span(c, d // 2)] = dot_nn(perm_ref[c], group).astype(BF16)

    copies.send(wo, wo2_hbm, slot_wo, partner())
    scatters = []
    for jobs, src, out, padded in ((WO_JOBS, go, go_out, True), (WQ_JOBS, gq, gq_out, False)):
        for job in jobs:
            five, bufs = bufs[:5], bufs[5:]
            if padded:
                five[4][...] = jnp.zeros(five[4].shape, F32)
            scatters.append(scatter_steps(copies, src, out, *job, five, padded))
    s_wo, s_0, s_1, s_2 = scatters[:2], scatters[2:3], scatters[3:5], scatters[5:]

    @pl.loop(0, 2)
    def _(m):
        @pl.loop(0, 3)
        def _(n):
            at, to = span(m, tile), span(n, 2 * GROUP)
            go[pl.ds(m * 2, 2), :, :, to] = dot_tn(o[:, at], dy[:, to]).reshape(2, 4, 48, 2 * GROUP)

    copies.drain()
    advance(s_wo)
    @pl.loop(0, 4)
    def _(n):
        at = span(n, tile)
        wq5[n, :, :, :, pl.ds(0, width)] = dot_nt(dy[at, :], wo[...]).astype(BF16).reshape(*RING, 24, width)


    def done(g):
        return pl.ds(g * GROUP, GROUP if g < 2 else 2 * GROUP)

    def wq_grad(to):

        @pl.loop(0, 4)
        def _(m):
            gq[m, :, :, :, to] = dot_tn(h[:, span(m, tile)], qkv[:, to]).reshape(*RING, 24, to.size)

    for g, (jobs, after) in enumerate(((s_0, s_wo), (s_1, s_0), (s_2, s_wo + s_0))):
        att.backward(g)
        if g == 2:
            att.backward_kv()
        copies.send(qkv.at[theirs, done(g)], dqkv2.at[:, done(g)], slot_dqkv + g, partner())
        if jobs is s_2:
            advance(s_1)
        wq_grad(done(g))
        advance(after, jobs)
    own = ar.at[Z, coord(Z)]
    own[...] = jnp.zeros(own.shape, F32)
    small = SmallSums(copies, ar)
    ones = jnp.ones((8, 2 * half), BF16)
    own[2:3, 0:cols] = dot_nn(ones, qkv[...])[0:1]
    own[3:4, 0:width] = dsink[...]
    own[1:2, :] = dot_nn(ones[:, 0:half], dy[mine, :])[0:1]
    loads = [pltpu.make_async_copy(x5_in.at[:, :, :, :, span(c, d // 2)], wo5.at[pl.ds(c * 2, 2)], loc_sem.at[c]) for c in PAIR]
    wo2 = h.at[pl.ds(0, half), :]
    loads.append(pltpu.make_async_copy(wo2_hbm, wo2, loc_sem.at[2]))
    for ref, slot in ((wo2_hbm, slot_wo), (wq2, slot_wq), (o2, slot_o)):
        copies.arrive(ref, slot, partner())
    for copy in loads:
        copy.start()
    for g in range(3):
        copies.arrive(dqkv2.at[:, done(g)], slot_dqkv + g, partner())
    wide_half = d // 2

    def dh_tiles(c):
        to = span(c, wide_half)

        @pl.loop(0, 2)
        def _(n):
            h[span(n, tile, half), to] = (dot_nt(qkv[span(n, tile, start), :], wq[to, :]) + dot_nt(dqkv2[span(n, tile), :], wq2[to, :])).astype(BF16)

    dh_tiles(0)
    advance(s_wo)
    dh_tiles(1)
    for copy in loads:
        copy.wait()
    rows = 48
    gain_sum[...] = jnp.zeros(gain_sum.shape, F32)

    def norm_back(c):
        count = half // rows // 2

        @pl.loop(c * count, c * count + count)
        def _(n):
            at = span(n, rows, start)
            z, yy, pair = lax.div(n, 8), lax.rem(lax.div(n, 2), 4), pl.ds(lax.rem(n, 2) * 2, 2)
            xv = jnp.concatenate([wo5[z + c, yy, pair].reshape(rows, d // 2) for c in (0, 2)], axis=1).astype(F32)
            dh = h[span(n, rows, half), :].astype(F32)
            inv = lax.rsqrt(jnp.mean(xv * xv, axis=-1, keepdims=True) + EPS)
            xn, gg = xv * inv, dh * gain
            dx = inv * (gg - xn * jnp.mean(gg * xn, axis=-1, keepdims=True))
            dy[at, :] = (dy[at, :].astype(F32) + dx).astype(BF16)
            gain_sum[...] = gain_sum[...] + jnp.sum((dh * xn).reshape(rows // 8, 8, d), axis=0)

    norm_back(0)
    advance(s_2)
    norm_back(1)
    own[0:1, :] = jnp.sum(gain_sum[...], axis=0, keepdims=True)
    store_dx = pltpu.make_async_copy(dy.at[mine, :], dx_out, loc_sem.at[7])
    store_dx.start()
    small.start(0)
    advance(s_1)
    def y_tiles(c):
        to = span(c, wide_half)

        @pl.loop(0, 2)
        def _(n):
            at = span(n, tile)
            xv = wo5[n + 2 * c].reshape(tile, wide_half).astype(F32)
            acc = dot_nn(o[span(n, tile, start), :], wo[:, to]) + dot_nn(o2[at, :], wo2[:, to])
            dy[span(n, tile, (1 - tp) * half), to] = (xv + acc + b_out[:, c * wide_half:(c + 1) * wide_half]).astype(BF16)

    y_tiles(0)
    small.finish(0)
    small.start(1)
    advance(s_2, s_0, s_wo)
    y_tiles(1)
    store_y = pltpu.make_async_copy(dy.at[theirs, :], y_out, loc_sem.at[6])
    store_y.start()
    small.finish(1)
    small.start(2)
    advance(s_2, s_1)
    small.finish(2)
    small.start(3)
    advance(s_0, s_wo, s_1, s_2)
    small.finish(3)
    both = ar[3, 0] + ar[3, 1]
    row = ar[3, tp]
    gain_out[...] = both[0]
    gbout_out[...] = both[1]
    bqkv_out[...] = row[2, 0:cols]
    lane = lax.broadcasted_iota(jnp.int32, (1, L), 1)
    sinks = jnp.zeros(lane.shape, F32)
    for n in range(width // L):
        sinks = jnp.where(lane == n, jnp.sum(row[3:4, n * L:n * L + L], axis=1, keepdims=True), sinks)
    sink_out[...] = sinks[0]
    stores = [pltpu.make_async_copy(a, b, loc_sem.at[n]) for n, (a, b) in enumerate(zip((gq_out, go_out, gain_out, gbout_out, bqkv_out, sink_out), hbm_outs))]
    for copy in stores[1:]:
        copy.start()
    for jobs in (s_wo, s_0, s_1, s_2):
        for job in jobs:
            assert next(job, None) is None
    copies.drain()
    stores[0].start()
    for copy in stores + [store_y, store_dx]:
        copy.wait()


VM = pl.BlockSpec(memory_space=pltpu.VMEM)
ANY = pl.BlockSpec(memory_space=pl.ANY)


def layer(wq, wo, x, x5, dy, gain, b_out, b_qkv, sinks, perm, tab, base):
    half, d = x.shape
    cols, width = wq.shape[1], wo.shape[1]
    seq = 2 * half
    n = 10 + 10 + len(ORDERS + ORDERS + WQ_JOBS) * 12 + len(WO_JOBS) * 15
    sds = jax.ShapeDtypeStruct
    shapes = ((4,) + RING + wq.shape, (4,) + RING + wo.shape, (seq, d), (seq, d), (seq, cols), (seq, width), (d, cols), (width, d), (d, cols), (half, width), (half, cols))
    scratch = [pltpu.VMEM(shape, BF16) for shape in shapes]
    scratch += [pltpu.VMEM((4, *RING, 24, cols), F32), pltpu.VMEM((*RING, 48, d), F32), pltpu.VMEM((4, *RING, d), F32)]
    scratch += [pltpu.VMEM((seq + L, L), t) for t in (BF16, BF16, F32, F32)] + [pltpu.VMEM((1, width), F32)]
    scratch += [pltpu.VMEM((seq // L, width), F32)] * 2 + [pltpu.VMEM((2, GROUP, L), BF16), pltpu.VMEM((8, d), F32)]
    outs = (sds((half, d), BF16), sds((half, d), BF16), sds((24, cols), F32), sds((12, d), F32), sds((d,), F32), sds((d,), F32), sds((cols,), F32), sds((L,), F32))
    scratch += [pltpu.VMEM(o.shape, F32) for o in outs[2:]] + [pltpu.SemaphoreType.DMA((k,)) for k in (8, n * 3 // 5, n)]
    results = pl.pallas_call(
        layer_kernel, name="layer", out_shape=outs + (sds((width, d), BF16),),
        in_specs=[VM, VM, ANY, ANY, ANY, VM, VM, VM, pl.BlockSpec(memory_space=pltpu.SMEM)] + [VM] * 3, out_specs=(ANY,) * 9, scratch_shapes=scratch + scatter_scratch(),
        compiler_params=pltpu.CompilerParams(collective_id=0, has_side_effects=True, vmem_limit_bytes=VMEM_LIMIT),
    )(wq, wo, x, x5, dy, gain, b_out, b_qkv, sinks, perm, tab, base)
    return pl.pallas_call(
        hand_over, name="hand_over", out_shape=outs, in_specs=[ANY] * 8, out_specs=(ANY,) * 8,
        scratch_shapes=[pltpu.VMEM(o.shape, o.dtype) for o in outs] + [pltpu.SemaphoreType.DMA((8, 4))] * 2,
    )(*results[:-1])


def hand_over(*refs):
    *refs, in_sem, out_sem = refs
    n = len(refs) // 3
    ins, outs, bufs = refs[:n], refs[n:2 * n], refs[2 * n:]
    copies = []
    for k, (a, buf, b) in enumerate(zip(ins, bufs, outs)):
        parts = in_sem.shape[1] if k < 2 else 1
        step = a.shape[0] // parts
        for n in range(parts):
            at = pl.ds(n * step, step)
            copies.append((pltpu.make_async_copy(a.at[at], buf.at[at], in_sem.at[k, n]), pltpu.make_async_copy(buf.at[at], b.at[at], out_sem.at[k, n])))
    for load, _ in copies:
        load.start()
    for load, store in copies:
        load.wait()
        store.start()
    for _, store in copies:
        store.wait()


def rope_constants(n_blocks):
    freq = np.tile(ROPE_BASE ** (-2.0 * np.arange(L // 2) / L), 2)
    sign = np.where(np.arange(L) < L // 2, -1.0, 1.0)

    def pair(positions):
        angle = positions[:, None] * freq[None, :]
        return jnp.asarray(np.stack([np.cos(angle), np.sin(angle) * sign]), F32)

    return pair(np.arange(L)), pair(np.arange(n_blocks) * L)


def row_permutation():
    row = np.arange(96)[:, None]
    col = np.arange(192)[None, :]
    return jnp.asarray(np.stack([col == row // 12 * 24 + c * 12 + row % 12 for c in PAIR]), BF16)


def solution(mesh):
    act_spec = P("fsdp", "tp", None)
    wout_spec = P(("tp", "fsdp"), None)
    in_specs = (act_spec, act_spec, P(), P("fsdp", "tp"), P("tp"), P("tp"), wout_spec, P())
    out_specs = (act_spec, act_spec, P(), P("fsdp", "tp"), P("tp"), P("tp"), wout_spec, P())

    def device_step(resid_loc, grad_loc, norm_gain, wqkv_loc, bqkv_loc, sink_loc, wout_loc, b_out):
        x, dy = resid_loc[0], grad_loc[0]
        half, d = x.shape
        heads = sink_loc.shape[0]
        wo_slab = jnp.concatenate([wout_loc[:, :d // 2], wout_loc[:, d // 2:]], axis=0)
        tab, base = rope_constants(2 * half // L)
        y, dx, gq, go, gain_g, bout_g, bqkv_g, sink_g = layer(wqkv_loc, wo_slab, x, x.reshape(2, *RING, 24, d), dy, norm_gain, b_out, bqkv_loc, sink_loc, row_permutation(), tab, base)
        return (y[None], dx[None], gain_g, gq, bqkv_g, sink_g[:heads], go, bout_g)

    return jax.shard_map(device_step, mesh=mesh, in_specs=in_specs, out_specs=out_specs, check_vma=False)
```

```python
import math

import jax
import jax.numpy as jnp
import numpy as np
from jax import lax
from jax.experimental import pallas as pl
from jax.experimental.pallas import tpu as pltpu
from jax.sharding import PartitionSpec as P

EPS = 1e-5
ROPE_BASE = 150000.0
WINDOW = 128
MESH = pl.DeviceIdType.MESH
STRIDE = (16, 4, 1)
F32 = jnp.float32
BF16 = jnp.bfloat16
VMEM_LIMIT = 67_000_000
Z, Y, X = range(3)
UP, DOWN, FAR = 1, -1, 2
L = 128
PAIR = (0, 1)
RING = (4, 4)
GROUP = 2 * L
TRIPLE = 3
NEG = -1e30


def coord(dim):
    return lax.rem(lax.div(lax.axis_index("fsdp"), STRIDE[dim]), 4)


def shifted(dim, k):
    return lax.rem(coord(dim) + (k + 4), 4)


def peer(dim, k):
    f = lax.axis_index("fsdp")
    return {"fsdp": f + (shifted(dim, k) - coord(dim)) * STRIDE[dim]}


def partner():
    return {"tp": 1 - lax.axis_index("tp")}


def span(n, size, base=0):
    return pl.ds(pl.multiple_of(base + n * size, math.gcd(size, L)), size)


def entry_barrier(peers):
    barrier = pltpu.get_barrier_semaphore()
    for p in peers:
        pl.semaphore_signal(barrier, inc=1, device_id=p, device_id_type=MESH)
    pl.semaphore_wait(barrier, len(peers))


class Copies:
    def __init__(self, send_sem, recv_sem):
        self.send_sem, self.recv_sem = send_sem, recv_sem
        self.n = 0
        self.sent = []

    def slots(self, count):
        first = self.n
        self.n += count
        return first

    def make(self, src, dst, slot, device):
        send = len(self.sent) % self.send_sem.shape[0]
        return pltpu.make_async_remote_copy(src_ref=src, dst_ref=dst, send_sem=self.send_sem.at[send], recv_sem=self.recv_sem.at[slot], device_id=device, device_id_type=MESH)

    def send(self, src, dst, slot, device):
        copy = self.make(src, dst, slot, device)
        copy.start()
        assert len(self.sent) < self.send_sem.shape[0]
        self.sent.append(copy)

    def arrive(self, ref, slot, device):
        self.make(ref, ref, slot, device).wait_recv()

    def drain(self):
        for copy in self.sent:
            copy.wait_send()
        self.sent = []


class GatherStage:
    def __init__(self, copies, dim, slot_view, own_view):
        self.c, self.dim, self.view, self.own = copies, dim, slot_view, own_view
        self.base = copies.slots(6)

    def start(self):
        me = coord(self.dim)
        for h in PAIR:
            self.c.send(self.own(h), self.view(me, h), self.base + h, peer(self.dim, UP))
            self.c.send(self.own(1 - h), self.view(me, 1 - h), self.base + 3 - h, peer(self.dim, DOWN))

    def sides(self):
        return [(shifted(self.dim, k), peer(self.dim, k)) for k in (DOWN, UP)]

    def mid(self):
        (lo, down), (hi, up) = self.sides()
        self.c.arrive(self.view(lo, 0), self.base, down)
        self.c.send(self.view(lo, 0), self.view(lo, 0), self.base + 4, up)
        self.c.arrive(self.view(hi, 1), self.base + 3, up)
        self.c.send(self.view(hi, 1), self.view(hi, 1), self.base + 5, down)

    def finish(self):
        (lo, down), (hi, up) = self.sides()
        far = shifted(self.dim, FAR)
        for n, (at, h, dev) in enumerate(((lo, 1, down), (hi, 0, up))):
            self.c.arrive(self.view(at, h), self.base + 1 + n, dev)
            self.c.arrive(self.view(far, n), self.base + 4 + n, dev)


class GatherDirect:
    def __init__(self, copies, dim, view, own):
        self.c, self.dim, self.view, self.own = copies, dim, view, own
        self.base = copies.slots(3)

    def start(self):
        for slot, k in enumerate((UP, DOWN, FAR)):
            self.c.send(self.own(), self.view(coord(self.dim)), self.base + slot, peer(self.dim, k))

    def finish(self):
        for slot, k in enumerate((UP, DOWN, FAR)):
            self.c.arrive(self.view(shifted(self.dim, -k)), self.base + slot, peer(self.dim, k))


def gather_stages(copies, in_ref, out_ref, order, first, size):
    rows = pl.ds(first, size)

    def view(n, c, h=None):
        idx = [coord(dim) for dim in (Z, Y, X)]
        for dim in order[:n]:
            idx[dim] = slice(None)
        idx[order[n]] = c
        if h is not None:
            cut = min(order[:n])
            idx[cut] = pl.ds(h * 2, 2)
        return out_ref.at[tuple(idx) + (rows,)]

    return (GatherDirect(copies, order[0], lambda c: view(0, c), lambda: in_ref.at[rows]),
            GatherDirect(copies, order[1], lambda c: view(1, c), lambda: view(1, coord(order[1]))),
            GatherStage(copies, order[2], lambda c, h: view(2, c, h), lambda h: view(2, coord(order[2]), h)))


ORDERS = ((X, Y, Z), (Y, Z, X), (Z, X, Y))


def rotate(vals, cos, sin):
    return vals * cos + pltpu.roll(vals, L // 2, 1) * sin


def stack_heads(vals):
    return jnp.concatenate([vals[:, n:n + L] for n in range(0, vals.shape[1], L)], axis=0)


def unstack_heads(vals):
    return jnp.concatenate([vals[n:n + L, :] for n in range(0, vals.shape[0], L)], axis=1)


def dot_nn(a, b):
    return jnp.dot(a, b, preferred_element_type=F32)


def dot_tn(a, b):
    return lax.dot_general(a, b, (((0,), (0,)), ((), ())), preferred_element_type=F32)


def dot_nt(a, b):
    return lax.dot_general(a, b, (((1,), (1,)), ((), ())), preferred_element_type=F32)


class Attention:
    def __init__(self, qkv, o, d_o, tab, base, sink_ref, dsink, keys, vals, dk, dv, top, inv, bias):
        self.qkv, self.o, self.d_o, self.tab, self.base, self.dsink = qkv, o, d_o, tab, base, dsink
        self.keys, self.vals, self.dk, self.dv, self.top, self.inv, self.bias = keys, vals, dk, dv, top, inv, bias
        self.width = o.shape[1]
        self.blocks = o.shape[0] // L
        self.scale = L ** -0.5
        self.sink = jnp.concatenate([jnp.full((1, L), sink_ref[n], F32) for n in range(self.width // L)], axis=1)

    def prepare(self):
        for ref in (self.keys, self.vals, self.dk, self.dv):
            ref[pl.ds(0, L), :] = jnp.zeros((L, L), ref.dtype)
        self.dsink[...] = jnp.zeros(self.dsink.shape, F32)
        k_idx = lax.broadcasted_iota(jnp.int32, (GROUP, L), 0)
        q_idx = lax.broadcasted_iota(jnp.int32, (GROUP, L), 1)
        allowed = (k_idx > q_idx) & (k_idx <= q_idx + WINDOW)
        self.bias[1] = jnp.where(allowed, 0.0, NEG).astype(BF16)
        self.bias[0] = jnp.where(allowed & (k_idx >= WINDOW), 0.0, NEG).astype(BF16)

    def tables(self, i):
        cos_b, sin_b = self.base[0, pl.ds(i, 1), :], self.base[1, pl.ds(i, 1), :]
        cos_r, sin_r = self.tab[0], self.tab[1]
        return cos_b * cos_r - sin_b * sin_r, sin_b * cos_r + cos_b * sin_r

    def scores(self, i, keys, q, heads):
        bias = self.bias[jnp.minimum(i, 1)].astype(F32)
        return dot_nt(keys, q) * self.scale + jnp.concatenate([bias] * heads, axis=1)

    def forward(self, first, last):
        heads = self.width // L

        @pl.loop(first // len(PAIR), last // len(PAIR))
        def _(m):
            at = span(m, GROUP)
            blocks = [m * len(PAIR) + n for n in PAIR]
            tables = [self.tables(i) for i in blocks]
            cos, sin = (jnp.concatenate(t, axis=0) for t in zip(*tables))
            new = pl.ds(pl.multiple_of(m * GROUP + L, L), GROUP)
            self.keys[new, :] = rotate(self.qkv[at, pl.ds(self.width, L)].astype(F32), cos, sin).astype(BF16)
            self.vals[new, :] = self.qkv[at, pl.ds(self.width + L, L)]
            for ref in (self.dk, self.dv):
                ref[new, :] = jnp.zeros((GROUP, L), F32)
            seen = pl.ds(pl.multiple_of(m * GROUP, L), TRIPLE * L)
            all_keys, all_vals = self.keys[seen, :], self.vals[seen, :]
            keys, vals = ([t[n * L:n * L + GROUP] for n in PAIR] for t in (all_keys, all_vals))
            raw = [stack_heads(self.qkv[span(i, L), pl.ds(0, self.width)]) for i in blocks]
            wide = [[jnp.concatenate([t] * heads, axis=0) for t in pair] for pair in tables]
            queries = [rotate(q.astype(F32), *w).astype(BF16) for q, w in zip(raw, wide)]
            scores = [self.scores(i, k, q, heads) for i, k, q in zip(blocks, keys, queries)]
            tops = [jnp.maximum(jnp.max(sc, axis=0, keepdims=True), self.sink) for sc in scores]
            probs = [jnp.exp(sc - top) for sc, top in zip(scores, tops)]
            invs = [1.0 / (jnp.sum(p, axis=0, keepdims=True) + jnp.exp(self.sink - top)) for p, top in zip(probs, tops)]
            outs = [dot_tn((p * inv).astype(BF16), v) for p, inv, v in zip(probs, invs, vals)]
            for ref, parts in ((self.o, outs), (self.qkv, queries)):
                ref[at, pl.ds(0, self.width)] = jnp.concatenate([unstack_heads(p.astype(BF16)) for p in parts], axis=0)
            for i, top, inv in zip(blocks, tops, invs):
                self.top[pl.ds(i, 1), :] = top
                self.inv[pl.ds(i, 1), :] = inv

    def backward(self, g):
        heads = GROUP // L
        here = span(g, GROUP)
        sink = self.sink[:, g * GROUP:(g + 1) * GROUP]

        @pl.loop(0, self.blocks // TRIPLE)
        def _(m):
            d_o = self.d_o[m, :, :, :, here].reshape(TRIPLE * L, GROUP)
            loads = []
            for n in range(TRIPLE):
                i = m * TRIPLE + n
                pair = pl.ds(pl.multiple_of(i * L, L), GROUP)
                loads.append((i, stack_heads(self.qkv[span(i, L), here]), stack_heads(d_o[n * L:(n + 1) * L]), self.keys[pair, :], self.vals[pair, :],
                              self.top[pl.ds(i, 1), here], self.inv[pl.ds(i, 1), here], self.tables(i)))
            wide = [[jnp.concatenate([t] * heads, axis=0) for t in load[-1]] for load in loads]
            scores = [self.scores(i, keys, q, heads) for i, q, _, keys, *_ in loads]
            d_probs = [dot_nt(load[4], load[2]) for load in loads]
            probs = [jnp.exp(sc - load[5]) * load[6] for sc, load in zip(scores, loads)]
            d_probs = [dp.astype(BF16).astype(F32) for dp in d_probs]
            dvs = [dot_nn(p.astype(BF16), load[2]) for p, load in zip(probs, loads)]
            row_dots = [jnp.sum(p * dp, axis=0, keepdims=True) for p, dp in zip(probs, d_probs)]
            d_scores = [(p * (dp - rd)).astype(BF16) for p, dp, rd in zip(probs, d_probs, row_dots)]
            d_sink = self.dsink[:, here]
            for rd, load in zip(row_dots, loads):
                d_sink = d_sink - jnp.exp(sink - load[5]) * load[6] * rd
            dqs = [(dot_tn(ds, load[3]) * self.scale).astype(BF16).astype(F32) for ds, load in zip(d_scores, loads)]
            dks = [dot_nn(ds, load[1]) * self.scale for ds, load in zip(d_scores, loads)]
            stores = [unstack_heads(rotate(dq, cos, -sin).astype(BF16)) for dq, (cos, sin) in zip(dqs, wide)]
            self.dsink[:, here] = d_sink
            self.qkv[span(m, TRIPLE * L), here] = jnp.concatenate(stores, axis=0)
            rows = pl.ds(pl.multiple_of(m * TRIPLE * L, L), (TRIPLE + 1) * L)
            for ref, new in ((self.dv, dvs), (self.dk, dks)):
                parts = [new[0][:L]] + [p[L:] + q[:L] for p, q in zip(new, new[1:])] + [new[-1][L:]]
                ref[rows, :] = ref[rows, :] + jnp.concatenate(parts, axis=0)

    def backward_kv(self):
        @pl.loop(0, self.blocks)
        def _(i):
            at, nxt = (span(i + n, L) for n in PAIR)
            cos, sin = self.tables(i)
            self.qkv[at, pl.ds(self.width, L)] = rotate(self.dk[nxt, :].astype(BF16).astype(F32), cos, -sin).astype(BF16)
            self.qkv[at, pl.ds(self.width + L, L)] = self.dv[nxt, :].astype(BF16)


class ScatterStage:
    def __init__(self, copies, dim, blk, buf, put):
        self.c, self.dim, self.blk, self.buf, self.put = copies, dim, blk, buf, put
        self.base = copies.slots(3)
        self.a_up, self.a_down, self.lo = 0, 1, (2, 3)
        self.hi = (4, 5)

    def send(self, src, slot, k):
        self.c.send(src, self.buf.at[slot], self.base + min(slot, 2), peer(self.dim, k))

    def arrive(self, slot, k):
        self.c.arrive(self.buf.at[slot], self.base + slot, peer(self.dim, k))

    def start(self):
        up, down, far = (shifted(self.dim, k) for k in (UP, DOWN, FAR))
        self.send(self.blk(far, 0), self.a_up, UP)
        self.send(self.blk(far, 1), self.a_down, DOWN)
        self.send(self.blk(up, 1), self.lo[1], UP)
        self.send(self.blk(down, 0), self.hi[0], DOWN)

    def add(self, slot, src):
        dst = self.buf.at[slot]
        if len(src.shape) == 2:
            dst[...] = dst[...] + src[...]
        else:
            @pl.loop(0, src.shape[0])
            def _(j):
                dst[j] = dst[j] + src[j]

    def mid(self):
        self.arrive(self.a_up, DOWN)
        self.add(self.a_up, self.blk(shifted(self.dim, UP), 0))
        self.arrive(self.a_down, UP)
        self.add(self.a_down, self.blk(shifted(self.dim, DOWN), 1))
        self.send(self.buf.at[self.a_up], self.lo[0], UP)
        self.send(self.buf.at[self.a_down], self.hi[1], DOWN)

    def finish(self):
        me = coord(self.dim)
        self.c.arrive(self.buf.at[pl.ds(2, 4)], self.base + 2, peer(self.dim, UP))
        for h in PAIR:
            own, a, b = self.blk(me, h), self.buf.at[self.lo[h]], self.buf.at[self.hi[h]]
            if len(own.shape) == 2:
                self.put(h, None, own[...] + a[...] + b[...])
            else:
                @pl.loop(0, own.shape[0])
                def _(j):
                    self.put(h, j, own[j] + a[j] + b[j])


class DirectStage:
    def __init__(self, copies, dim, blk, buf, put):
        self.c, self.dim, self.blk, self.buf, self.put = copies, dim, blk, buf, put
        self.base = copies.slots(1)

    def start(self):
        for slot, k in enumerate((UP, DOWN, FAR)):
            self.c.send(self.blk(shifted(self.dim, k)), self.buf.at[slot], self.base, peer(self.dim, k))

    def finish(self):
        self.c.arrive(self.buf, self.base, peer(self.dim, UP))
        b = self.buf
        self.put((self.blk(coord(self.dim))[...] + b[0]) + (b[1] + b[2]))


def scatter_steps(copies, src, out, order, first, width, band, bufs, padded):
    r1, r2, r3, s2, s3 = bufs
    rows = out.shape[0] if padded else band.size
    rest = [dim for dim in (Z, Y, X) if dim != order[0]]

    def pick(ref, at, t, h, in_band, cols):
        idx = [slice(None)] * (len(ref.shape) - 2) + [in_band]
        cut = 1 if at == 0 else 0
        half = ref.shape[cut] // 2
        idx[at], idx[cut] = t, pl.ds(h * half, half)
        return ref.at[tuple(idx) + (cols,)]

    def put1(h, j, val):
        s2[h * 2 + j] = val

    def put2(h, j, val):
        for t in PAIR:
            s3[h * 2 + t, 0:rows, :] = val[rows * t:rows * t + rows, :]

    def put_slabs(val):
        s3[...] = val

    def put3(val):
        out[pl.ds(0, rows) if padded else band, pl.ds(first, width)] = val[0:rows, :]

    one = ScatterStage(copies, order[0], lambda t, h: pick(src, order[0], t, h, band, pl.ds(first, width)), r1, put1)
    three = DirectStage(copies, order[2], lambda t: s3.at[t], r3, put3)
    if padded:
        two = ScatterStage(copies, order[1], lambda t, h: pick(s2, rest.index(order[1]), t, h, slice(None), slice(None)), r2, put2)
        return iter(((one.start,), (one.mid,), (one.finish, two.start), (two.mid,), (two.finish, three.start), (three.finish,)))
    side = rest.index(order[1])
    two = DirectStage(copies, order[1], lambda t: s2.at[(slice(None),) * side + (t,)], r2, put_slabs)
    return iter(((one.start,), (one.mid,), (one.finish, two.start), (two.finish, three.start), (three.finish,)))


def advance(*groups):
    for jobs in groups:
        for job in jobs:
            for step in next(job):
                step()


WO_JOBS = tuple((order, n * 768, 768, pl.ds(0, 48)) for n, order in enumerate(((Y, Z, X), (Z, Y, X))))
SLAB = pl.ds(0, 24)
WQ_JOBS = tuple((order, first * L, size, SLAB) for order, first, size in zip(ORDERS * 2, (0, 2, 3, 4, 6, 7), (GROUP, L, L) * 2))


def scatter_scratch():
    out = []
    for jobs, lead, pad in ((WO_JOBS, (), 16), (WQ_JOBS, (4,), None)):
        for _, _, width, band in jobs:
            rows = band.size
            second = (3, 4, rows, width) if lead else (6, rows // 2, width)
            shapes = ((6, 2) + lead + (rows, width), second, (3, pad or rows, width), (4,) + lead + (rows, width), (4, pad or rows, width))
            out += [pltpu.VMEM(shape, F32) for shape in shapes]
    return out


class SmallSums:
    def __init__(self, copies, ar):
        self.c, self.ar = copies, ar
        self.base = copies.slots(10)

    def start(self, n):
        if n < 3:
            for slot, k in enumerate((UP, DOWN, FAR)):
                ref = self.ar.at[n, coord(n)]
                self.c.send(ref, ref, self.base + 3 * n + slot, peer(n, k))
        else:
            ref = self.ar.at[n, lax.axis_index("tp")]
            self.c.send(ref, ref, self.base + 3 * n, partner())

    def finish(self, n):
        ar = self.ar
        if n < 3:
            for slot, k in enumerate((UP, DOWN, FAR)):
                self.c.arrive(ar.at[n, shifted(n, -k)], self.base + 3 * n + slot, peer(n, k))
            total = (ar[n, 0] + ar[n, 1]) + (ar[n, 2] + ar[n, 3])
            ar[n + 1, coord(n + 1) if n < 2 else lax.axis_index("tp")] = total
        else:
            self.c.arrive(ar.at[n, 1 - lax.axis_index("tp")], self.base + 3 * n, partner())


def layer_kernel(wq_in, wo_in, x_in, x5_in, dy_in, gain_ref, bout_ref, bqkv_ref, sink_ref, perm_ref, tab_ref, base_ref,
                 y_out, dx_out, *outs_and_scratch):
    hbm_outs, wo2_hbm, bufs = outs_and_scratch[:6], outs_and_scratch[6], list(outs_and_scratch[7:])
    (wq5, wo5, h, dy, qkv, o, wq, wo, wq2, o2, dqkv2, gq, go, ar, keys, vals, dk, dv, dsink, top, inv, bias, gain_sum,
     gq_out, go_out, gain_out, gbout_out, bqkv_out, sink_out, loc_sem, send_sem, recv_sem) = bufs[:32]
    bufs = bufs[32:]
    tp = lax.axis_index("tp")
    half, d = x_in.shape
    width, cols = o.shape[1], qkv.shape[1]
    start = tp * half
    mine, theirs = span(tp, half), span(1 - tp, half)
    wide, rest = pl.ds(0, cols), pl.ds(0, d - cols)
    x_low, x_high = qkv.at[pl.ds(0, half), :], qkv.at[pl.ds(half, half), rest]
    local = [pltpu.make_async_copy(a, b, loc_sem.at[n]) for n, (a, b) in enumerate((
        (x_in.at[:, wide], x_low), (x_in.at[:, pl.ds(cols, d - cols)], x_high), (dy_in, dy.at[mine, :])))]
    for copy in local:
        copy.start()
    for ref, own in ((wq5, wq_in), (wo5, wo_in)):
        ref[coord(Z), coord(Y), coord(X)] = own[...]
    entry_barrier([peer(dim, k) for dim in (Z, Y, X) for k in (UP, DOWN, FAR)] + [partner()])
    copies = Copies(send_sem, recv_sem)
    jobs_q, jobs_o = ([gather_stages(copies, a, b, order, 8 * n, 8) for n, order in enumerate(ORDERS)] for a, b in ((wq_in, wq5), (wo_in, wo5)))

    def each(jobs, n, *names):
        for name in names:
            for job in jobs:
                getattr(job[n], name)()

    each(jobs_q, 0, "start")
    each(jobs_o, 0, "start")
    gain, b_out = gain_ref[...][None, :], bout_ref[...].astype(F32)[None, :]
    parts = 3
    step = half // parts
    slot_h = copies.slots(parts)
    slot_dy, slot_wq, slot_wo, slot_o, slot_dqkv = (copies.slots(n) for n in (1, 1, 1, 1, 3))
    att = Attention(qkv, o, wq5, tab_ref, base_ref, sink_ref, dsink, keys, vals, dk, dv, top, inv, bias)
    att.prepare()
    for copy in local:
        copy.wait()
    copies.send(dy.at[mine, :], dy.at[mine, :], slot_dy, partner())

    pieces = iter(range(parts))

    def norm_piece():
        k = next(pieces)
        first = k * step

        @pl.loop(0, step // 32)
        def _(i):
            at = span(i, 32, first)
            xv = jnp.concatenate([x_low[at, :], x_high[at, :]], axis=1).astype(F32)
            inv = lax.rsqrt(jnp.mean(xv * xv, axis=-1, keepdims=True) + EPS)
            h[span(i, 32, start + first), :] = (xv * inv * gain).astype(BF16)

        return k

    def send_piece(k):
        at = span(k, step, start)
        copies.send(h.at[at, :], h.at[at, :], slot_h + k, partner())

    ready = norm_piece()
    each(jobs_q, 0, "finish")
    each(jobs_q, 1, "start")
    each(jobs_o, 0, "finish")
    send_piece(ready)
    ready = norm_piece()
    each(jobs_q, 1, "finish")
    each(jobs_q, 2, "start")
    send_piece(ready)
    send_piece(norm_piece())
    each(jobs_q, 2, "mid")
    each(jobs_o, 1, "start")
    for k in range(parts):
        copies.arrive(h.at[span(k, step, (1 - tp) * half), :], slot_h + k, partner())
    copies.arrive(dy.at[theirs, :], slot_dy, partner())
    each(jobs_q, 2, "finish")

    @pl.loop(0, 16)
    def _(n):
        wq[span(n, 96), :] = wq5[lax.div(n, 4), lax.rem(n, 4)].reshape(96, cols)

    b_qkv = bqkv_ref[...].astype(F32)[None, :]
    tile = 384

    def qkv_tile(n):
        qkv[span(n, tile), :] = (dot_nn(h[span(n, tile), :], wq[...]) + b_qkv).astype(BF16)

    qkv_tile(0)
    copies.send(wq, wq2, slot_wq, partner())
    each(jobs_o, 1, "finish")
    each(jobs_o, 2, "start")
    for n in range(1, 4):
        qkv_tile(n)
    att.forward(0, att.blocks // 2)
    each(jobs_o, 2, "mid")
    att.forward(att.blocks // 2, att.blocks)
    copies.send(o.at[theirs, :], o2, slot_o, partner())
    each(jobs_o, 2, "finish")

    def slabs(z, pair):
        return wo5[z, pl.ds(pair * 2, 2)].reshape(192, d // 2)

    @pl.loop(0, 8)
    def _(n):
        group = slabs(lax.div(n, 2), lax.rem(n, 2))
        for c in PAIR:
            wo[span(n, 96), span(c, d // 2)] = dot_nn(perm_ref[c], group).astype(BF16)

    copies.send(wo, wo2_hbm, slot_wo, partner())
    scatters = []
    for jobs, src, out, padded in ((WO_JOBS, go, go_out, True), (WQ_JOBS, gq, gq_out, False)):
        for job in jobs:
            five, bufs = bufs[:5], bufs[5:]
            if padded:
                five[4][...] = jnp.zeros(five[4].shape, F32)
            scatters.append(scatter_steps(copies, src, out, *job, five, padded))
    s_wo, s_0, s_1, s_2 = scatters[:2], scatters[2:3], scatters[3:5], scatters[5:]

    @pl.loop(0, 2)
    def _(m):
        @pl.loop(0, 3)
        def _(n):
            at, to = span(m, tile), span(n, 2 * GROUP)
            go[pl.ds(m * 2, 2), :, :, to] = dot_tn(o[:, at], dy[:, to]).reshape(2, 4, 48, 2 * GROUP)

    copies.drain()
    advance(s_wo)
    @pl.loop(0, 4)
    def _(n):
        at = span(n, tile)
        wq5[n, :, :, :, pl.ds(0, width)] = dot_nt(dy[at, :], wo[...]).astype(BF16).reshape(*RING, 24, width)


    def done(g):
        return pl.ds(g * GROUP, GROUP if g < 2 else 2 * GROUP)

    def wq_grad(to):

        @pl.loop(0, 4)
        def _(m):
            gq[m, :, :, :, to] = dot_tn(h[:, span(m, tile)], qkv[:, to]).reshape(*RING, 24, to.size)

    for g, (jobs, after) in enumerate(((s_0, s_wo), (s_1, s_0), (s_2, s_wo + s_0))):
        att.backward(g)
        if g == 2:
            att.backward_kv()
        copies.send(qkv.at[theirs, done(g)], dqkv2.at[:, done(g)], slot_dqkv + g, partner())
        if jobs is s_2:
            advance(s_1)
        wq_grad(done(g))
        advance(after, jobs)
    own = ar.at[Z, coord(Z)]
    own[...] = jnp.zeros(own.shape, F32)
    small = SmallSums(copies, ar)
    ones = jnp.ones((8, 2 * half), BF16)
    own[2:3, 0:cols] = dot_nn(ones, qkv[...])[0:1]
    own[3:4, 0:width] = dsink[...]
    own[1:2, :] = dot_nn(ones[:, 0:half], dy[mine, :])[0:1]
    loads = [pltpu.make_async_copy(x5_in.at[:, :, :, :, span(c, d // 2)], wo5.at[pl.ds(c * 2, 2)], loc_sem.at[c]) for c in PAIR]
    wo2 = h.at[pl.ds(0, half), :]
    loads.append(pltpu.make_async_copy(wo2_hbm, wo2, loc_sem.at[2]))
    for ref, slot in ((wo2_hbm, slot_wo), (wq2, slot_wq), (o2, slot_o)):
        copies.arrive(ref, slot, partner())
    for copy in loads:
        copy.start()
    for g in range(3):
        copies.arrive(dqkv2.at[:, done(g)], slot_dqkv + g, partner())
    wide_half = d // 2

    def dh_tiles(c):
        to = span(c, wide_half)

        @pl.loop(0, 2)
        def _(n):
            h[span(n, tile, half), to] = (dot_nt(qkv[span(n, tile, start), :], wq[to, :]) + dot_nt(dqkv2[span(n, tile), :], wq2[to, :])).astype(BF16)

    dh_tiles(0)
    advance(s_wo)
    dh_tiles(1)
    for copy in loads:
        copy.wait()
    rows = 48
    gain_sum[...] = jnp.zeros(gain_sum.shape, F32)

    def norm_back(c):
        count = half // rows // 2

        @pl.loop(c * count, c * count + count)
        def _(n):
            at = span(n, rows, start)
            z, yy, pair = lax.div(n, 8), lax.rem(lax.div(n, 2), 4), pl.ds(lax.rem(n, 2) * 2, 2)
            xv = jnp.concatenate([wo5[z + c, yy, pair].reshape(rows, d // 2) for c in (0, 2)], axis=1).astype(F32)
            dh = h[span(n, rows, half), :].astype(F32)
            inv = lax.rsqrt(jnp.mean(xv * xv, axis=-1, keepdims=True) + EPS)
            xn, gg = xv * inv, dh * gain
            dx = inv * (gg - xn * jnp.mean(gg * xn, axis=-1, keepdims=True))
            dy[at, :] = (dy[at, :].astype(F32) + dx).astype(BF16)
            gain_sum[...] = gain_sum[...] + jnp.sum((dh * xn).reshape(rows // 8, 8, d), axis=0)

    norm_back(0)
    advance(s_2)
    norm_back(1)
    own[0:1, :] = jnp.sum(gain_sum[...], axis=0, keepdims=True)
    store_dx = pltpu.make_async_copy(dy.at[mine, :], dx_out, loc_sem.at[7])
    store_dx.start()
    small.start(0)
    advance(s_1)
    def y_tiles(c):
        to = span(c, wide_half)

        @pl.loop(0, 2)
        def _(n):
            at = span(n, tile)
            xv = wo5[n + 2 * c].reshape(tile, wide_half).astype(F32)
            acc = dot_nn(o[span(n, tile, start), :], wo[:, to]) + dot_nn(o2[at, :], wo2[:, to])
            dy[span(n, tile, (1 - tp) * half), to] = (xv + acc + b_out[:, c * wide_half:(c + 1) * wide_half]).astype(BF16)

    y_tiles(0)
    small.finish(0)
    small.start(1)
    advance(s_2, s_0, s_wo)
    y_tiles(1)
    store_y = pltpu.make_async_copy(dy.at[theirs, :], y_out, loc_sem.at[6])
    store_y.start()
    small.finish(1)
    small.start(2)
    advance(s_2, s_1)
    small.finish(2)
    small.start(3)
    advance(s_0, s_wo, s_1, s_2)
    small.finish(3)
    both = ar[3, 0] + ar[3, 1]
    row = ar[3, tp]
    gain_out[...] = both[0]
    gbout_out[...] = both[1]
    bqkv_out[...] = row[2, 0:cols]
    lane = lax.broadcasted_iota(jnp.int32, (1, L), 1)
    sinks = jnp.zeros(lane.shape, F32)
    for n in range(width // L):
        sinks = jnp.where(lane == n, jnp.sum(row[3:4, n * L:n * L + L], axis=1, keepdims=True), sinks)
    sink_out[...] = sinks[0]
    stores = [pltpu.make_async_copy(a, b, loc_sem.at[n]) for n, (a, b) in enumerate(zip((gq_out, go_out, gain_out, gbout_out, bqkv_out, sink_out), hbm_outs))]
    for copy in stores[1:]:
        copy.start()
    for jobs in (s_wo, s_0, s_1, s_2):
        for job in jobs:
            assert next(job, None) is None
    copies.drain()
    stores[0].start()
    for copy in stores + [store_y, store_dx]:
        copy.wait()


VM = pl.BlockSpec(memory_space=pltpu.VMEM)
ANY = pl.BlockSpec(memory_space=pl.ANY)


def layer(wq, wo, x, x5, dy, gain, b_out, b_qkv, sinks, perm, tab, base):
    half, d = x.shape
    cols, width = wq.shape[1], wo.shape[1]
    seq = 2 * half
    n = 10 + 10 + len(ORDERS + ORDERS) * 12 + len(WQ_JOBS) * 5 + len(WO_JOBS) * 7
    sds = jax.ShapeDtypeStruct
    shapes = ((4,) + RING + wq.shape, (4,) + RING + wo.shape, (seq, d), (seq, d), (seq, cols), (seq, width), (d, cols), (width, d), (d, cols), (half, width), (half, cols))
    scratch = [pltpu.VMEM(shape, BF16) for shape in shapes]
    scratch += [pltpu.VMEM((4, *RING, 24, cols), F32), pltpu.VMEM((*RING, 48, d), F32), pltpu.VMEM((4, *RING, d), F32)]
    scratch += [pltpu.VMEM((seq + L, L), t) for t in (BF16, BF16, F32, F32)] + [pltpu.VMEM((1, width), F32)]
    scratch += [pltpu.VMEM((seq // L, width), F32)] * 2 + [pltpu.VMEM((2, GROUP, L), BF16), pltpu.VMEM((8, d), F32)]
    outs = (sds((half, d), BF16), sds((half, d), BF16), sds((24, cols), F32), sds((12, d), F32), sds((d,), F32), sds((d,), F32), sds((cols,), F32), sds((L,), F32))
    scratch += [pltpu.VMEM(o.shape, F32) for o in outs[2:]] + [pltpu.SemaphoreType.DMA((k,)) for k in (8, 116, n)]
    results = pl.pallas_call(
        layer_kernel, name="layer", out_shape=outs + (sds((width, d), BF16),),
        in_specs=[VM, VM, ANY, ANY, ANY, VM, VM, VM, pl.BlockSpec(memory_space=pltpu.SMEM)] + [VM] * 3, out_specs=(ANY,) * 9, scratch_shapes=scratch + scatter_scratch(),
        compiler_params=pltpu.CompilerParams(collective_id=0, has_side_effects=True, vmem_limit_bytes=VMEM_LIMIT),
    )(wq, wo, x, x5, dy, gain, b_out, b_qkv, sinks, perm, tab, base)
    return pl.pallas_call(
        hand_over, name="hand_over", out_shape=outs, in_specs=[ANY] * 8, out_specs=(ANY,) * 8,
        scratch_shapes=[pltpu.VMEM(o.shape, o.dtype) for o in outs] + [pltpu.SemaphoreType.DMA((8, 4))] * 2,
    )(*results[:-1])


def hand_over(*refs):
    *refs, in_sem, out_sem = refs
    n = len(refs) // 3
    ins, outs, bufs = refs[:n], refs[n:2 * n], refs[2 * n:]
    copies = []
    for k, (a, buf, b) in enumerate(zip(ins, bufs, outs)):
        parts = in_sem.shape[1] if k < 2 else 1
        step = a.shape[0] // parts
        for n in range(parts):
            at = pl.ds(n * step, step)
            copies.append((pltpu.make_async_copy(a.at[at], buf.at[at], in_sem.at[k, n]), pltpu.make_async_copy(buf.at[at], b.at[at], out_sem.at[k, n])))
    for load, _ in copies:
        load.start()
    for load, store in copies:
        load.wait()
        store.start()
    for _, store in copies:
        store.wait()


def rope_constants(n_blocks):
    freq = np.tile(ROPE_BASE ** (-2.0 * np.arange(L // 2) / L), 2)
    sign = np.where(np.arange(L) < L // 2, -1.0, 1.0)

    def pair(positions):
        angle = positions[:, None] * freq[None, :]
        return jnp.asarray(np.stack([np.cos(angle), np.sin(angle) * sign]), F32)

    return pair(np.arange(L)), pair(np.arange(n_blocks) * L)


def row_permutation():
    row = np.arange(96)[:, None]
    col = np.arange(192)[None, :]
    return jnp.asarray(np.stack([col == row // 12 * 24 + c * 12 + row % 12 for c in PAIR]), BF16)


def solution(mesh):
    act_spec = P("fsdp", "tp", None)
    wout_spec = P(("tp", "fsdp"), None)
    in_specs = (act_spec, act_spec, P(), P("fsdp", "tp"), P("tp"), P("tp"), wout_spec, P())
    out_specs = (act_spec, act_spec, P(), P("fsdp", "tp"), P("tp"), P("tp"), wout_spec, P())

    def device_step(resid_loc, grad_loc, norm_gain, wqkv_loc, bqkv_loc, sink_loc, wout_loc, b_out):
        x, dy = resid_loc[0], grad_loc[0]
        half, d = x.shape
        heads = sink_loc.shape[0]
        wo_slab = jnp.concatenate([wout_loc[:, :d // 2], wout_loc[:, d // 2:]], axis=0)
        tab, base = rope_constants(2 * half // L)
        y, dx, gq, go, gain_g, bout_g, bqkv_g, sink_g = layer(wqkv_loc, wo_slab, x, x.reshape(2, *RING, 24, d), dy, norm_gain, b_out, bqkv_loc, sink_loc, row_permutation(), tab, base)
        return (y[None], dx[None], gain_g, gq, bqkv_g, sink_g[:heads], go, bout_g)

    return jax.shard_map(device_step, mesh=mesh, in_specs=in_specs, out_specs=out_specs, check_vma=False)
```
